256 devices in a mesh: seq: 64 (over x, z, core), head: 4 (over y).
Axes of the slice: x: 4, y: 4, z: 8, core: 2. Of those that a mesh axis runs over, the one named last changes fastest.
Arguments:
- hidden_in: bfloat16 [256, 4096], P(None, 'seq'), may hold values from -6 to 6
- norm_gain: bfloat16 [1, 4096], P(None, 'seq'), may hold values from 0.25 to 1.75
- w_query: bfloat16 [4096, 4096], P('seq', 'head'), may hold values from -1 to 1
- w_key: bfloat16 [4096, 1024], P('seq', 'head'), may hold values from -1 to 1
- w_value: bfloat16 [4096, 1024], P('seq', 'head'), may hold values from -0.09375 to 0.09375
- w_out: bfloat16 [4096, 4096], P('head', 'seq'), may hold values from -0.09375 to 0.09375
- cache_keys: bfloat16 [262144, 8, 128], P('seq', 'head'), may hold values from -400 to 400
- cache_values: bfloat16 [262144, 8, 128], P('seq', 'head'), may hold values from -12 to 12
- lengths: int32 [64], replicated, may hold values from 512 to 4096, as said below
- span_start: int32 [1], replicated, may hold values from 0 to 256
Outputs:
- attn_out: bfloat16 [256, 4096], P('head', 'seq')
The draws below stay inside these ranges and needn't reach their ends.
Inputs may be any that keep to these rules, and one draw needn't show every extreme that they name: Slots 0 to lengths[s] - 1 of shard s are live, the others empty; in every draw some shard is full.
All inputs are finite; a program needn't handle non-finite values.
Results may differ from the reference program's by a relative error of at most 0.039.
The reference program's roundings to bfloat16 on the way count: a program that leaves them out, or rounds other values in their place, can miss the bound.
Values may be sent and summed in bfloat16 or wider, within the bound.
A program may use at most 64 MiB of HBM per device.

```python
import math
import jax
import jax.numpy as jnp
from jax import lax

D = 4096
HEADS = 32
KV_HEADS = 8
HEAD_DIM = 128
SPAN = 256
CACHE_DEV = 4096
CACHE = 262144


def draw_lengths(key, part):
    key = jax.random.fold_in(key, 7)
    shard_count = CACHE // CACHE_DEV
    key_light, key_heavy, key_order = jax.random.split(key, 3)
    light_len = jax.random.randint(key_light, (shard_count,), CACHE_DEV // 8, CACHE_DEV // 3 + 1)
    heavy_len = jax.random.randint(key_heavy, (shard_count,), CACHE_DEV * 3 // 4, CACHE_DEV + 1)
    position_rank = jnp.argsort(jax.random.permutation(key_order, shard_count))
    lengths = jnp.where(position_rank < shard_count // 4, heavy_len, light_len)
    return jnp.where(position_rank == 0, CACHE_DEV, lengths).astype(jnp.int32)


def shared_projections(key):
    key_common, key_private = jax.random.split(jax.random.fold_in(key, 17), 2)
    group_size = HEADS // KV_HEADS
    spread = D ** (-0.5)
    common = jnp.clip(jax.random.normal(key_common, (D, KV_HEADS, 1, HEAD_DIM), jnp.float32), -6.0, 6.0) * spread
    private = jnp.clip(jax.random.normal(key_private, (D, KV_HEADS, group_size, HEAD_DIM), jnp.float32), -6.0, 6.0) * spread
    coupling = min(0.95, (math.log(0.4 * CACHE) + 0.8) / (2.005 * math.sqrt(HEAD_DIM)))
    query_part = coupling * common + math.sqrt(1.0 - coupling * coupling) * private
    return (query_part.reshape(D, HEADS * HEAD_DIM), common.reshape(D, KV_HEADS * HEAD_DIM))


def draw_w_query(key, part):
    return shared_projections(key)[0].astype(jnp.bfloat16)


def draw_w_key(key, part):
    return shared_projections(key)[1].astype(jnp.bfloat16)


def draw_cache_keys(key, part):
    key_base = jax.random.fold_in(jax.random.fold_in(key, 11), 0)
    normal_part = jnp.clip(jax.random.normal(key_base, (CACHE, KV_HEADS, HEAD_DIM), jnp.float32), -6.0, 6.0)
    return normal_part.astype(jnp.bfloat16)


def draw_cache_values(key, part):
    shard_count = CACHE // CACHE_DEV
    key_noise, key_shift = jax.random.split(jax.random.fold_in(key, 13), 2)
    shifts = jnp.clip(jax.random.normal(key_shift, (shard_count, 1, KV_HEADS, HEAD_DIM), jnp.float32), -4.0, 4.0)
    noise = jnp.clip(jax.random.normal(key_noise, (shard_count, CACHE_DEV, KV_HEADS, HEAD_DIM), jnp.float32), -4.0, 4.0)
    return (noise + shifts).reshape(CACHE, KV_HEADS, HEAD_DIM).astype(jnp.bfloat16)


def level_of(own_key, extent, shards, least, top_value):
    def one(axis_at, parts):
        draws = jax.random.uniform(jax.random.fold_in(jax.random.fold_in(own_key, 6), axis_at), (parts,), jnp.float32, least / len(shards), top_value / len(shards))
        return jnp.repeat(jnp.exp(draws), extent[axis_at] // parts).reshape((-1,) + (1,) * (len(extent) - axis_at - 1))

    factor_of = one(*shards[0])
    for cut in shards[1:]:
        factor_of = factor_of * one(*cut)
    return factor_of


def normal_values(stream_key, dims, scale, most, shards=(), kind=jnp.bfloat16):
    result = jax.random.normal(stream_key, dims, jnp.float32) * scale
    if len(shards) > 0:
        result = level_of(stream_key, dims, shards, -0.22, 0.18) * result
    return jnp.clip(result, min=-most, max=most).astype(kind)


def setup_inputs(seed: int = 0) -> dict:
    keys = jax.random.split(jax.random.key(seed), 11)
    hidden_in = normal_values(keys[0], (SPAN, D), 1.0, 6.0, ((1, 64),))
    norm_gain = jnp.clip(1.0 + 0.15 * jax.random.normal(keys[1], (1, D), jnp.float32), 0.25, 1.75).astype(jnp.bfloat16)
    w_query = draw_w_query(jax.random.fold_in(keys[10], 71), 0)
    w_key = draw_w_key(jax.random.fold_in(keys[10], 71), 0)
    w_value = normal_values(keys[4], (D, KV_HEADS * HEAD_DIM), D ** -0.5, 0.09375, ((0, 64), (1, 4)))
    w_out = normal_values(keys[5], (HEADS * HEAD_DIM, D), (HEADS * HEAD_DIM) ** -0.5, 0.09375, ((0, 4), (1, 64)))
    cache_keys = draw_cache_keys(jax.random.fold_in(keys[10], 71), 0)
    cache_values = draw_cache_values(jax.random.fold_in(keys[10], 71), 0)
    lengths = draw_lengths(jax.random.fold_in(keys[10], 71), 0)
    span_start = jax.random.randint(keys[9], (1,), 0, SPAN + 1).astype(jnp.int32)
    return dict(hidden_in=hidden_in, norm_gain=norm_gain, w_query=w_query, w_key=w_key, w_value=w_value, w_out=w_out, cache_keys=cache_keys, cache_values=cache_values, lengths=lengths, span_start=span_start)


rope_base = 500000.0
stretch = 64.0
initial_context = 8192.0
ramp_low = 1.0
ramp_high = 32.0
epsilon = 1e-05
negative = -1e+30

def rope_parts(positions, head_dim):
    half_dim = head_dim // 2
    indices = jnp.arange(half_dim, dtype=jnp.float32)
    base_freq = jnp.power(jnp.float32(rope_base), -2.0 * indices / head_dim)
    wavelength = 2.0 * math.pi / base_freq
    turn_count = initial_context / wavelength
    ramp_share = jnp.clip((turn_count - ramp_low) / (ramp_high - ramp_low), 0.0, 1.0)
    frequency = (1.0 - ramp_share) * base_freq / stretch + ramp_share * base_freq
    angles = positions[:, None] * frequency[None, :]
    mscale = 0.1 * math.log(stretch) + 1.0
    return (jnp.cos(angles) * mscale, jnp.sin(angles) * mscale)

def rotate(vectors, cosine, sine_part):
    half_dim = vectors.shape[-1] // 2
    lower_half = vectors[..., :half_dim]
    upper_half = vectors[..., half_dim:]
    cosine = cosine[:, None, :]
    sine_part = sine_part[:, None, :]
    return jnp.concatenate([lower_half * cosine - upper_half * sine_part, upper_half * cosine + lower_half * sine_part], -1)

def round_trip(values):
    return lax.optimization_barrier(values.astype(jnp.bfloat16)).astype(jnp.float32)

def attend(running, queries, key_block, value_block, visible):
    maxima, totals, weighted = running
    scores = jnp.einsum('tgrd,kgd->grtk', queries, key_block)
    scores = jnp.where(visible, scores, negative)
    new_max = jnp.maximum(maxima, lax.optimization_barrier(jnp.max(scores, axis=-1)))
    probability = jnp.where(visible, jnp.exp(scores - new_max[..., None]), 0.0)
    rescale = jnp.exp(maxima - new_max)
    totals = totals * rescale + lax.optimization_barrier(jnp.sum(probability, axis=-1))
    weighted = weighted * rescale[..., None] + jnp.einsum('grtk,kgd->grtd', round_trip(probability), value_block)
    return (new_max, totals, weighted)

def reference(hidden_in, norm_gain, w_query, w_key, w_value, w_out, cache_keys, cache_values, lengths, span_start):
    group_size = HEADS // KV_HEADS
    input_f32 = hidden_in.astype(jnp.float32)
    inv_rms = lax.rsqrt(lax.optimization_barrier(jnp.mean(input_f32 * input_f32, axis=1, keepdims=True)) + epsilon)
    normed = (input_f32 * inv_rms * norm_gain.astype(jnp.float32)).astype(jnp.bfloat16)
    queries = jnp.dot(normed, w_query, preferred_element_type=jnp.float32)
    new_keys = round_trip(jnp.dot(normed, w_key, preferred_element_type=jnp.float32))
    new_values = round_trip(jnp.dot(normed, w_value, preferred_element_type=jnp.float32))
    new_values = new_values.reshape(SPAN, KV_HEADS, HEAD_DIM)
    first_pos = jnp.sum(lengths).astype(jnp.int32) + span_start[0]
    query_pos = (first_pos + jnp.arange(SPAN, dtype=jnp.int32)).astype(jnp.float32)
    cosine, sine_part = rope_parts(query_pos, HEAD_DIM)
    rotated = rotate(queries.reshape(SPAN, HEADS, HEAD_DIM), cosine, sine_part) * HEAD_DIM ** (-0.5)
    query_f32 = round_trip(rotated).reshape(SPAN, KV_HEADS, group_size, HEAD_DIM)
    key_rot = round_trip(rotate(new_keys.reshape(SPAN, KV_HEADS, HEAD_DIM), cosine, sine_part))
    offsets = jnp.cumsum(lengths) - lengths
    block_len = math.gcd(CACHE, 4096)

    def sweep_block(running, block_index):
        block_start = block_index * block_len
        key_block = lax.dynamic_slice_in_dim(cache_keys, block_start, block_len, 0).astype(jnp.float32)
        value_block = lax.dynamic_slice_in_dim(cache_values, block_start, block_len, 0).astype(jnp.float32)
        slot_ids = block_start + jnp.arange(block_len, dtype=jnp.int32)
        shard_ids = slot_ids // CACHE_DEV
        slot_in_shard = slot_ids - shard_ids * CACHE_DEV
        occupied = slot_in_shard < jnp.take(lengths, shard_ids)
        positions = (jnp.take(offsets, shard_ids) + slot_in_shard).astype(jnp.float32)
        block_cos, block_sin = rope_parts(positions, HEAD_DIM)
        block_keys = round_trip(rotate(key_block, block_cos, block_sin))
        return (attend(running, query_f32, block_keys, value_block, occupied[None, None, None, :]), None)
    running = (jnp.full((KV_HEADS, group_size, SPAN), negative, jnp.float32), jnp.zeros((KV_HEADS, group_size, SPAN), jnp.float32), jnp.zeros((KV_HEADS, group_size, SPAN, HEAD_DIM), jnp.float32))
    running, leftover = lax.scan(sweep_block, running, jnp.arange(CACHE // block_len, dtype=jnp.int32))
    causal = jnp.arange(SPAN)[None, :] <= jnp.arange(SPAN)[:, None]
    maxima, totals, weighted = attend(running, query_f32, key_rot, new_values, causal[None, None])
    attended = (weighted / totals[..., None]).transpose(2, 0, 1, 3).reshape(SPAN, HEADS * HEAD_DIM)
    attended = attended.astype(jnp.bfloat16)
    return jnp.dot(attended, w_out, preferred_element_type=jnp.float32).astype(jnp.bfloat16)
```

```python
import functools
import math

import jax
import jax.numpy as jnp
from jax import lax
from jax.experimental import pallas as pl
from jax.experimental.pallas import tpu as pltpu
from jax.sharding import Mesh
from jax.sharding import PartitionSpec as P

F32 = jnp.float32
BF16 = jnp.bfloat16
MESH = pl.DeviceIdType.MESH
LANES = 128
HALF = 64
ROWS = 32
CHUNK = 128
KEYS = 512

rope_base = 500000.0
stretch = 64.0
initial_context = 8192.0
ramp_low = 1.0
ramp_high = 32.0
epsilon = 1e-05
negative = -1e30
mscale = 0.1 * math.log(stretch) + 1.0


def frequencies():
    indices = jnp.arange(HALF, dtype=F32)
    base = jnp.power(F32(rope_base), -2.0 * indices / LANES)
    turns = initial_context / (2.0 * math.pi / base)
    share = jnp.clip((turns - ramp_low) / (ramp_high - ramp_low), 0.0, 1.0)
    freq = (1.0 - share) * base / stretch + share * base
    return jnp.concatenate([freq, freq])[None, :]


def cos_sin(angles):
    turns = jnp.floor(angles * (1.0 / (2.0 * math.pi)) + 0.5)
    first, second = 6.28125, 253.0 / 2.0**17
    third = 2.0 * math.pi - first - second
    rest = angles - turns * first - turns * second - turns * third
    return jnp.cos(rest), jnp.sin(rest)


def iota(shape, dim):
    return lax.broadcasted_iota(jnp.int32, shape, dim)


def signed(sine):
    return jnp.where(iota(sine.shape, 1) < HALF, -sine, sine)


def rotated(vectors, cosine, sine):
    return vectors * cosine + pltpu.roll(vectors, HALF, 1) * sine


def hi_lo(sums):
    high = sums.astype(BF16).astype(F32)
    return jnp.where(iota(sums.shape, 1) < HALF, high, sums - high)


def as_columns(rows):
    spare = LANES - rows.shape[0]
    if spare:
        rows = jnp.concatenate([rows, jnp.zeros((spare, LANES), F32)], 0)
    return rows.T


def kernel(
    dims,
    h_ref, g_ref, wq_ref, wk_ref, wv_ref, wo_ref, freq_ref, len_ref, start_ref, k_hbm, v_hbm,
    out_ref,
    kraw, vraw, tmp, ks, vs, tab_a, tab_b, k0,
    sb, rb, own, xs, xr, zs, zr, inv_ref, qbuf, s_ref,
    ob, lb, obs, obr, lss, lsr, oxs, oxr, lxs, lxr, ozs, ozr, lzs, lzr, wt,
    att, wobuf, p5s, p5r,
    kv_sem,
    c1s, c1r, x1s, x1r, z1s, z1r,
    z2s, z2r, x2s, x2r, c2s, c2r, ws, wr,
    c3s, c3r, c3ls, c3lr, x3s, x3r, x3ls, x3lr, z3s, z3r, z3ls, z3lr,
    z4s, z4r, c4s, c4r, y5s, y5r,
):
    nx, nz, nc, ny, d_model = dims
    x, z, c, y = (lax.axis_index(n) for n in ("x", "z", "c", "y"))
    sib = 1 - c
    slots = kraw.shape[0] // 2
    group = wq_ref.shape[1] // wk_ref.shape[1]
    kv = wk_ref.shape[1] // LANES
    heads = kv * group
    quarters = nz // kv
    tail = ROWS // quarters
    qc = heads * LANES
    kc = kv * LANES
    per_x = nc * ROWS

    def copy(src, dst, send, recv, **to):
        return pltpu.make_async_remote_copy(
            src_ref=src, dst_ref=dst, send_sem=send, recv_sem=recv, device_id=to, device_id_type=MESH
        )

    def other_x(k):
        return lax.rem(x + k, nx)

    def other_z(k):
        return lax.rem(z + k, nz)

    x_far = sorted(range(1, nx), key=lambda k: -min(k, nx - k))
    z_far = sorted(range(1, nz), key=lambda k: -min(k, nz - k))
    z_near = z_far[::-1]
    x_near = x_far[::-1]

    get_k = pltpu.make_async_copy(k_hbm, kraw, kv_sem.at[0])
    get_v = pltpu.make_async_copy(v_hbm, vraw, kv_sem.at[1])
    get_k.start()
    get_v.start()

    barrier = pltpu.get_barrier_semaphore()

    def greet(**to):
        pl.semaphore_signal(barrier, inc=1, device_id=to, device_id_type=MESH)

    greet(c=sib)
    for k in range(1, nx):
        greet(x=other_x(k))
    for k in range(1, nz):
        greet(z=other_z(k))
    for k in range(1, ny):
        greet(x=y, y=lax.rem(y + k, ny))

    @pl.when(x != y)
    def _():
        greet(x=y, y=y)

    hidden = h_ref[...].astype(F32)
    scaled = (hidden * g_ref[...].astype(F32)).astype(BF16)
    squares = jnp.sum(hidden * hidden, axis=1, keepdims=True)
    sums = hi_lo(jnp.broadcast_to(squares, (h_ref.shape[0], LANES)))

    def part(value, cc):
        blocks = [
            jnp.where(cc == 0, value[b * per_x : b * per_x + ROWS], value[b * per_x + ROWS : b * per_x + 2 * ROWS])
            for b in range(nx)
        ]
        return jnp.concatenate(blocks, 0)

    def project(cc, store):
        rows = part(scaled.astype(F32), cc).astype(BF16)
        for at, w in ((0, wq_ref), (qc, wk_ref), (qc + kc, wv_ref)):
            got = jnp.dot(rows, w[...], preferred_element_type=F32)
            for b in range(nx):
                store(b, at, got[b * ROWS : (b + 1) * ROWS])
        extra = part(sums, cc)
        for b in range(nx):
            store(b, qc + 2 * kc, extra[b * ROWS : (b + 1) * ROWS])

    def to_sibling(b, at, value):
        sb[b, :, at : at + value.shape[1]] = value.astype(BF16)

    def to_own(b, at, value):
        own[b, :, at : at + value.shape[1]] = value

    project(sib, to_sibling)

    my = (x * nz + z) * nc + c
    count = nx * nz * nc

    def add_lengths(r, carry):
        before, total = carry
        return before + jnp.where(r < my, len_ref[r], 0), total + len_ref[r]

    offset, first_pos = lax.fori_loop(0, count, add_lengths, (jnp.int32(0), jnp.int32(0)))
    first_pos = first_pos + start_ref[0]
    live = len_ref[my]
    freq = freq_ref[...]

    peers = 1 + (nx - 1) + (nz - 1) + (ny - 1)
    pl.semaphore_wait(barrier, jnp.where(x != y, peers + 1, peers))

    core1 = [copy(sb.at[b], rb.at[b], c1s.at[b], c1r.at[b], c=sib) for b in range(nx)]
    for b in range(nx):
        core1[b].start()

    project(c, to_own)
    half = wo_ref.shape[0] // 2
    wobuf[x] = jnp.concatenate([wo_ref[0:half, :], wo_ref[half:, :]], 1)

    for b in range(nx):
        core1[b].wait_recv()
    for k in x_far:
        b = other_x(k)
        xs[b] = (own[b] + rb[b].astype(F32)).astype(BF16)
        copy(xs.at[b], xr.at[x], x1s.at[b], x1r.at[x], x=b).start()

    a_count = slots // CHUNK
    a_pos = (offset + CHUNK * iota((a_count, LANES), 0)).astype(F32)
    a_cos, a_sin = cos_sin(a_pos * freq)
    tab_a[0] = a_cos * mscale
    tab_a[1] = a_sin * mscale
    b_cos, b_sin = cos_sin(iota((CHUNK, LANES), 0).astype(F32) * freq)
    tab_b[0] = b_cos
    tab_b[1] = b_sin

    get_k.wait()

    def rotate_chunk(a, _):
        at = pl.multiple_of(a * CHUNK, CHUNK)
        tmp[...] = kraw[pl.ds(pl.multiple_of(2 * at, 2 * CHUNK), 2 * CHUNK), :].astype(F32)
        cos_a = tab_a[0, pl.ds(a, 1), :]
        sin_a = tab_a[1, pl.ds(a, 1), :]
        cosine = cos_a * tab_b[0] - sin_a * tab_b[1]
        sine = signed(sin_a * tab_b[0] + cos_a * tab_b[1])
        alive = at + iota((CHUNK, LANES), 0) < live
        for g in range(kv):
            keys = rotated(tmp[pl.ds(g, CHUNK, stride=kv), :], cosine, sine)

            @pl.when(a == 0)
            def _():
                k0[g] = keys[0:8]

            keys = jnp.where(alive, keys, k0[g, 0:1, :])
            ks[g, pl.ds(at, CHUNK), :] = keys.astype(BF16)
        return 0

    lax.fori_loop(0, a_count, rotate_chunk, 0)

    gathered = own[x] + rb[x].astype(F32)
    for k in x_near:
        b = other_x(k)
        copy(xs.at[b], xr.at[b], x1s.at[b], x1r.at[b], x=b).wait_recv()
        gathered = gathered + xr[b].astype(F32)
    own[x] = gathered
    mixed = own[x, :, qc + 2 * kc : qc + 2 * kc + LANES]
    zs_sums = hi_lo(mixed + pltpu.roll(mixed, HALF, 1)).astype(BF16)
    for t in range(nz):
        g, quarter = t // quarters, t % quarters
        zs[t, 0:ROWS, :] = own[x, :, t * LANES : (t + 1) * LANES].astype(BF16)
        pair = [
            own[x, quarter * tail : (quarter + 1) * tail, at + g * LANES : at + (g + 1) * LANES]
            for at in (qc, qc + kc)
        ]
        zs[t, ROWS : ROWS + 2 * tail, :] = jnp.concatenate(pair, 0).astype(BF16)
        zs[t, ROWS + 2 * tail :, :] = zs_sums
    for k in z_far:
        b = other_z(k)
        copy(zs.at[b], zr.at[z], z1s.at[b], z1r.at[z], z=b).start()

    get_v.wait()

    def value_chunk(a, _):
        at = pl.multiple_of(a * CHUNK, CHUNK)
        tmp[...] = vraw[pl.ds(pl.multiple_of(2 * at, 2 * CHUNK), 2 * CHUNK), :].astype(F32)
        alive = at + iota((CHUNK, LANES), 0) < live
        ones = jnp.where(alive, 1.0, 0.0).astype(BF16)
        for g in range(kv):
            values = jnp.where(alive, tmp[pl.ds(g, CHUNK, stride=kv), :], 0.0)
            vs[g, pl.ds(at, CHUNK), 0:LANES] = values.astype(BF16)
            vs[g, pl.ds(at, CHUNK), LANES:] = ones
        return 0

    lax.fori_loop(0, a_count, value_chunk, 0)

    total = zs[z].astype(F32)
    for k in z_near:
        b = other_z(k)
        copy(zs.at[b], zr.at[b], z1s.at[b], z1r.at[b], z=b).wait_recv()
        total = total + zr[b].astype(F32)
    mixed = total[ROWS + 2 * tail :]
    inverse = lax.rsqrt((mixed + pltpu.roll(mixed, HALF, 1)) * (1.0 / d_model) + epsilon)
    inv_ref[...] = inverse
    my_g, my_quarter = lax.div(z, quarters), lax.rem(z, quarters)
    first_token = x * per_x + c * ROWS
    q_pos = (first_pos + first_token + iota((ROWS, LANES), 0)).astype(F32)
    q_cos, q_sin = cos_sin(q_pos * freq)
    scale = LANES**-0.5
    query = rotated(total[0:ROWS] * inverse, q_cos * mscale, signed(q_sin * mscale)) * scale
    qbuf[c, x, z] = query.astype(BF16)

    z2 = []
    for k in z_far:
        b = other_z(k)
        copy(qbuf.at[c, x, z], qbuf.at[c, x, z], z2s.at[b], z2r.at[z], z=b).start()

    def piece_to_x(t):
        for k in x_far:
            b = other_x(k)
            copy(qbuf.at[c, x, t], qbuf.at[c, x, t], x2s.at[b, t], x2r.at[x, t], x=b).start()

    piece_to_x(z)

    k_first = first_token + my_quarter * tail
    inv_new = inv_ref[pl.ds(pl.multiple_of(my_quarter * tail, tail), tail), :]
    k_pos = (first_pos + k_first + iota((tail, LANES), 0)).astype(F32)
    k_cos, k_sin = cos_sin(k_pos * freq)
    new_k = (total[ROWS : ROWS + tail] * inv_new).astype(BF16).astype(F32)
    new_k = rotated(new_k, k_cos * mscale, signed(k_sin * mscale))
    new_v = total[ROWS + tail : ROWS + 2 * tail] * inv_new
    empty = jnp.zeros((LANES - tail, LANES), F32)
    new_k = jnp.concatenate([new_k, empty], 0).astype(BF16)
    new_v = jnp.concatenate([new_v, empty], 0).astype(BF16)
    new_ones = jnp.where(iota((LANES, LANES), 0) < tail, 1.0, 0.0).astype(BF16)
    for g in range(kv):
        ks[g, slots:, :] = new_k
        vs[g, slots:, 0:LANES] = new_v
        vs[g, slots:, LANES:] = new_ones

    for k in z_near:
        b = other_z(k)
        copy(qbuf.at[c, x, b], qbuf.at[c, x, b], z2s.at[b], z2r.at[b], z=b).wait_recv()
        piece_to_x(b)

    def block_to_core(b):
        return copy(qbuf.at[c, b], qbuf.at[c, b], c2s.at[b], c2r.at[b], c=sib)

    block_to_core(x).start()
    for k in x_near:
        b = other_x(k)
        for t in range(nz):
            copy(qbuf.at[c, b, t], qbuf.at[c, b, t], x2s.at[b, t], x2r.at[b, t], x=b).wait_recv()
        block_to_core(b).start()
    for k in x_far:
        b = other_x(k)
        copy(wobuf.at[x], wobuf.at[x], ws.at[b], wr.at[x], x=b).start()

    rows = 2 * group * ROWS
    pairs = nx // 2

    def attend(cc, p):
        token = (
            2 * p * per_x
            + lax.div(iota((rows, LANES), 0), group * ROWS) * per_x
            + cc * ROWS
            + lax.rem(iota((rows, LANES), 0), ROWS)
        )
        lane = iota((rows, LANES), 1)
        seen = jnp.logical_and(lane < tail, k_first + lane <= token)
        for g in range(kv):
            q = qbuf[cc, pl.ds(2 * p, 2), g * group : (g + 1) * group].reshape(rows, LANES)
            most = jnp.full((rows, LANES), negative, F32)
            for at in range(0, slots, KEYS):
                score = lax.dot_general(
                    q, ks[g, at : at + KEYS, :], (((1,), (1,)), ((), ())), preferred_element_type=F32
                )
                s_ref[g, :, at : at + KEYS] = score
                for lo in range(0, KEYS, LANES):
                    most = jnp.maximum(most, score[:, lo : lo + LANES])
            score = lax.dot_general(
                q, ks[g, slots:, :], (((1,), (1,)), ((), ())), preferred_element_type=F32
            )
            score = jnp.where(jnp.logical_and(seen, my_g == g), score, negative)
            most = jnp.max(jnp.maximum(most, score), axis=1, keepdims=True)
            acc = jnp.dot(
                jnp.exp(score - most).astype(BF16), vs[g, slots:, :], preferred_element_type=F32
            )
            for at in range(0, slots, KEYS):
                prob = jnp.exp(s_ref[g, :, at : at + KEYS] - most).astype(BF16)
                acc = acc + jnp.dot(prob, vs[g, at : at + KEYS, :], preferred_element_type=F32)
            sums = acc[:, LANES:]
            result = acc[:, 0:LANES] / sums
            lse = most + jnp.log(sums)
            for j in range(2):
                cut = slice(j * group * ROWS, (j + 1) * group * ROWS)
                ob[2 * p + j, g * group * ROWS : (g + 1) * group * ROWS, :] = result[cut]
                lb[2 * p + j, g : g + 1, :] = lse[cut].T[0:1]

    def core3(b):
        return (
            copy(obs.at[b], obr.at[b], c3s.at[b], c3r.at[b], c=sib),
            copy(lss.at[b], lsr.at[b], c3ls.at[b], c3lr.at[b], c=sib),
        )

    def combine(outs, logs):
        top = functools.reduce(jnp.maximum, logs)
        weights = [jnp.exp(v - top) for v in logs]
        whole = sum(weights)
        columns = as_columns(jnp.concatenate([w / whole for w in weights], 0))
        parts = []
        for g in range(kv):
            cut = slice(g * group * ROWS, (g + 1) * group * ROWS)
            parts.append(sum(columns[:, 8 * i + g : 8 * i + g + 1] * o[cut] for i, o in enumerate(outs)))
        return jnp.concatenate(parts, 0), top + jnp.log(whole)

    lb[...] = jnp.zeros_like(lb)
    for k in range(nx):
        b = other_x(k)
        copy(qbuf.at[sib, b], qbuf.at[sib, b], c2s.at[b], c2r.at[b], c=sib).wait_recv()

    def pair_of(j):
        return lax.rem(lax.div(x, 2) + 1 + j, pairs)

    def sibling_unit(j, _):
        p = pair_of(j)
        attend(sib, p)
        for i in range(2):
            b = 2 * p + i
            obs[b] = ob[b].astype(BF16)
            lss[b] = lb[b]
            for one in core3(b):
                one.start()
        return 0

    for j in range(pairs):
        sibling_unit(j, 0)

    def own_unit(j, _):
        p = pair_of(j)
        attend(c, p)
        for i in range(2):
            b = 2 * p + i
            for one in core3(b):
                one.wait_recv()
            out, lse = combine([ob[b], obr[b].astype(F32)], [lb[b], lsr[b]])
            ob[b] = out
            lb[b] = lse
            oxs[b] = out.astype(BF16)
            lxs[b] = lse

            @pl.when(b != x)
            def _():
                copy(oxs.at[b], oxr.at[x], x3s.at[b], x3r.at[x], x=b).start()
                copy(lxs.at[b], lxr.at[x], x3ls.at[b], x3lr.at[x], x=b).start()

        return 0

    for j in range(pairs):
        own_unit(j, 0)

    outs, logs = [ob[x]], [lb[x]]
    for k in x_near:
        b = other_x(k)
        copy(oxs.at[b], oxr.at[b], x3s.at[b], x3r.at[b], x=b).wait_recv()
        copy(lxs.at[b], lxr.at[b], x3ls.at[b], x3lr.at[b], x=b).wait_recv()
        outs.append(oxr[b].astype(F32))
        logs.append(lxr[b])
    out, lse = combine(outs, logs)
    ozs[...] = out.astype(BF16).reshape(nz, ROWS, LANES)
    lzs[...] = lse
    for k in z_far:
        b = other_z(k)
        copy(ozs.at[b], ozr.at[z], z3s.at[b], z3r.at[z], z=b).start()
        copy(lzs, lzr.at[z], z3ls.at[b], z3lr.at[z], z=b).start()

    outs, logs = [ozs[z].astype(F32)], [lzs[...]]
    for k in z_near:
        b = other_z(k)
        copy(ozs.at[b], ozr.at[b], z3s.at[b], z3r.at[b], z=b).wait_recv()
        copy(lzs, lzr.at[b], z3ls.at[b], z3lr.at[b], z=b).wait_recv()
        outs.append(ozr[b].astype(F32))
        logs.append(lzr[b])
    picked = []
    for v in logs:
        row = v[0:1]
        for g in range(1, kv):
            row = jnp.where(my_g == g, v[g : g + 1], row)
        picked.append(row)
    weights = jnp.concatenate(picked, 0)
    weights = jnp.exp(weights - jnp.max(weights, axis=0, keepdims=True))
    wt[...] = as_columns(weights / jnp.sum(weights, axis=0, keepdims=True))
    mine = wt[pl.ds(pl.multiple_of(my_quarter * ROWS, ROWS), ROWS), :]
    attended = sum(mine[:, i : i + 1] * o for i, o in enumerate(outs))
    att[c, z] = attended.astype(BF16)

    def piece_to_core(t):
        return copy(att.at[c, t], att.at[c, t], c4s.at[t], c4r.at[t], c=sib)

    for k in z_far:
        b = other_z(k)
        copy(att.at[c, z], att.at[c, z], z4s.at[b], z4r.at[z], z=b).start()
    piece_to_core(z).start()
    for k in x_near:
        b = other_x(k)
        copy(wobuf.at[b], wobuf.at[b], ws.at[b], wr.at[b], x=b).wait_recv()
    for k in z_near:
        b = other_z(k)
        copy(att.at[c, b], att.at[c, b], z4s.at[b], z4r.at[b], z=b).wait_recv()
        piece_to_core(b).start()
    for t in range(nz):
        copy(att.at[sib, t], att.at[sib, t], c4s.at[t], c4r.at[t], c=sib).wait_recv()

    per_half = heads // 2
    lhs = jnp.concatenate(
        [
            jnp.concatenate([att[cc, per_half * side + j] for j in range(per_half)], 1)
            for side in range(2)
            for cc in range(nc)
        ],
        0,
    )
    low = iota((ROWS, LANES), 1) < HALF
    for k in (*x_far, 0):
        b = other_x(k)
        got = jnp.dot(lhs, wobuf[b], preferred_element_type=F32)
        both = got[0:per_x] + pltpu.roll(got[per_x:], HALF, 1)
        packed = jnp.where(low, both[0:ROWS], pltpu.roll(both[ROWS:], HALF, 1))
        p5s[b] = packed.astype(BF16)
        last = copy(p5s.at[b], p5r.at[y], y5s.at[b], y5r.at[y], x=b, y=x)
        if k:
            last.start()
        else:

            @pl.when(x != y)
            def _():
                last.start()

            @pl.when(x == y)
            def _():
                p5r[y] = p5s[x]

    def arrival(b):
        return copy(p5s.at[y], p5r.at[b], y5s.at[y], y5r.at[b], x=y, y=b)

    for k in range(1, ny):
        arrival(lax.rem(y + k, ny)).wait_recv()

    @pl.when(x != y)
    def _():
        arrival(y).wait_recv()

    final = sum(p5r[b].astype(F32) for b in range(ny))
    out_ref[0:ROWS, :] = final[:, 0:HALF].astype(BF16)
    out_ref[ROWS:, :] = pltpu.roll(final, HALF, 1)[:, 0:HALF].astype(BF16)

    for b in range(nx):
        core1[b].wait_send()
        block_to_core(b).wait_send()
        for one in core3(b):
            one.wait_send()
    for k in range(1, nx):
        b = other_x(k)
        copy(xs.at[b], xr.at[x], x1s.at[b], x1r.at[x], x=b).wait_send()
        copy(wobuf.at[x], wobuf.at[x], ws.at[b], wr.at[x], x=b).wait_send()
        for t in range(nz):
            copy(qbuf.at[c, x, t], qbuf.at[c, x, t], x2s.at[b, t], x2r.at[x, t], x=b).wait_send()
        copy(oxs.at[b], oxr.at[x], x3s.at[b], x3r.at[x], x=b).wait_send()
        copy(lxs.at[b], lxr.at[x], x3ls.at[b], x3lr.at[x], x=b).wait_send()
        copy(p5s.at[b], p5r.at[y], y5s.at[b], y5r.at[y], x=b, y=x).wait_send()
    for k in range(1, nz):
        b = other_z(k)
        copy(zs.at[b], zr.at[z], z1s.at[b], z1r.at[z], z=b).wait_send()
        copy(qbuf.at[c, x, z], qbuf.at[c, x, z], z2s.at[b], z2r.at[z], z=b).wait_send()
        copy(ozs.at[b], ozr.at[z], z3s.at[b], z3r.at[z], z=b).wait_send()
        copy(lzs, lzr.at[z], z3ls.at[b], z3lr.at[z], z=b).wait_send()
        copy(att.at[c, z], att.at[c, z], z4s.at[b], z4r.at[z], z=b).wait_send()
    for t in range(nz):
        piece_to_core(t).wait_send()

    @pl.when(x != y)
    def _():
        copy(p5s.at[x], p5r.at[y], y5s.at[x], y5r.at[y], x=x, y=x).wait_send()


def local(
    sizes, hidden_in, norm_gain, w_query, w_key, w_value, w_out, cache_keys, cache_values, lengths, span_start
):
    nx, nz, nc, ny = sizes
    slots, kv, head_dim = cache_keys.shape
    span, own_cols = hidden_in.shape
    heads = w_query.shape[1] // head_dim
    assert head_dim == LANES and heads == nz and nc == 2 and span == nx * nc * ROWS and nx == ny
    assert w_out.shape[1] == HALF and slots % KEYS == 0 and kv == 2
    cols = w_query.shape[1] + 2 * w_key.shape[1] + LANES
    block = heads * ROWS
    piece = ROWS + 2 * (ROWS * kv // nz) + ROWS
    keys = slots + LANES
    rows = 2 * (heads // kv) * ROWS
    vmem = pl.BlockSpec(memory_space=pltpu.VMEM)
    smem = pl.BlockSpec(memory_space=pltpu.SMEM)
    hbm = pl.BlockSpec(memory_space=pltpu.HBM)
    V = pltpu.VMEM
    dma = pltpu.SemaphoreType.DMA
    scratch = [
        V((slots * kv, LANES), BF16), V((slots * kv, LANES), BF16), V((CHUNK * kv, LANES), F32),
        V((kv, keys, LANES), BF16), V((kv, keys, 2 * LANES), BF16),
        V((2, slots // CHUNK, LANES), F32), V((2, CHUNK, LANES), F32), V((kv, 8, LANES), F32),
        V((nx, ROWS, cols), BF16), V((nx, ROWS, cols), BF16), V((nx, ROWS, cols), F32),
        V((nx, ROWS, cols), BF16), V((nx, ROWS, cols), BF16),
        V((nz, piece, LANES), BF16), V((nz, piece, LANES), BF16), V((ROWS, LANES), F32),
        V((nc, nx, heads, ROWS, LANES), BF16), V((kv, rows, slots), F32),
        V((nx, block, LANES), F32), V((nx, 8, LANES), F32),
        V((nx, block, LANES), BF16), V((nx, block, LANES), BF16), V((nx, 8, LANES), F32), V((nx, 8, LANES), F32),
        V((nx, block, LANES), BF16), V((nx, block, LANES), BF16), V((nx, 8, LANES), F32), V((nx, 8, LANES), F32),
        V((nz, ROWS, LANES), BF16), V((nz, ROWS, LANES), BF16), V((8, LANES), F32), V((nz, 8, LANES), F32),
        V((LANES, LANES), F32),
        V((nc, heads, ROWS, LANES), BF16), V((nx, w_out.shape[0] // 2, LANES), BF16),
        V((nx, ROWS, LANES), BF16), V((ny, ROWS, LANES), BF16),
        dma((2,)),
        dma((nx,)), dma((nx,)), dma((nx,)), dma((nx,)), dma((nz,)), dma((nz,)),
        dma((nz,)), dma((nz,)), dma((nx, nz)), dma((nx, nz)), dma((nx,)), dma((nx,)), dma((nx,)), dma((nx,)),
        dma((nx,)), dma((nx,)), dma((nx,)), dma((nx,)), dma((nx,)), dma((nx,)), dma((nx,)), dma((nx,)),
        dma((nz,)), dma((nz,)), dma((nz,)), dma((nz,)),
        dma((nz,)), dma((nz,)), dma((nz,)), dma((nz,)), dma((nx,)), dma((ny,)),
    ]
    return pl.pallas_call(
        functools.partial(kernel, (nx, nz, nc, ny, nx * nz * nc * own_cols)),
        out_shape=jax.ShapeDtypeStruct((nc * ROWS, HALF), BF16),
        in_specs=[vmem] * 7 + [smem] * 2 + [hbm] * 2,
        out_specs=vmem,
        scratch_shapes=scratch,
        compiler_params=pltpu.CompilerParams(
            collective_id=0, has_side_effects=True, vmem_limit_bytes=60 * 1024 * 1024
        ),
    )(
        hidden_in, norm_gain, w_query, w_key, w_value, w_out, frequencies(), lengths, span_start,
        cache_keys.reshape(slots * kv, LANES), cache_values.reshape(slots * kv, LANES),
    )


def solution(mesh):
    physical = mesh.devices.shape
    ny = mesh.shape["head"]
    nc, nz = 2, 8
    nx = physical[0] // (nc * nz)
    finer = Mesh(mesh.devices.reshape(nx, nz, nc, ny), ("x", "z", "c", "y"))
    seq = ("x", "z", "c")
    return jax.shard_map(
        functools.partial(local, (nx, nz, nc, ny)),
        mesh=finer,
        in_specs=(
            P(None, seq), P(None, seq), P(seq, "y"), P(seq, "y"), P(seq, "y"), P("y", seq),
            P(seq, "y", None), P(seq, "y", None), P(), P(),
        ),
        out_specs=P("y", seq),
        check_vma=False,
    )
```

```python
import functools
import math

import jax
import jax.numpy as jnp
import numpy as np
from jax import lax
from jax.experimental import pallas as pl
from jax.experimental.pallas import tpu as pltpu
from jax.sharding import Mesh
from jax.sharding import PartitionSpec as P

F32 = jnp.float32
BF16 = jnp.bfloat16
MESH = pl.DeviceIdType.MESH
LANES = 128
HALF = 64
ROWS = 32
CHUNK = 128
KEYS = 512

rope_base = 500000.0
stretch = 64.0
initial_context = 8192.0
ramp_low = 1.0
ramp_high = 32.0
epsilon = 1e-05
negative = -1e30
mscale = 0.1 * math.log(stretch) + 1.0


class Phases:
    def __init__(self):
        self.open = None

    def __call__(self, name):
        if self.open is not None:
            self.open.__exit__(None, None, None)
        self.open = None
        if name:
            self.open = jax.named_scope(name)
            self.open.__enter__()


def frequencies():
    base = rope_base ** (-2.0 * np.arange(HALF) / LANES)
    turns = initial_context * base / (2.0 * math.pi)
    share = np.clip((turns - ramp_low) / (ramp_high - ramp_low), 0.0, 1.0)
    freq = (1.0 - share) * base / stretch + share * base
    return np.concatenate([freq, freq])[None, :].astype(np.float32)


def cos_sin(angles):
    turns = jnp.floor(angles * (1.0 / (2.0 * math.pi)) + 0.5)
    first, second = 6.28125, 253.0 / 2.0**17
    third = 2.0 * math.pi - first - second
    rest = angles - turns * first - turns * second - turns * third
    return jnp.cos(rest), jnp.sin(rest)


def iota(shape, dim):
    return lax.broadcasted_iota(jnp.int32, shape, dim)


def signed(sine):
    return jnp.where(iota(sine.shape, 1) < HALF, -sine, sine)


def rotated(vectors, cosine, sine):
    return vectors * cosine + pltpu.roll(vectors, HALF, 1) * sine


def as_columns(rows):
    spare = LANES - rows.shape[0]
    if spare:
        rows = jnp.concatenate([rows, jnp.zeros((spare, LANES), F32)], 0)
    return rows.T


def kernel(
    dims,
    len_ref, start_ref, h_hbm, g_hbm, wq_hbm, wk_hbm, wv_hbm, wo_hbm, freq_hbm, k_hbm, v_hbm,
    out_ref,
    h_ref, g_ref, wq_ref, wk_ref, wv_ref, freq_ref, kraw, vraw, tmp, ks, vs, tab_a, tab_b,
    sb, rb, own, xs, xr, zs, zr, ssc, sscr, ssx, ssxr, ssz, sszr, qbuf, s_ref,
    ob, lb, obs, obr, lss, lsr, oxs, oxr, lxs, lxr, ozs, ozr, lzs, lzr, wt,
    att, wobuf, p5s, p5r,
    in_sem,
    c1s, c1r, x1s, x1r, z1s, z1r, css, csr, xss, xsr, zss, zsr,
    z2s, z2r, x2s, x2r, c2s, c2r, ws, wr, wcs, wcr,
    c3s, c3r, c3ls, c3lr, x3s, x3r, x3ls, x3lr, z3s, z3r, z3ls, z3lr,
    z4s, z4r, y5s, y5r,
):
    nx, nz, nc, ny, d_model = dims
    x, z, c, y = (lax.axis_index(n) for n in ("x", "z", "c", "y"))
    sib = 1 - c
    slots = kraw.shape[0] // 2
    group = wq_ref.shape[1] // wk_ref.shape[1]
    kv = wk_ref.shape[1] // LANES
    heads = kv * group
    quarters = nz // kv
    tail = ROWS // quarters
    qc = heads * LANES
    kc = kv * LANES
    per_x = nc * ROWS
    block = group * ROWS
    depth, span = h_ref.shape
    phase = Phases()

    def copy(src, dst, send, recv, **to):
        return pltpu.make_async_remote_copy(
            src_ref=src, dst_ref=dst, send_sem=send, recv_sem=recv, device_id=to, device_id_type=MESH
        )

    def other_x(k):
        return lax.rem(x + k, nx)

    def other_z(k):
        return lax.rem(z + k, nz)

    x_far = sorted(range(1, nx), key=lambda k: -min(k, nx - k))
    z_far = sorted(range(1, nz), key=lambda k: -min(k, nz - k))
    z_near = z_far[::-1]
    x_near = x_far[::-1]

    phase("entry")
    barrier = pltpu.get_barrier_semaphore()

    def greet(**to):
        pl.semaphore_signal(barrier, inc=1, device_id=to, device_id_type=MESH)

    for k in z_far:
        greet(z=other_z(k))
    for k in range(1, ny):
        for cc in range(nc):
            greet(x=y, y=lax.rem(y + k, ny), c=cc)

    @pl.when(x != y)
    def _():
        for cc in range(nc):
            greet(x=y, c=cc)

    for k in x_far:
        greet(x=other_x(k))
    greet(c=sib)

    fetches = []
    for i, (src, dst) in enumerate(
        (
            (h_hbm, h_ref), (g_hbm, g_ref), (wq_hbm, wq_ref), (wk_hbm, wk_ref), (wv_hbm, wv_ref),
            (freq_hbm, freq_ref), (k_hbm, kraw), (v_hbm, vraw), (wo_hbm, wobuf.at[x, c]),
        )
    ):
        fetches.append(pltpu.make_async_copy(src, dst, in_sem.at[i]))
        fetches[-1].start()
    get_h, get_g, get_wq, get_wk, get_wv, get_freq, get_k, get_v, get_wo = fetches

    my = (x * nz + z) * nc + c
    count = nx * nz * nc

    def add_lengths(r, carry):
        before, total = carry
        return before + jnp.where(r < my, len_ref[r], 0), total + len_ref[r]

    offset, first_pos = lax.fori_loop(0, count, add_lengths, (jnp.int32(0), jnp.int32(0)))
    first_pos = first_pos + start_ref[0]
    live = len_ref[my]

    get_h.wait()
    get_g.wait()
    hidden = h_ref[...].astype(F32)
    squares = jnp.sum(hidden * hidden, axis=0, keepdims=True)
    for r in range(span // LANES):
        ssc[r : r + 1, :] = squares[:, r * LANES : (r + 1) * LANES]
    gain = jnp.concatenate([g_ref[...].astype(F32), jnp.zeros((1, LANES - depth), F32)], 1)
    gain = jnp.broadcast_to(gain, (LANES, LANES)).T[0:depth, 0:1]
    scaled = jnp.concatenate([hidden * gain, jnp.zeros((LANES - depth, span), F32)], 0).T
    get_wq.wait()
    get_wk.wait()
    get_wv.wait()

    def project(cc, store):
        blocks = [
            jnp.where(cc == 0, scaled[b * per_x : b * per_x + ROWS], scaled[b * per_x + ROWS : (b + 1) * per_x])
            for b in range(nx)
        ]
        rows = jnp.concatenate(blocks, 0)[:, 0:depth].astype(BF16)
        for at, w in ((0, wq_ref), (qc, wk_ref), (qc + kc, wv_ref)):
            got = jnp.dot(rows, w[...], preferred_element_type=F32)
            for b in range(nx):
                store(b, at, got[b * ROWS : (b + 1) * ROWS])

    def to_sibling(b, at, value):
        sb[b, :, at : at + value.shape[1]] = value.astype(BF16)

    def to_own(b, at, value):
        own[b, :, at : at + value.shape[1]] = value

    project(sib, to_sibling)

    phase("barrier")
    peers = 1 + (nx - 1) + (nz - 1) + nc * (ny - 1)
    pl.semaphore_wait(barrier, jnp.where(x != y, peers + nc, peers))

    phase("core1_project")
    core1 = [copy(sb.at[b], rb.at[b], c1s.at[b], c1r.at[b], c=sib) for b in range(nx)]
    for b in range(nx):
        core1[b].start()
    sum_c = copy(ssc, sscr, css.at[0], csr.at[0], c=sib)
    sum_c.start()

    project(c, to_own)
    get_freq.wait()
    freq = freq_ref[...]

    phase("core1_wait")
    for b in range(nx):
        core1[b].wait_recv()
    for k in x_far:
        b = other_x(k)
        xs[b] = (own[b] + rb[b].astype(F32)).astype(BF16)
        copy(xs.at[b], xr.at[x], x1s.at[b], x1r.at[x], x=b).start()
    sum_c.wait_recv()
    ssx[...] = ssc[...] + sscr[...]
    for k in x_far:
        b = other_x(k)
        copy(ssx, ssxr.at[x], xss.at[b], xsr.at[x], x=b).start()

    phase("keys")
    a_count = slots // CHUNK
    a_pos = (offset + CHUNK * iota((a_count, LANES), 0)).astype(F32)
    a_cos, a_sin = cos_sin(a_pos * freq)
    tab_a[0] = a_cos * mscale
    tab_a[1] = a_sin * mscale
    b_cos, b_sin = cos_sin(iota((CHUNK, LANES), 0).astype(F32) * freq)
    tab_b[0] = b_cos
    tab_b[1] = b_sin
    first_token = x * per_x + c * ROWS
    my_g, my_quarter = lax.div(z, quarters), lax.rem(z, quarters)
    k_first = first_token + my_quarter * tail
    q_pos = (first_pos + first_token + iota((ROWS, LANES), 0)).astype(F32)
    q_cos, q_sin = cos_sin(q_pos * freq)
    k_pos = (first_pos + k_first + iota((tail, LANES), 0)).astype(F32)
    k_cos, k_sin = cos_sin(k_pos * freq)
    q_cos, q_sin = q_cos * mscale, signed(q_sin * mscale)
    k_cos, k_sin = k_cos * mscale, signed(k_sin * mscale)

    get_k.wait()

    def slot_angles(a, size):
        cos_a = tab_a[0, pl.ds(a, 1), :]
        sin_a = tab_a[1, pl.ds(a, 1), :]
        cos_b, sin_b = tab_b[0, 0:size, :], tab_b[1, 0:size, :]
        return cos_a * cos_b - sin_a * sin_b, signed(sin_a * cos_b + cos_a * sin_b)

    tmp[0, 0 : 8 * kv, :] = kraw[0 : 8 * kv, :].astype(F32)
    slot_cos, slot_sin = slot_angles(0, 8)
    head_keys = [
        rotated(tmp[0, pl.ds(g, 8, stride=kv), :], slot_cos, slot_sin)[0:1] for g in range(kv)
    ]

    def rotate_chunks(j, _):
        for u in range(2):
            a = 2 * j + u
            at = pl.multiple_of(a * CHUNK, CHUNK)
            tmp[u] = kraw[pl.ds(pl.multiple_of(2 * at, 2 * CHUNK), 2 * CHUNK), :].astype(F32)
            cosine, sine = slot_angles(a, CHUNK)
            alive = at + iota((CHUNK, LANES), 0) < live
            for g in range(kv):
                keys = rotated(tmp[u, pl.ds(g, CHUNK, stride=kv), :], cosine, sine)
                ks[g, pl.ds(at, CHUNK), :] = jnp.where(alive, keys, head_keys[g]).astype(BF16)
        return 0

    steps = a_count // 2
    early = steps * 3 // 4
    lax.fori_loop(0, early, rotate_chunks, 0)

    phase("x1_wait")
    gathered = own[x] + rb[x].astype(F32)
    for k in x_near:
        b = other_x(k)
        copy(xs.at[b], xr.at[b], x1s.at[b], x1r.at[b], x=b).wait_recv()
        gathered = gathered + xr[b].astype(F32)
    for t in range(nz):
        g, quarter = t // quarters, t % quarters
        zs[t, 0:ROWS, :] = gathered[:, t * LANES : (t + 1) * LANES].astype(BF16)
        pair = [
            gathered[quarter * tail : (quarter + 1) * tail, at + g * LANES : at + (g + 1) * LANES]
            for at in (qc, qc + kc)
        ]
        zs[t, ROWS : ROWS + 2 * tail, :] = jnp.concatenate(pair, 0).astype(BF16)
    for k in z_far:
        b = other_z(k)
        copy(zs.at[b], zr.at[z], z1s.at[b], z1r.at[z], z=b).start()
    squares = ssx[...]
    for k in x_near:
        b = other_x(k)
        copy(ssx, ssxr.at[b], xss.at[b], xsr.at[b], x=b).wait_recv()
        squares = squares + ssxr[b]
    ssz[...] = squares
    for k in z_far:
        b = other_z(k)
        copy(ssz, sszr.at[z], zss.at[b], zsr.at[z], z=b).start()

    phase("values")
    lax.fori_loop(early, steps, rotate_chunks, 0)
    get_v.wait()

    def value_chunks(j, _):
        for u in range(2):
            at = pl.multiple_of((2 * j + u) * CHUNK, CHUNK)
            tmp[u] = vraw[pl.ds(pl.multiple_of(2 * at, 2 * CHUNK), 2 * CHUNK), :].astype(F32)
            alive = at + iota((CHUNK, LANES), 0) < live
            ones = jnp.where(alive, 1.0, 0.0).astype(BF16)
            for g in range(kv):
                values = jnp.where(alive, tmp[u, pl.ds(g, CHUNK, stride=kv), :], 0.0)
                vs[g, pl.ds(at, CHUNK), 0:LANES] = values.astype(BF16)
                vs[g, pl.ds(at, CHUNK), LANES:] = ones
        return 0

    lax.fori_loop(0, steps, value_chunks, 0)
    get_wo.wait()

    phase("z1_wait")
    total = zs[z].astype(F32)
    for k in z_near:
        b = other_z(k)
        copy(zs.at[b], zr.at[b], z1s.at[b], z1r.at[b], z=b).wait_recv()
        total = total + zr[b].astype(F32)
    for k in z_near:
        b = other_z(k)
        copy(ssz, sszr.at[b], zss.at[b], zsr.at[b], z=b).wait_recv()
        squares = squares + sszr[b]
    wt[...] = as_columns(lax.rsqrt(squares * (1.0 / d_model) + epsilon))
    which = lax.div(first_token, LANES)
    lane = lax.rem(first_token, LANES)

    def inverse_of(at, size):
        cols = wt[pl.ds(pl.multiple_of(at, 8), size), :]
        picked = cols[:, 0:1]
        for r in range(1, span // LANES):
            picked = jnp.where(which == r, cols[:, r : r + 1], picked)
        return picked

    query = rotated(total[0:ROWS] * inverse_of(lane, ROWS), q_cos, q_sin) * LANES**-0.5
    qbuf[c, x, z] = query.astype(BF16)

    for k in z_far:
        b = other_z(k)
        copy(qbuf.at[c, x, z], qbuf.at[c, x, z], z2s.at[b], z2r.at[z], z=b).start()

    def piece_to_x(t):
        for k in x_far:
            b = other_x(k)
            copy(qbuf.at[c, x, t], qbuf.at[c, x, t], x2s.at[b, t], x2r.at[x, t], x=b).start()

    piece_to_x(z)

    phase("new_keys")
    inv_new = inverse_of(lane + my_quarter * tail, tail)
    new_k = (total[ROWS : ROWS + tail] * inv_new).astype(BF16).astype(F32)
    new_k = rotated(new_k, k_cos, k_sin)
    new_v = total[ROWS + tail : ROWS + 2 * tail] * inv_new
    empty = jnp.zeros((LANES - tail, LANES), F32)
    new_k = jnp.concatenate([new_k, empty], 0).astype(BF16)
    new_v = jnp.concatenate([new_v, empty], 0).astype(BF16)
    new_ones = jnp.where(iota((LANES, LANES), 0) < tail, 1.0, 0.0).astype(BF16)
    for g in range(kv):
        ks[g, slots:, :] = new_k
        vs[g, slots:, 0:LANES] = new_v
        vs[g, slots:, LANES:] = new_ones

    phase("z2_wait")
    for k in z_near:
        b = other_z(k)
        copy(qbuf.at[c, x, b], qbuf.at[c, x, b], z2s.at[b], z2r.at[b], z=b).wait_recv()
        piece_to_x(b)

    phase("x2_wait")

    def block_to_core(b):
        return copy(qbuf.at[c, b], qbuf.at[c, b], c2s.at[b], c2r.at[b], c=sib)

    block_to_core(x).start()
    for k in x_near:
        b = other_x(k)
        for t in range(nz):
            copy(qbuf.at[c, b, t], qbuf.at[c, b, t], x2s.at[b, t], x2r.at[b, t], x=b).wait_recv()
        block_to_core(b).start()
    for k in x_far:
        b = other_x(k)
        copy(wobuf.at[x, c], wobuf.at[x, c], ws.at[b], wr.at[x], x=b).start()

    def weights_to_core(b):
        return copy(wobuf.at[b, c], wobuf.at[b, c], wcs.at[b], wcr.at[b], c=sib)

    weights_to_core(x).start()

    rows = 2 * block
    apart = nx // 2
    pairs = [(i, i + apart) for i in range(apart)]

    def attend(cc, pair):
        blocks = [other_x(k) for k in pair]
        row = iota((rows, LANES), 0)
        token = jnp.where(row < block, blocks[0], blocks[1]) * per_x + cc * ROWS + lax.rem(row, ROWS)
        lane = iota((rows, LANES), 1)
        seen = jnp.logical_and(lane < tail, k_first + lane <= token)
        for g in range(kv):
            q = jnp.concatenate(
                [qbuf[cc, b, g * group : (g + 1) * group].reshape(block, LANES) for b in blocks], 0
            )
            most = jnp.full((rows, LANES), negative, F32)
            for at in range(0, slots, KEYS):
                score = lax.dot_general(
                    q, ks[g, at : at + KEYS, :], (((1,), (1,)), ((), ())), preferred_element_type=F32
                )
                s_ref[g, :, at : at + KEYS] = score
                for lo in range(0, KEYS, LANES):
                    most = jnp.maximum(most, score[:, lo : lo + LANES])
            score = lax.dot_general(
                q, ks[g, slots:, :], (((1,), (1,)), ((), ())), preferred_element_type=F32
            )
            score = jnp.where(jnp.logical_and(seen, my_g == g), score, negative)
            most = jnp.max(jnp.maximum(most, score), axis=1, keepdims=True)
            acc = jnp.dot(
                jnp.exp(score - most).astype(BF16), vs[g, slots:, :], preferred_element_type=F32
            )
            for at in range(0, slots, KEYS):
                prob = jnp.exp(s_ref[g, :, at : at + KEYS] - most).astype(BF16)
                acc = acc + jnp.dot(prob, vs[g, at : at + KEYS, :], preferred_element_type=F32)
            sums = acc[:, LANES:]
            result = acc[:, 0:LANES] / sums
            lse = most + jnp.log(sums)
            for j, b in enumerate(blocks):
                cut = slice(j * block, (j + 1) * block)
                yield b, g, result[cut], lse[cut].T[0:1]

    def core3(b):
        return (
            copy(obs.at[b], obr.at[b], c3s.at[b], c3r.at[b], c=sib),
            copy(lss.at[b], lsr.at[b], c3ls.at[b], c3lr.at[b], c=sib),
        )

    def combine(outs, logs):
        top = functools.reduce(jnp.maximum, logs)
        weights = [jnp.exp(v - top) for v in logs]
        whole = sum(weights)
        spare = jnp.zeros((8 - kv, LANES), F32)
        columns = as_columns(
            jnp.concatenate([jnp.concatenate([w / whole, spare], 0) for w in weights], 0)
        )
        parts = []
        for g in range(kv):
            cut = slice(g * block, (g + 1) * block)
            parts.append(sum(columns[:, 8 * i + g : 8 * i + g + 1] * o[cut] for i, o in enumerate(outs)))
        return jnp.concatenate(parts, 0), top + jnp.log(whole)

    def own_unit(pair):
        for b, g, result, lse in attend(c, pair):
            ob[b, g * block : (g + 1) * block, :] = result
            lb[b, g : g + 1, :] = lse

    def sibling_unit(pair):
        for b, g, result, lse in attend(sib, pair):
            obs[b, g * block : (g + 1) * block, :] = result.astype(BF16)
            lss[b, g : g + 1, :] = lse
        for k in pair:
            for one in core3(other_x(k)):
                one.start()

    def join_cores(pair):
        for k in pair:
            b = other_x(k)
            for one in core3(b):
                one.wait_recv()
            out, lse = combine([ob[b], obr[b].astype(F32)], [lb[b], lsr[b]])
            if k:
                oxs[b] = out.astype(BF16)
                lxs[b] = lse
                copy(oxs.at[b], oxr.at[x], x3s.at[b], x3r.at[x], x=b).start()
                copy(lxs.at[b], lxr.at[x], x3ls.at[b], x3lr.at[x], x=b).start()
            else:
                ob[b] = out
                lb[b] = lse

    phase("unit_0")
    own_unit(pairs[0])
    phase("c2_wait")
    for k in range(nx):
        b = other_x(k)
        copy(qbuf.at[sib, b], qbuf.at[sib, b], c2s.at[b], c2r.at[b], c=sib).wait_recv()
    for i, pair in enumerate(pairs):
        phase("unit_1")
        sibling_unit(pair)
        if i == 0:
            phase("weights")
            for k in x_near:
                b = other_x(k)
                copy(wobuf.at[b, c], wobuf.at[b, c], ws.at[b], wr.at[b], x=b).wait_recv()
                weights_to_core(b).start()
    phase("join")
    join_cores(pairs[0])
    for pair in pairs[1:]:
        phase("unit_2")
        own_unit(pair)
        phase("join_2")
        join_cores(pair)

    phase("x3_wait")
    outs, logs = [ob[x]], [lb[x]]
    for k in x_far:
        b = other_x(k)
        copy(oxs.at[b], oxr.at[b], x3s.at[b], x3r.at[b], x=b).wait_recv()
        copy(lxs.at[b], lxr.at[b], x3ls.at[b], x3lr.at[b], x=b).wait_recv()
        outs.append(oxr[b].astype(F32))
        logs.append(lxr[b])
    out, lse = combine(outs, logs)
    ozs[...] = out.astype(BF16).reshape(nz, ROWS, LANES)
    lzs[...] = lse
    for k in z_far:
        b = other_z(k)
        copy(ozs.at[b], ozr.at[z], z3s.at[b], z3r.at[z], z=b).start()
        copy(lzs, lzr.at[z], z3ls.at[b], z3lr.at[z], z=b).start()

    phase("z3_wait")
    outs, logs = [ozs[z].astype(F32)], [lzs[...]]
    for k in z_near:
        b = other_z(k)
        copy(ozs.at[b], ozr.at[b], z3s.at[b], z3r.at[b], z=b).wait_recv()
        copy(lzs, lzr.at[b], z3ls.at[b], z3lr.at[b], z=b).wait_recv()
        outs.append(ozr[b].astype(F32))
        logs.append(lzr[b])
    picked = []
    for v in logs:
        row = v[0:1]
        for g in range(1, kv):
            row = jnp.where(my_g == g, v[g : g + 1], row)
        picked.append(row)
    weights = jnp.concatenate(picked, 0)
    weights = jnp.exp(weights - jnp.max(weights, axis=0, keepdims=True))
    wt[...] = as_columns(weights / jnp.sum(weights, axis=0, keepdims=True))
    mine = wt[pl.ds(pl.multiple_of(my_quarter * ROWS, ROWS), ROWS), :]
    attended = sum(mine[:, i : i + 1] * o for i, o in enumerate(outs))
    att[z] = attended.astype(BF16)

    for k in z_far:
        b = other_z(k)
        copy(att.at[z], att.at[z], z4s.at[b], z4r.at[z], z=b).start()

    phase("z4_wait")
    for k in range(1, nx):
        b = other_x(k)
        copy(wobuf.at[b, sib], wobuf.at[b, sib], wcs.at[b], wcr.at[b], c=sib).wait_recv()
    copy(wobuf.at[x, sib], wobuf.at[x, sib], wcs.at[x], wcr.at[x], c=sib).wait_recv()
    for k in z_near:
        b = other_z(k)
        copy(att.at[b], att.at[b], z4s.at[b], z4r.at[b], z=b).wait_recv()

    phase("w_out")
    lhs = jnp.concatenate([att[t] for t in range(heads)], 1)
    rhs = wobuf[...].reshape(nx * nc * HALF, heads * LANES)
    got = lax.dot_general(lhs, rhs, (((1,), (1,)), ((), ())), preferred_element_type=F32)
    deep = ROWS // 2
    low = iota((deep, LANES), 1) < HALF
    for b in range(nx):
        both = got[:, b * LANES : (b + 1) * LANES]
        turned = pltpu.roll(both, HALF, 1)
        p5s[b, 0] = jnp.where(low, both[0:deep], turned[deep:]).astype(BF16)
        p5s[b, 1] = jnp.where(low, turned[0:deep], both[deep:]).astype(BF16)

    def last(b, cc):
        return copy(p5s.at[b, cc], p5r.at[c, y], y5s.at[b, cc], y5r.at[c, y], x=b, c=cc, y=x)

    for k in x_far:
        for cc in range(nc):
            last(other_x(k), cc).start()
    last(x, sib).start()

    @pl.when(x != y)
    def _():
        last(x, c).start()

    @pl.when(x == y)
    def _():
        p5r[c, y] = p5s[x, c]

    phase("y5_wait")

    def arrival(cc, b):
        return copy(p5s.at[y, cc], p5r.at[cc, b], y5s.at[y, cc], y5r.at[cc, b], x=y, c=cc, y=b)

    for k in range(1, ny):
        for cc in range(nc):
            arrival(cc, lax.rem(y + k, ny)).wait_recv()
    arrival(sib, y).wait_recv()

    @pl.when(x != y)
    def _():
        arrival(c, y).wait_recv()

    for cc in range(nc):
        final = sum(p5r[cc, b].astype(F32) for b in range(ny))
        at = cc * ROWS
        out_ref[at : at + deep, :] = final[:, 0:HALF].astype(BF16)
        out_ref[at + deep : at + ROWS, :] = pltpu.roll(final, HALF, 1)[:, 0:HALF].astype(BF16)

    phase("drain")
    sum_c.wait_send()
    for b in range(nx):
        core1[b].wait_send()
        block_to_core(b).wait_send()
        weights_to_core(b).wait_send()
        for one in core3(b):
            one.wait_send()
    for k in range(1, nx):
        b = other_x(k)
        copy(xs.at[b], xr.at[x], x1s.at[b], x1r.at[x], x=b).wait_send()
        copy(ssx, ssxr.at[x], xss.at[b], xsr.at[x], x=b).wait_send()
        copy(wobuf.at[x, c], wobuf.at[x, c], ws.at[b], wr.at[x], x=b).wait_send()
        for t in range(nz):
            copy(qbuf.at[c, x, t], qbuf.at[c, x, t], x2s.at[b, t], x2r.at[x, t], x=b).wait_send()
        copy(oxs.at[b], oxr.at[x], x3s.at[b], x3r.at[x], x=b).wait_send()
        copy(lxs.at[b], lxr.at[x], x3ls.at[b], x3lr.at[x], x=b).wait_send()
        for cc in range(nc):
            last(b, cc).wait_send()
    for k in range(1, nz):
        b = other_z(k)
        copy(zs.at[b], zr.at[z], z1s.at[b], z1r.at[z], z=b).wait_send()
        copy(ssz, sszr.at[z], zss.at[b], zsr.at[z], z=b).wait_send()
        copy(qbuf.at[c, x, z], qbuf.at[c, x, z], z2s.at[b], z2r.at[z], z=b).wait_send()
        copy(ozs.at[b], ozr.at[z], z3s.at[b], z3r.at[z], z=b).wait_send()
        copy(lzs, lzr.at[z], z3ls.at[b], z3lr.at[z], z=b).wait_send()
        copy(att.at[z], att.at[z], z4s.at[b], z4r.at[z], z=b).wait_send()
    last(x, sib).wait_send()

    @pl.when(x != y)
    def _():
        last(x, c).wait_send()

    phase(None)


def local(
    sizes, hidden_in, norm_gain, w_query, w_key, w_value, w_out, cache_keys, cache_values, lengths, span_start
):
    nx, nz, nc, ny = sizes
    slots, kv, head_dim = cache_keys.shape
    span, depth = hidden_in.shape
    heads = w_query.shape[1] // head_dim
    assert head_dim == LANES and heads == nz and nc == 2 and span == nx * nc * ROWS and nx == ny
    assert w_out.shape[1] == HALF and slots % KEYS == 0 and kv == 2
    cols = w_query.shape[1] + 2 * w_key.shape[1]
    block = heads * ROWS
    piece = ROWS + 2 * (ROWS * kv // nz)
    keys = slots + LANES
    rows = 2 * (heads // kv) * ROWS
    lines = span // LANES
    smem = pl.BlockSpec(memory_space=pltpu.SMEM)
    hbm = pl.BlockSpec(memory_space=pltpu.HBM)
    V = pltpu.VMEM
    dma = pltpu.SemaphoreType.DMA
    scratch = [
        V((depth, span), BF16), V((1, depth), BF16), V(w_query.shape, BF16), V(w_key.shape, BF16),
        V(w_value.shape, BF16), V((1, LANES), F32),
        V((slots * kv, LANES), BF16), V((slots * kv, LANES), BF16), V((2, CHUNK * kv, LANES), F32),
        V((kv, keys, LANES), BF16), V((kv, keys, 2 * LANES), BF16),
        V((2, slots // CHUNK, LANES), F32), V((2, CHUNK, LANES), F32),
        V((nx, ROWS, cols), BF16), V((nx, ROWS, cols), BF16), V((nx, ROWS, cols), F32),
        V((nx, ROWS, cols), BF16), V((nx, ROWS, cols), BF16),
        V((nz, piece, LANES), BF16), V((nz, piece, LANES), BF16),
        V((lines, LANES), F32), V((lines, LANES), F32), V((lines, LANES), F32), V((nx, lines, LANES), F32),
        V((lines, LANES), F32), V((nz, lines, LANES), F32),
        V((nc, nx, heads, ROWS, LANES), BF16), V((kv, rows, slots), F32),
        V((nx, block, LANES), F32), V((nx, kv, LANES), F32),
        V((nx, block, LANES), BF16), V((nx, block, LANES), BF16), V((nx, kv, LANES), F32), V((nx, kv, LANES), F32),
        V((nx, block, LANES), BF16), V((nx, block, LANES), BF16), V((nx, kv, LANES), F32), V((nx, kv, LANES), F32),
        V((nz, ROWS, LANES), BF16), V((nz, ROWS, LANES), BF16), V((kv, LANES), F32), V((nz, kv, LANES), F32),
        V((LANES, LANES), F32),
        V((heads, ROWS, LANES), BF16), V((nx, nc, HALF, w_out.shape[0]), BF16),
        V((nx, nc, ROWS // 2, LANES), BF16), V((nc, ny, ROWS // 2, LANES), BF16),
        dma((9,)),
        dma((nx,)), dma((nx,)), dma((nx,)), dma((nx,)), dma((nz,)), dma((nz,)),
        dma((1,)), dma((1,)), dma((nx,)), dma((nx,)), dma((nz,)), dma((nz,)),
        dma((nz,)), dma((nz,)), dma((nx, nz)), dma((nx, nz)), dma((nx,)), dma((nx,)),
        dma((nx,)), dma((nx,)), dma((nx,)), dma((nx,)),
        dma((nx,)), dma((nx,)), dma((nx,)), dma((nx,)), dma((nx,)), dma((nx,)), dma((nx,)), dma((nx,)),
        dma((nz,)), dma((nz,)), dma((nz,)), dma((nz,)),
        dma((nz,)), dma((nz,)), dma((nx, nc)), dma((nc, ny)),
    ]
    return pl.pallas_call(
        functools.partial(kernel, (nx, nz, nc, ny, nx * nz * nc * depth)),
        out_shape=jax.ShapeDtypeStruct((nc * ROWS, HALF), BF16),
        in_specs=[smem] * 2 + [hbm] * 9,
        out_specs=pl.BlockSpec(memory_space=pltpu.VMEM),
        scratch_shapes=scratch,
        compiler_params=pltpu.CompilerParams(
            collective_id=0, has_side_effects=True, vmem_limit_bytes=60 * 1024 * 1024
        ),
    )(
        lengths, span_start, hidden_in.T, norm_gain, w_query, w_key, w_value, w_out.T, frequencies(),
        cache_keys.reshape(slots * kv, LANES), cache_values.reshape(slots * kv, LANES),
    )


def solution(mesh):
    physical = mesh.devices.shape
    ny = mesh.shape["head"]
    nc, nz = 2, 8
    nx = physical[0] // (nc * nz)
    finer = Mesh(mesh.devices.reshape(nx, nz, nc, ny), ("x", "z", "c", "y"))
    seq = ("x", "z", "c")
    return jax.shard_map(
        functools.partial(local, (nx, nz, nc, ny)),
        mesh=finer,
        in_specs=(
            P(None, seq), P(None, seq), P(seq, "y"), P(seq, "y"), P(seq, "y"), P("y", seq),
            P(seq, "y", None), P(seq, "y", None), P(), P(),
        ),
        out_specs=P("y", seq),
        check_vma=False,
    )
```

```python
import functools
import math

import jax
import jax.numpy as jnp
import numpy as np
from jax import lax
from jax.experimental import pallas as pl
from jax.experimental.pallas import tpu as pltpu
from jax.sharding import Mesh
from jax.sharding import PartitionSpec as P

F32 = jnp.float32
BF16 = jnp.bfloat16
MESH = pl.DeviceIdType.MESH
LANES = 128
HALF = 64
ROWS = 32
CHUNK = 128
KEYS = 512

rope_base = 500000.0
stretch = 64.0
initial_context = 8192.0
ramp_low = 1.0
ramp_high = 32.0
epsilon = 1e-05
negative = -1e30
mscale = 0.1 * math.log(stretch) + 1.0


class Phases:
    def __init__(self):
        self.open = None

    def __call__(self, name):
        if self.open is not None:
            self.open.__exit__(None, None, None)
        self.open = None
        if name:
            self.open = jax.named_scope(name)
            self.open.__enter__()


def frequencies():
    base = rope_base ** (-2.0 * np.arange(HALF) / LANES)
    turns = initial_context * base / (2.0 * math.pi)
    share = np.clip((turns - ramp_low) / (ramp_high - ramp_low), 0.0, 1.0)
    freq = (1.0 - share) * base / stretch + share * base
    return np.concatenate([freq, freq])[None, :].astype(np.float32)


def cos_sin(angles):
    turns = jnp.floor(angles * (1.0 / (2.0 * math.pi)) + 0.5)
    first, second = 6.28125, 253.0 / 2.0**17
    third = 2.0 * math.pi - first - second
    rest = angles - turns * first - turns * second - turns * third
    return jnp.cos(rest), jnp.sin(rest)


def iota(shape, dim):
    return lax.broadcasted_iota(jnp.int32, shape, dim)


def signed(sine):
    return jnp.where(iota(sine.shape, 1) < HALF, -sine, sine)


def rotated(vectors, cosine, sine):
    return vectors * cosine + pltpu.roll(vectors, HALF, 1) * sine


def as_columns(rows):
    spare = LANES - rows.shape[0]
    if spare:
        rows = jnp.concatenate([rows, jnp.zeros((spare, LANES), F32)], 0)
    return rows.T


def kernel(
    dims,
    len_hbm, start_hbm, h_hbm, g_hbm, wq_hbm, wk_hbm, wv_hbm, wo_hbm, freq_hbm, k_hbm, v_hbm,
    out_ref,
    len_ref, start_ref,
    h_ref, g_ref, wq_ref, wk_ref, wv_ref, freq_ref, kraw, vraw, tmp, ks, vs, tab_a, tab_b,
    sb, rb, own, xs, xr, zs, zr, sb2, rb2, own2, xs2, xr2, zs2, zr2,
    ssc, sscr, ssx, ssxr, ssz, sszr, qbuf, s_ref,
    ob, lb, obs, obr, lss, lsr, oxs, oxr, lxs, lxr, wt,
    att, wobuf, p5s, p5r,
    in_sem,
    c1s, c1r, x1s, x1r, z1s, z1r, d1s, d1r, w1s, w1r, v1s, v1r, css, csr, xss, xsr, zss, zsr,
    z2s, z2r, x2s, x2r, c2s, c2r, ws, wr, wcs, wcr,
    c3s, c3r, c3ls, c3lr, x3s, x3r, x3ls, x3lr,
    z4s, z4r, y5s, y5r,
):
    nx, nz, nc, ny, d_model = dims
    x, z, c, y = (lax.axis_index(n) for n in ("x", "z", "c", "y"))
    sib = 1 - c
    slots = kraw.shape[0] // 2
    group = wq_ref.shape[1] // wk_ref.shape[1]
    kv = wk_ref.shape[1] // LANES
    heads = kv * group
    quarters = nz // kv
    tail = ROWS // quarters
    qc = heads * LANES
    kc = kv * LANES
    per_x = nc * ROWS
    block = group * ROWS
    depth, span = h_ref.shape
    phase = Phases()

    def copy(src, dst, send, recv, **to):
        return pltpu.make_async_remote_copy(
            src_ref=src, dst_ref=dst, send_sem=send, recv_sem=recv, device_id=to, device_id_type=MESH
        )

    def other_x(k):
        return lax.rem(x + k, nx)

    def other_z(k):
        return lax.rem(z + k, nz)

    x_far = sorted(range(1, nx), key=lambda k: -min(k, nx - k))
    z_far = sorted(range(1, nz), key=lambda k: -min(k, nz - k))
    z_near = z_far[::-1]
    x_near = x_far[::-1]

    phase("entry")
    barrier = pltpu.get_barrier_semaphore()

    def greet(**to):
        pl.semaphore_signal(barrier, inc=1, device_id=to, device_id_type=MESH)

    for k in z_far:
        greet(z=other_z(k))
    for k in range(1, ny):
        for cc in range(nc):
            greet(x=y, y=lax.rem(y + k, ny), c=cc)

    @pl.when(x != y)
    def _():
        for cc in range(nc):
            greet(x=y, c=cc)

    for k in x_far:
        greet(x=other_x(k))
    greet(c=sib)

    fetches = []
    for i, (src, dst) in enumerate(
        (
            (h_hbm, h_ref), (g_hbm, g_ref), (wq_hbm, wq_ref), (wk_hbm, wk_ref), (wv_hbm, wv_ref),
            (freq_hbm, freq_ref), (len_hbm, len_ref), (start_hbm, start_ref),
            (k_hbm, kraw), (v_hbm, vraw), (wo_hbm, wobuf.at[x, c]),
        )
    ):
        fetches.append(pltpu.make_async_copy(src, dst, in_sem.at[i]))
        fetches[-1].start()
    get_h, get_g, get_wq, get_wk, get_wv, get_freq, get_len, get_start, get_k, get_v, get_wo = fetches

    get_h.wait()
    get_g.wait()
    hidden = h_ref[...].astype(F32)
    squares = jnp.sum(hidden * hidden, axis=0, keepdims=True)
    for r in range(span // LANES):
        ssc[r : r + 1, :] = squares[:, r * LANES : (r + 1) * LANES]
    gain = jnp.concatenate([g_ref[...].astype(F32), jnp.zeros((1, LANES - depth), F32)], 1)
    gain = jnp.broadcast_to(gain, (LANES, LANES)).T[0:depth, 0:1]
    scaled = jnp.concatenate([hidden * gain, jnp.zeros((LANES - depth, span), F32)], 0).T
    get_wq.wait()
    get_wk.wait()
    get_wv.wait()

    def rows_of(cc):
        blocks = [
            jnp.where(cc == 0, scaled[b * per_x : b * per_x + ROWS], scaled[b * per_x + ROWS : (b + 1) * per_x])
            for b in range(nx)
        ]
        return jnp.concatenate(blocks, 0)[:, 0:depth].astype(BF16)

    def project(rows, weights, to):
        at = 0
        for w in weights:
            got = jnp.dot(rows, w[...], preferred_element_type=F32)
            for b in range(nx):
                to[b, :, at : at + got.shape[1]] = got[b * ROWS : (b + 1) * ROWS].astype(to.dtype)
            at += got.shape[1]

    project(rows_of(sib), (wq_ref,), sb)
    project(rows_of(sib), (wk_ref, wv_ref), sb2)

    phase("barrier")
    peers = 1 + (nx - 1) + (nz - 1) + nc * (ny - 1)
    pl.semaphore_wait(barrier, jnp.where(x != y, peers + nc, peers))

    phase("core1_project")
    core1 = [copy(sb.at[b], rb.at[b], c1s.at[b], c1r.at[b], c=sib) for b in range(nx)]
    core2 = [copy(sb2.at[b], rb2.at[b], d1s.at[b], d1r.at[b], c=sib) for b in range(nx)]
    sum_c = copy(ssc, sscr, css.at[0], csr.at[0], c=sib)
    for one in (*core1, sum_c, *core2):
        one.start()

    project(rows_of(c), (wq_ref,), own)
    project(rows_of(c), (wk_ref, wv_ref), own2)
    get_freq.wait()
    freq = freq_ref[...]

    phase("core1_wait")
    for b in range(nx):
        core1[b].wait_recv()
    for k in x_far:
        b = other_x(k)
        xs[b] = (own[b] + rb[b].astype(F32)).astype(BF16)
        copy(xs.at[b], xr.at[x], x1s.at[b], x1r.at[x], x=b).start()
    sum_c.wait_recv()
    ssx[...] = ssc[...] + sscr[...]
    for k in x_far:
        b = other_x(k)
        copy(ssx, ssxr.at[x], xss.at[b], xsr.at[x], x=b).start()

    phase("keys")
    get_len.wait()
    get_start.wait()
    my = (x * nz + z) * nc + c
    count = nx * nz * nc

    def add_lengths(r, carry):
        before, total = carry
        return before + jnp.where(r < my, len_ref[r], 0), total + len_ref[r]

    offset, first_pos = lax.fori_loop(0, count, add_lengths, (jnp.int32(0), jnp.int32(0)))
    first_pos = first_pos + start_ref[0]
    live = len_ref[my]

    a_count = slots // CHUNK
    a_pos = (offset + CHUNK * iota((a_count, LANES), 0)).astype(F32)
    a_cos, a_sin = cos_sin(a_pos * freq)
    tab_a[0] = a_cos * mscale
    tab_a[1] = a_sin * mscale
    b_cos, b_sin = cos_sin(iota((CHUNK, LANES), 0).astype(F32) * freq)
    tab_b[0] = b_cos
    tab_b[1] = b_sin
    first_token = x * per_x + c * ROWS
    my_g, my_quarter = lax.div(z, quarters), lax.rem(z, quarters)
    k_first = first_token + my_quarter * tail
    q_pos = (first_pos + first_token + iota((ROWS, LANES), 0)).astype(F32)
    q_cos, q_sin = cos_sin(q_pos * freq)
    k_pos = (first_pos + k_first + iota((tail, LANES), 0)).astype(F32)
    k_cos, k_sin = cos_sin(k_pos * freq)
    q_cos, q_sin = q_cos * mscale, signed(q_sin * mscale)
    k_cos, k_sin = k_cos * mscale, signed(k_sin * mscale)

    get_k.wait()

    def slot_angles(a, size):
        cos_a = tab_a[0, pl.ds(a, 1), :]
        sin_a = tab_a[1, pl.ds(a, 1), :]
        cos_b, sin_b = tab_b[0, 0:size, :], tab_b[1, 0:size, :]
        return cos_a * cos_b - sin_a * sin_b, signed(sin_a * cos_b + cos_a * sin_b)

    tmp[0, 0 : 8 * kv, :] = kraw[0 : 8 * kv, :].astype(F32)
    slot_cos, slot_sin = slot_angles(0, 8)
    head_keys = [
        rotated(tmp[0, pl.ds(g, 8, stride=kv), :], slot_cos, slot_sin)[0:1] for g in range(kv)
    ]

    def rotate_chunks(j, _):
        for u in range(2):
            a = 2 * j + u
            at = pl.multiple_of(a * CHUNK, CHUNK)
            tmp[u] = kraw[pl.ds(pl.multiple_of(2 * at, 2 * CHUNK), 2 * CHUNK), :].astype(F32)
            cosine, sine = slot_angles(a, CHUNK)
            alive = at + iota((CHUNK, LANES), 0) < live
            for g in range(kv):
                keys = rotated(tmp[u, pl.ds(g, CHUNK, stride=kv), :], cosine, sine)
                ks[g, pl.ds(at, CHUNK), :] = jnp.where(alive, keys, head_keys[g]).astype(BF16)
        return 0

    steps = a_count // 2
    early = steps * 3 // 4
    lax.fori_loop(0, early, rotate_chunks, 0)

    phase("x1_wait")
    gathered = own[x] + rb[x].astype(F32)
    for k in x_near:
        b = other_x(k)
        copy(xs.at[b], xr.at[b], x1s.at[b], x1r.at[b], x=b).wait_recv()
        gathered = gathered + xr[b].astype(F32)
    for t in range(nz):
        zs[t] = gathered[:, t * LANES : (t + 1) * LANES].astype(BF16)
    for k in z_far:
        b = other_z(k)
        copy(zs.at[b], zr.at[z], z1s.at[b], z1r.at[z], z=b).start()
    squares = ssx[...]
    for k in x_near:
        b = other_x(k)
        copy(ssx, ssxr.at[b], xss.at[b], xsr.at[b], x=b).wait_recv()
        squares = squares + ssxr[b]
    ssz[...] = squares
    for k in z_far:
        b = other_z(k)
        copy(ssz, sszr.at[z], zss.at[b], zsr.at[z], z=b).start()

    for b in range(nx):
        core2[b].wait_recv()
    for k in x_far:
        b = other_x(k)
        xs2[b] = (own2[b] + rb2[b].astype(F32)).astype(BF16)
        copy(xs2.at[b], xr2.at[x], w1s.at[b], w1r.at[x], x=b).start()

    phase("values")
    lax.fori_loop(early, steps, rotate_chunks, 0)
    get_v.wait()

    def value_chunks(j, _):
        for u in range(2):
            at = pl.multiple_of((2 * j + u) * CHUNK, CHUNK)
            tmp[u] = vraw[pl.ds(pl.multiple_of(2 * at, 2 * CHUNK), 2 * CHUNK), :].astype(F32)
            alive = at + iota((CHUNK, LANES), 0) < live
            ones = jnp.where(alive, 1.0, 0.0).astype(BF16)
            for g in range(kv):
                values = jnp.where(alive, tmp[u, pl.ds(g, CHUNK, stride=kv), :], 0.0)
                vs[g, pl.ds(at, CHUNK), 0:LANES] = values.astype(BF16)
                vs[g, pl.ds(at, CHUNK), LANES:] = ones
        return 0

    lax.fori_loop(0, steps, value_chunks, 0)
    get_wo.wait()

    phase("z1_wait")
    total = zs[z].astype(F32)
    for k in z_near:
        b = other_z(k)
        copy(zs.at[b], zr.at[b], z1s.at[b], z1r.at[b], z=b).wait_recv()
        total = total + zr[b].astype(F32)
    for k in z_near:
        b = other_z(k)
        copy(ssz, sszr.at[b], zss.at[b], zsr.at[b], z=b).wait_recv()
        squares = squares + sszr[b]
    wt[...] = as_columns(lax.rsqrt(squares * (1.0 / d_model) + epsilon))
    which = lax.div(first_token, LANES)
    lane = lax.rem(first_token, LANES)

    def inverse_of(at, size):
        cols = wt[pl.ds(pl.multiple_of(at, 8), size), :]
        picked = cols[:, 0:1]
        for r in range(1, span // LANES):
            picked = jnp.where(which == r, cols[:, r : r + 1], picked)
        return picked

    query = rotated(total * inverse_of(lane, ROWS), q_cos, q_sin) * LANES**-0.5
    qbuf[c, x, z] = query.astype(BF16)

    for k in z_far:
        b = other_z(k)
        copy(qbuf.at[c, x, z], qbuf.at[c, x, z], z2s.at[b], z2r.at[z], z=b).start()

    def piece_to_x(t):
        for k in x_far:
            b = other_x(k)
            copy(qbuf.at[c, x, t], qbuf.at[c, x, t], x2s.at[b, t], x2r.at[x, t], x=b).start()

    piece_to_x(z)

    phase("new_keys")
    gathered = own2[x] + rb2[x].astype(F32)
    for k in x_near:
        b = other_x(k)
        copy(xs2.at[b], xr2.at[b], w1s.at[b], w1r.at[b], x=b).wait_recv()
        gathered = gathered + xr2[b].astype(F32)
    for t in range(nz):
        g, quarter = t // quarters, t % quarters
        pair = [
            gathered[quarter * tail : (quarter + 1) * tail, at + g * LANES : at + (g + 1) * LANES]
            for at in (0, kc)
        ]
        zs2[t] = jnp.concatenate(pair, 0).astype(BF16)
    for k in z_far:
        b = other_z(k)
        copy(zs2.at[b], zr2.at[z], v1s.at[b], v1r.at[z], z=b).start()

    phase("z2_wait")
    for k in z_near:
        b = other_z(k)
        copy(qbuf.at[c, x, b], qbuf.at[c, x, b], z2s.at[b], z2r.at[b], z=b).wait_recv()
        piece_to_x(b)

    phase("x2_wait")

    def block_to_core(b):
        return copy(qbuf.at[c, b], qbuf.at[c, b], c2s.at[b], c2r.at[b], c=sib)

    block_to_core(x).start()
    for k in x_near:
        b = other_x(k)
        for t in range(nz):
            copy(qbuf.at[c, b, t], qbuf.at[c, b, t], x2s.at[b, t], x2r.at[b, t], x=b).wait_recv()
        block_to_core(b).start()
    for k in x_far:
        b = other_x(k)
        copy(wobuf.at[x, c], wobuf.at[x, c], ws.at[b], wr.at[x], x=b).start()

    def weights_to_core(b):
        return copy(wobuf.at[b, c], wobuf.at[b, c], wcs.at[b], wcr.at[b], c=sib)

    weights_to_core(x).start()

    phase("new_keys_wait")
    total = zs2[z].astype(F32)
    for k in z_near:
        b = other_z(k)
        copy(zs2.at[b], zr2.at[b], v1s.at[b], v1r.at[b], z=b).wait_recv()
        total = total + zr2[b].astype(F32)
    inv_new = inverse_of(lane + my_quarter * tail, tail)
    new_k = (total[0:tail] * inv_new).astype(BF16).astype(F32)
    new_k = rotated(new_k, k_cos, k_sin)
    new_v = total[tail:] * inv_new
    empty = jnp.zeros((LANES - tail, LANES), F32)
    new_k = jnp.concatenate([new_k, empty], 0).astype(BF16)
    new_v = jnp.concatenate([new_v, empty], 0).astype(BF16)
    new_ones = jnp.where(iota((LANES, LANES), 0) < tail, 1.0, 0.0).astype(BF16)
    for g in range(kv):
        ks[g, slots:, :] = new_k
        vs[g, slots:, 0:LANES] = new_v
        vs[g, slots:, LANES:] = new_ones

    rows = 2 * block
    apart = nx // 2
    pairs = [(i, i + apart) for i in range(apart)]

    def attend(cc, pair):
        blocks = [other_x(k) for k in pair]
        row = iota((rows, LANES), 0)
        token = jnp.where(row < block, blocks[0], blocks[1]) * per_x + cc * ROWS + lax.rem(row, ROWS)
        lane = iota((rows, LANES), 1)
        seen = jnp.logical_and(lane < tail, k_first + lane <= token)
        for g in range(kv):
            q = jnp.concatenate(
                [qbuf[cc, b, g * group : (g + 1) * group].reshape(block, LANES) for b in blocks], 0
            )
            most = jnp.full((rows, LANES), negative, F32)
            for at in range(0, slots, KEYS):
                score = lax.dot_general(
                    q, ks[g, at : at + KEYS, :], (((1,), (1,)), ((), ())), preferred_element_type=F32
                )
                s_ref[g, :, at : at + KEYS] = score
                for lo in range(0, KEYS, LANES):
                    most = jnp.maximum(most, score[:, lo : lo + LANES])
            score = lax.dot_general(
                q, ks[g, slots:, :], (((1,), (1,)), ((), ())), preferred_element_type=F32
            )
            score = jnp.where(jnp.logical_and(seen, my_g == g), score, negative)
            most = jnp.max(jnp.maximum(most, score), axis=1, keepdims=True)
            acc = jnp.dot(
                jnp.exp(score - most).astype(BF16), vs[g, slots:, :], preferred_element_type=F32
            )
            for at in range(0, slots, KEYS):
                prob = jnp.exp(s_ref[g, :, at : at + KEYS] - most).astype(BF16)
                acc = acc + jnp.dot(prob, vs[g, at : at + KEYS, :], preferred_element_type=F32)
            sums = acc[:, LANES:]
            result = acc[:, 0:LANES] / sums
            lse = most + jnp.log(sums)
            for j, b in enumerate(blocks):
                cut = slice(j * block, (j + 1) * block)
                yield b, g, result[cut], lse[cut].T[0:1]

    def core3(b):
        return (
            copy(obs.at[b], obr.at[b], c3s.at[b], c3r.at[b], c=sib),
            copy(lss.at[b], lsr.at[b], c3ls.at[b], c3lr.at[b], c=sib),
        )

    def combine(outs, logs):
        top = functools.reduce(jnp.maximum, logs)
        weights = [jnp.exp(v - top) for v in logs]
        whole = sum(weights)
        spare = jnp.zeros((8 - kv, LANES), F32)
        columns = as_columns(
            jnp.concatenate([jnp.concatenate([w / whole, spare], 0) for w in weights], 0)
        )
        parts = []
        for g in range(kv):
            cut = slice(g * block, (g + 1) * block)
            parts.append(sum(columns[:, 8 * i + g : 8 * i + g + 1] * o[cut] for i, o in enumerate(outs)))
        return jnp.concatenate(parts, 0), top + jnp.log(whole)

    def own_unit(pair):
        for b, g, result, lse in attend(c, pair):
            ob[b, g * block : (g + 1) * block, :] = result
            lb[b, g : g + 1, :] = lse

    def sibling_unit(pair):
        for b, g, result, lse in attend(sib, pair):
            obs[b, g * block : (g + 1) * block, :] = result.astype(BF16)
            lss[b, g : g + 1, :] = lse
        for k in pair:
            for one in core3(other_x(k)):
                one.start()

    away = sorted(
        ((i, j) for i in range(nx) for j in range(nz)),
        key=lambda k: -min(k[0], nx - k[0]) - min(k[1], nz - k[1]),
    )

    def piece3(i, j):
        b, t = other_x(i), other_z(j)
        return (
            copy(oxs.at[b, t], oxr.at[x, z], x3s.at[b, t], x3r.at[x, z], x=b, z=t),
            copy(lxs.at[b], lxr.at[x, z], x3ls.at[b, t], x3lr.at[x, z], x=b, z=t),
        )

    def arrival3(i, j):
        b, t = other_x(i), other_z(j)
        return (
            copy(oxs.at[b, t], oxr.at[b, t], x3s.at[b, t], x3r.at[b, t], x=b, z=t),
            copy(lxs.at[b], lxr.at[b, t], x3ls.at[b, t], x3lr.at[b, t], x=b, z=t),
        )

    def join_cores(pair):
        for k in pair:
            b = other_x(k)
            for one in core3(b):
                one.wait_recv()
            out, lse = combine([ob[b], obr[b].astype(F32)], [lb[b], lsr[b]])
            oxs[b] = out.astype(BF16).reshape(nz, ROWS, LANES)
            lxs[b] = lse
        for i, j in away:
            if i in pair and (i or j):
                for one in piece3(i, j):
                    one.start()

    phase("unit_0")
    own_unit(pairs[0])
    phase("c2_wait")
    for k in range(nx):
        b = other_x(k)
        copy(qbuf.at[sib, b], qbuf.at[sib, b], c2s.at[b], c2r.at[b], c=sib).wait_recv()
    for i, pair in enumerate(pairs):
        phase("unit_1")
        sibling_unit(pair)
        if i == 0:
            phase("weights")
            for k in x_near:
                b = other_x(k)
                copy(wobuf.at[b, c], wobuf.at[b, c], ws.at[b], wr.at[b], x=b).wait_recv()
                weights_to_core(b).start()
    phase("join")
    join_cores(pairs[0])
    for pair in pairs[1:]:
        phase("unit_2")
        own_unit(pair)
        phase("join_2")
        join_cores(pair)

    phase("x3_wait")
    outs, logs = [oxs[x, z]], [lxs[x]]
    for i, j in away[::-1]:
        if i or j:
            for one in arrival3(i, j):
                one.wait_recv()
            outs.append(oxr[other_x(i), other_z(j)])
            logs.append(lxr[other_x(i), other_z(j)])
    phase("combine")
    picked = []
    for v in logs:
        row = v[0:1]
        for g in range(1, kv):
            row = jnp.where(my_g == g, v[g : g + 1], row)
        picked.append(row)
    weights = jnp.concatenate(picked, 0)
    weights = jnp.exp(weights - jnp.max(weights, axis=0, keepdims=True))
    wt[...] = as_columns(weights / jnp.sum(weights, axis=0, keepdims=True))
    mine = wt[pl.ds(pl.multiple_of(my_quarter * ROWS, ROWS), ROWS), :]
    attended = sum(mine[:, i : i + 1] * o.astype(F32) for i, o in enumerate(outs))
    att[z] = attended.astype(BF16)

    for k in z_far:
        b = other_z(k)
        copy(att.at[z], att.at[z], z4s.at[b], z4r.at[z], z=b).start()

    phase("z4_wait")
    for k in range(1, nx):
        b = other_x(k)
        copy(wobuf.at[b, sib], wobuf.at[b, sib], wcs.at[b], wcr.at[b], c=sib).wait_recv()
    copy(wobuf.at[x, sib], wobuf.at[x, sib], wcs.at[x], wcr.at[x], c=sib).wait_recv()
    for k in z_near:
        b = other_z(k)
        copy(att.at[b], att.at[b], z4s.at[b], z4r.at[b], z=b).wait_recv()

    phase("w_out")
    lhs = jnp.concatenate([att[t] for t in range(heads)], 1)
    rhs = wobuf[...].reshape(nx * nc * HALF, heads * LANES)
    got = lax.dot_general(lhs, rhs, (((1,), (1,)), ((), ())), preferred_element_type=F32)
    deep = ROWS // 2
    low = iota((deep, LANES), 1) < HALF
    for b in range(nx):
        both = got[:, b * LANES : (b + 1) * LANES]
        turned = pltpu.roll(both, HALF, 1)
        p5s[b, 0] = jnp.where(low, both[0:deep], turned[deep:]).astype(BF16)
        p5s[b, 1] = jnp.where(low, turned[0:deep], both[deep:]).astype(BF16)

    def last(b, cc):
        return copy(p5s.at[b, cc], p5r.at[c, y], y5s.at[b, cc], y5r.at[c, y], x=b, c=cc, y=x)

    for k in x_far:
        for cc in range(nc):
            last(other_x(k), cc).start()
    last(x, sib).start()

    @pl.when(x != y)
    def _():
        last(x, c).start()

    @pl.when(x == y)
    def _():
        p5r[c, y] = p5s[x, c]

    phase("y5_wait")

    def arrival(cc, b):
        return copy(p5s.at[y, cc], p5r.at[cc, b], y5s.at[y, cc], y5r.at[cc, b], x=y, c=cc, y=b)

    for k in range(1, ny):
        for cc in range(nc):
            arrival(cc, lax.rem(y + k, ny)).wait_recv()
    arrival(sib, y).wait_recv()

    @pl.when(x != y)
    def _():
        arrival(c, y).wait_recv()

    for cc in range(nc):
        final = sum(p5r[cc, b].astype(F32) for b in range(ny))
        at = cc * ROWS
        out_ref[at : at + deep, :] = final[:, 0:HALF].astype(BF16)
        out_ref[at + deep : at + ROWS, :] = pltpu.roll(final, HALF, 1)[:, 0:HALF].astype(BF16)

    phase("drain")
    sum_c.wait_send()
    for b in range(nx):
        core1[b].wait_send()
        core2[b].wait_send()
        block_to_core(b).wait_send()
        weights_to_core(b).wait_send()
        for one in core3(b):
            one.wait_send()
    for k in range(1, nx):
        b = other_x(k)
        copy(xs.at[b], xr.at[x], x1s.at[b], x1r.at[x], x=b).wait_send()
        copy(ssx, ssxr.at[x], xss.at[b], xsr.at[x], x=b).wait_send()
        copy(wobuf.at[x, c], wobuf.at[x, c], ws.at[b], wr.at[x], x=b).wait_send()
        for t in range(nz):
            copy(qbuf.at[c, x, t], qbuf.at[c, x, t], x2s.at[b, t], x2r.at[x, t], x=b).wait_send()
        copy(xs2.at[b], xr2.at[x], w1s.at[b], w1r.at[x], x=b).wait_send()
        for cc in range(nc):
            last(b, cc).wait_send()
    for k in range(1, nz):
        b = other_z(k)
        copy(zs.at[b], zr.at[z], z1s.at[b], z1r.at[z], z=b).wait_send()
        copy(ssz, sszr.at[z], zss.at[b], zsr.at[z], z=b).wait_send()
        copy(qbuf.at[c, x, z], qbuf.at[c, x, z], z2s.at[b], z2r.at[z], z=b).wait_send()
        copy(zs2.at[b], zr2.at[z], v1s.at[b], v1r.at[z], z=b).wait_send()
        copy(att.at[z], att.at[z], z4s.at[b], z4r.at[z], z=b).wait_send()
    last(x, sib).wait_send()
    for i, j in away:
        if i or j:
            for one in piece3(i, j):
                one.wait_send()

    @pl.when(x != y)
    def _():
        last(x, c).wait_send()

    phase(None)


def local(
    sizes, hidden_in, norm_gain, w_query, w_key, w_value, w_out, cache_keys, cache_values, lengths, span_start
):
    nx, nz, nc, ny = sizes
    slots, kv, head_dim = cache_keys.shape
    span, depth = hidden_in.shape
    heads = w_query.shape[1] // head_dim
    assert head_dim == LANES and heads == nz and nc == 2 and span == nx * nc * ROWS and nx == ny
    assert w_out.shape[1] == HALF and slots % KEYS == 0 and kv == 2
    cols, cols2 = w_query.shape[1], 2 * w_key.shape[1]
    block = heads * ROWS
    piece = 2 * (ROWS * kv // nz)
    keys = slots + LANES
    rows = 2 * (heads // kv) * ROWS
    lines = span // LANES
    hbm = pl.BlockSpec(memory_space=pltpu.HBM)
    V = pltpu.VMEM
    dma = pltpu.SemaphoreType.DMA
    scratch = [
        pltpu.SMEM(lengths.shape, jnp.int32), pltpu.SMEM(span_start.shape, jnp.int32),
        V((depth, span), BF16), V((1, depth), BF16), V(w_query.shape, BF16), V(w_key.shape, BF16),
        V(w_value.shape, BF16), V((1, LANES), F32),
        V((slots * kv, LANES), BF16), V((slots * kv, LANES), BF16), V((2, CHUNK * kv, LANES), F32),
        V((kv, keys, LANES), BF16), V((kv, keys, 2 * LANES), BF16),
        V((2, slots // CHUNK, LANES), F32), V((2, CHUNK, LANES), F32),
        V((nx, ROWS, cols), BF16), V((nx, ROWS, cols), BF16), V((nx, ROWS, cols), F32),
        V((nx, ROWS, cols), BF16), V((nx, ROWS, cols), BF16),
        V((nz, ROWS, LANES), BF16), V((nz, ROWS, LANES), BF16),
        V((nx, ROWS, cols2), BF16), V((nx, ROWS, cols2), BF16), V((nx, ROWS, cols2), F32),
        V((nx, ROWS, cols2), BF16), V((nx, ROWS, cols2), BF16),
        V((nz, piece, LANES), BF16), V((nz, piece, LANES), BF16),
        V((lines, LANES), F32), V((lines, LANES), F32), V((lines, LANES), F32), V((nx, lines, LANES), F32),
        V((lines, LANES), F32), V((nz, lines, LANES), F32),
        V((nc, nx, heads, ROWS, LANES), BF16), V((kv, rows, slots), F32),
        V((nx, block, LANES), F32), V((nx, kv, LANES), F32),
        V((nx, block, LANES), BF16), V((nx, block, LANES), BF16), V((nx, kv, LANES), F32), V((nx, kv, LANES), F32),
        V((nx, nz, ROWS, LANES), BF16), V((nx, nz, ROWS, LANES), BF16),
        V((nx, kv, LANES), F32), V((nx, nz, kv, LANES), F32),
        V((LANES, LANES), F32),
        V((heads, ROWS, LANES), BF16), V((nx, nc, HALF, w_out.shape[0]), BF16),
        V((nx, nc, ROWS // 2, LANES), BF16), V((nc, ny, ROWS // 2, LANES), BF16),
        dma((11,)),
        dma((nx,)), dma((nx,)), dma((nx,)), dma((nx,)), dma((nz,)), dma((nz,)),
        dma((nx,)), dma((nx,)), dma((nx,)), dma((nx,)), dma((nz,)), dma((nz,)),
        dma((1,)), dma((1,)), dma((nx,)), dma((nx,)), dma((nz,)), dma((nz,)),
        dma((nz,)), dma((nz,)), dma((nx, nz)), dma((nx, nz)), dma((nx,)), dma((nx,)),
        dma((nx,)), dma((nx,)), dma((nx,)), dma((nx,)),
        dma((nx,)), dma((nx,)), dma((nx,)), dma((nx,)),
        dma((nx, nz)), dma((nx, nz)), dma((nx, nz)), dma((nx, nz)),
        dma((nz,)), dma((nz,)), dma((nx, nc)), dma((nc, ny)),
    ]
    return pl.pallas_call(
        functools.partial(kernel, (nx, nz, nc, ny, nx * nz * nc * depth)),
        out_shape=pltpu.VMEM((nc * ROWS, HALF), BF16),
        in_specs=[hbm] * 11,
        out_specs=pl.BlockSpec(memory_space=pltpu.VMEM),
        scratch_shapes=scratch,
        compiler_params=pltpu.CompilerParams(
            collective_id=0, has_side_effects=True, vmem_limit_bytes=60 * 1024 * 1024
        ),
    )(
        lengths, span_start, hidden_in.T, norm_gain, w_query, w_key, w_value, w_out.T, frequencies(),
        cache_keys.reshape(slots * kv, LANES), cache_values.reshape(slots * kv, LANES),
    )


def solution(mesh):
    physical = mesh.devices.shape
    ny = mesh.shape["head"]
    nc, nz = 2, 8
    nx = physical[0] // (nc * nz)
    finer = Mesh(mesh.devices.reshape(nx, nz, nc, ny), ("x", "z", "c", "y"))
    seq = ("x", "z", "c")
    return jax.shard_map(
        functools.partial(local, (nx, nz, nc, ny)),
        mesh=finer,
        in_specs=(
            P(None, seq), P(None, seq), P(seq, "y"), P(seq, "y"), P(seq, "y"), P("y", seq),
            P(seq, "y", None), P(seq, "y", None), P(), P(),
        ),
        out_specs=P("y", seq),
        check_vma=False,
    )
```

```python
import functools
import math

import jax
import jax.numpy as jnp
import numpy as np
from jax import lax
from jax.experimental import pallas as pl
from jax.experimental.pallas import tpu as pltpu
from jax.sharding import Mesh
from jax.sharding import PartitionSpec as P

F32 = jnp.float32
BF16 = jnp.bfloat16
MESH = pl.DeviceIdType.MESH
LANES = 128
HALF = 64
ROWS = 32
CHUNK = 128
KEYS = 512
SMALL, BIG, WEIGHTS, LAST = range(4)

rope_base = 500000.0
stretch = 64.0
initial_context = 8192.0
ramp_low = 1.0
ramp_high = 32.0
epsilon = 1e-05
negative = -1e30
mscale = 0.1 * math.log(stretch) + 1.0


class Phases:
    def __init__(self):
        self.open = None

    def __call__(self, name):
        if self.open is not None:
            self.open.__exit__(None, None, None)
        self.open = None
        if name:
            self.open = jax.named_scope(name)
            self.open.__enter__()


def frequencies():
    base = rope_base ** (-2.0 * np.arange(HALF) / LANES)
    turns = initial_context * base / (2.0 * math.pi)
    share = np.clip((turns - ramp_low) / (ramp_high - ramp_low), 0.0, 1.0)
    freq = (1.0 - share) * base / stretch + share * base
    return np.concatenate([freq, freq])[None, :].astype(np.float32)


def cos_sin(angles):
    turns = jnp.floor(angles * (1.0 / (2.0 * math.pi)) + 0.5)
    first, second = 6.28125, 253.0 / 2.0**17
    third = 2.0 * math.pi - first - second
    rest = angles - turns * first - turns * second - turns * third
    return jnp.cos(rest), jnp.sin(rest)


def iota(shape, dim):
    return lax.broadcasted_iota(jnp.int32, shape, dim)


def signed(sine):
    return jnp.where(iota(sine.shape, 1) < HALF, -sine, sine)


def rotated(vectors, cosine, sine):
    return vectors * cosine + pltpu.roll(vectors, HALF, 1) * sine


def as_columns(rows):
    spare = LANES - rows.shape[0]
    if spare:
        rows = jnp.concatenate([rows, jnp.zeros((spare, LANES), F32)], 0)
    return rows.T


def kernel(
    dims,
    len_hbm, start_hbm, h_hbm, g_hbm, wq_hbm, wk_hbm, wv_hbm, wo_hbm, freq_hbm, k_hbm, v_hbm,
    out_ref,
    len_ref, start_ref,
    h_ref, g_ref, wq_ref, wk_ref, wv_ref, freq_ref, kraw, vraw, tmp, ks, vs, tab_a, tab_b,
    sb, rb, own, xs, xr, zs, zr, sb2, rb2, own2, xs2, xr2, zs2, zr2,
    ssc, sscr, ssx, ssxr, ssz, sszr, qbuf, s_ref,
    ob, lb, obs, obr, lss, lsr, oxs, oxr, lxs, lxr, wt,
    att, wobuf, p5s, p5r,
    dummy, in_sem, sent_sem,
    c1r, x1r, z1r, d1r, w1r, v1r, csr, xsr, zsr,
    z2r, x2r, c2r, wr, wcr, c3r, c3lr, x3r, x3lr, z4r, y5r,
):
    nx, nz, nc, ny, d_model = dims
    x, z, c, y = (lax.axis_index(n) for n in ("x", "z", "c", "y"))
    sib = 1 - c
    slots = kraw.shape[0] // 2
    group = wq_ref.shape[1] // wk_ref.shape[1]
    kv = wk_ref.shape[1] // LANES
    heads = kv * group
    quarters = nz // kv
    tail = ROWS // quarters
    qc = heads * LANES
    kc = kv * LANES
    per_x = nc * ROWS
    block = group * ROWS
    depth, span = h_ref.shape
    phase = Phases()

    sent = [0, 0, 0, 0]

    def copy(src, dst, kind, recv, **to):
        return pltpu.make_async_remote_copy(
            src_ref=src, dst_ref=dst, send_sem=sent_sem.at[kind], recv_sem=recv,
            device_id=to, device_id_type=MESH,
        )

    def send(src, dst, kind, recv, **to):
        copy(src, dst, kind, recv, **to).start()
        sent[kind] += math.prod(src.shape) * jnp.dtype(src.dtype).itemsize

    def receive(dst, recv):
        copy(dst, dst, SMALL, recv, c=sib).wait_recv()

    def other_x(k):
        return lax.rem(x + k, nx)

    def other_z(k):
        return lax.rem(z + k, nz)

    x_far = sorted(range(1, nx), key=lambda k: -min(k, nx - k))
    z_far = sorted(range(1, nz), key=lambda k: -min(k, nz - k))
    z_near = z_far[::-1]
    x_near = x_far[::-1]

    phase("entry")
    barrier = pltpu.get_barrier_semaphore()

    def greet(**to):
        pl.semaphore_signal(barrier, inc=1, device_id=to, device_id_type=MESH)

    for k in z_far:
        greet(z=other_z(k))
    for k in range(1, ny):
        for cc in range(nc):
            greet(x=y, y=lax.rem(y + k, ny), c=cc)

    @pl.when(x != y)
    def _():
        for cc in range(nc):
            greet(x=y, c=cc)

    for k in x_far:
        greet(x=other_x(k))
    greet(c=sib)

    fetches = []
    for i, (src, dst) in enumerate(
        (
            (h_hbm, h_ref), (g_hbm, g_ref), (wq_hbm, wq_ref), (wk_hbm, wk_ref), (wv_hbm, wv_ref),
            (freq_hbm, freq_ref), (len_hbm, len_ref), (start_hbm, start_ref),
            (k_hbm, kraw), (v_hbm, vraw), (wo_hbm, wobuf.at[x, c]),
        )
    ):
        fetches.append(pltpu.make_async_copy(src, dst, in_sem.at[i]))
        fetches[-1].start()
    get_h, get_g, get_wq, get_wk, get_wv, get_freq, get_len, get_start, get_k, get_v, get_wo = fetches

    get_h.wait()
    get_g.wait()
    hidden = h_ref[...].astype(F32)
    squares = jnp.sum(hidden * hidden, axis=0, keepdims=True)
    for r in range(span // LANES):
        ssc[r : r + 1, :] = squares[:, r * LANES : (r + 1) * LANES]
    gain = jnp.concatenate([g_ref[...].astype(F32), jnp.zeros((1, LANES - depth), F32)], 1)
    gain = jnp.broadcast_to(gain, (LANES, LANES)).T[0:depth, 0:1]
    scaled = jnp.concatenate([hidden * gain, jnp.zeros((LANES - depth, span), F32)], 0).T
    get_wq.wait()
    get_wk.wait()
    get_wv.wait()

    def rows_of(cc):
        blocks = [
            jnp.where(cc == 0, scaled[b * per_x : b * per_x + ROWS], scaled[b * per_x + ROWS : (b + 1) * per_x])
            for b in range(nx)
        ]
        return jnp.concatenate(blocks, 0)[:, 0:depth].astype(BF16)

    def project(rows, weights, to):
        at = 0
        for w in weights:
            got = jnp.dot(rows, w[...], preferred_element_type=F32)
            for b in range(nx):
                to[b, :, at : at + got.shape[1]] = got[b * ROWS : (b + 1) * ROWS].astype(to.dtype)
            at += got.shape[1]

    project(rows_of(sib), (wq_ref,), sb)
    project(rows_of(sib), (wk_ref, wv_ref), sb2)

    phase("barrier")
    peers = 1 + (nx - 1) + (nz - 1) + nc * (ny - 1)
    pl.semaphore_wait(barrier, jnp.where(x != y, peers + nc, peers))

    phase("core1_project")
    for b in range(nx):
        send(sb.at[b], rb.at[b], BIG, c1r, c=sib)
    send(ssc, sscr, SMALL, csr, c=sib)
    for b in range(nx):
        send(sb2.at[b], rb2.at[b], BIG, d1r, c=sib)

    project(rows_of(c), (wq_ref,), own)
    project(rows_of(c), (wk_ref, wv_ref), own2)
    get_freq.wait()
    freq = freq_ref[...]

    phase("core1_wait")
    receive(rb, c1r)
    for k in x_far:
        b = other_x(k)
        xs[b] = (own[b] + rb[b].astype(F32)).astype(BF16)
        send(xs.at[b], xr.at[x], BIG, x1r, x=b)
    receive(sscr, csr)
    ssx[...] = ssc[...] + sscr[...]
    for k in x_far:
        send(ssx, ssxr.at[x], SMALL, xsr, x=other_x(k))

    phase("keys")
    get_len.wait()
    get_start.wait()
    my = (x * nz + z) * nc + c
    count = nx * nz * nc

    def add_lengths(r, carry):
        before, total = carry
        return before + jnp.where(r < my, len_ref[r], 0), total + len_ref[r]

    offset, first_pos = lax.fori_loop(0, count, add_lengths, (jnp.int32(0), jnp.int32(0)))
    first_pos = first_pos + start_ref[0]
    live = len_ref[my]

    a_count = slots // CHUNK
    a_pos = (offset + CHUNK * iota((a_count, LANES), 0)).astype(F32)
    a_cos, a_sin = cos_sin(a_pos * freq)
    tab_a[0] = a_cos * mscale
    tab_a[1] = a_sin * mscale
    b_cos, b_sin = cos_sin(iota((CHUNK, LANES), 0).astype(F32) * freq)
    tab_b[0] = b_cos
    tab_b[1] = b_sin
    first_token = x * per_x + c * ROWS
    my_g, my_quarter = lax.div(z, quarters), lax.rem(z, quarters)
    k_first = first_token + my_quarter * tail
    q_pos = (first_pos + first_token + iota((ROWS, LANES), 0)).astype(F32)
    q_cos, q_sin = cos_sin(q_pos * freq)
    k_pos = (first_pos + k_first + iota((tail, LANES), 0)).astype(F32)
    k_cos, k_sin = cos_sin(k_pos * freq)
    q_cos, q_sin = q_cos * mscale, signed(q_sin * mscale)
    k_cos, k_sin = k_cos * mscale, signed(k_sin * mscale)

    get_k.wait()

    def slot_angles(a, size):
        cos_a = tab_a[0, pl.ds(a, 1), :]
        sin_a = tab_a[1, pl.ds(a, 1), :]
        cos_b, sin_b = tab_b[0, 0:size, :], tab_b[1, 0:size, :]
        return cos_a * cos_b - sin_a * sin_b, signed(sin_a * cos_b + cos_a * sin_b)

    tmp[0, 0 : 8 * kv, :] = kraw[0 : 8 * kv, :].astype(F32)
    slot_cos, slot_sin = slot_angles(0, 8)
    head_keys = [
        rotated(tmp[0, pl.ds(g, 8, stride=kv), :], slot_cos, slot_sin)[0:1] for g in range(kv)
    ]

    def rotate_chunks(j, _):
        for u in range(2):
            a = 2 * j + u
            at = pl.multiple_of(a * CHUNK, CHUNK)
            tmp[u] = kraw[pl.ds(pl.multiple_of(2 * at, 2 * CHUNK), 2 * CHUNK), :].astype(F32)
            cosine, sine = slot_angles(a, CHUNK)
            alive = at + iota((CHUNK, LANES), 0) < live
            for g in range(kv):
                keys = rotated(tmp[u, pl.ds(g, CHUNK, stride=kv), :], cosine, sine)
                ks[g, pl.ds(at, CHUNK), :] = jnp.where(alive, keys, head_keys[g]).astype(BF16)
        return 0

    steps = a_count // 2
    early = steps * 3 // 4
    lax.fori_loop(0, early, rotate_chunks, 0)

    phase("x1_wait")
    gathered = own[x] + rb[x].astype(F32)
    receive(xr.at[pl.ds(0, nx - 1)], x1r)
    for k in range(1, nx):
        gathered = gathered + xr[other_x(k)].astype(F32)
    for t in range(nz):
        zs[t] = gathered[:, t * LANES : (t + 1) * LANES].astype(BF16)
    for k in z_far:
        b = other_z(k)
        send(zs.at[b], zr.at[z], BIG, z1r, z=b)
    squares = ssx[...]
    receive(ssxr.at[pl.ds(0, nx - 1)], xsr)
    for k in range(1, nx):
        squares = squares + ssxr[other_x(k)]
    ssz[...] = squares
    for k in z_far:
        send(ssz, sszr.at[z], SMALL, zsr, z=other_z(k))

    receive(rb2, d1r)
    for k in x_far:
        b = other_x(k)
        xs2[b] = (own2[b] + rb2[b].astype(F32)).astype(BF16)
        send(xs2.at[b], xr2.at[x], BIG, w1r, x=b)

    phase("values")
    lax.fori_loop(early, steps, rotate_chunks, 0)
    get_v.wait()

    def value_chunks(j, _):
        for u in range(2):
            at = pl.multiple_of((2 * j + u) * CHUNK, CHUNK)
            tmp[u] = vraw[pl.ds(pl.multiple_of(2 * at, 2 * CHUNK), 2 * CHUNK), :].astype(F32)
            alive = at + iota((CHUNK, LANES), 0) < live
            ones = jnp.where(alive, 1.0, 0.0).astype(BF16)
            for g in range(kv):
                values = jnp.where(alive, tmp[u, pl.ds(g, CHUNK, stride=kv), :], 0.0)
                vs[g, pl.ds(at, CHUNK), 0:LANES] = values.astype(BF16)
                vs[g, pl.ds(at, CHUNK), LANES:] = ones
        return 0

    lax.fori_loop(0, steps, value_chunks, 0)
    get_wo.wait()

    phase("z1_wait")
    total = zs[z].astype(F32)
    receive(zr.at[pl.ds(0, nz - 1)], z1r)
    for k in range(1, nz):
        total = total + zr[other_z(k)].astype(F32)
    receive(sszr.at[pl.ds(0, nz - 1)], zsr)
    for k in range(1, nz):
        squares = squares + sszr[other_z(k)]
    wt[...] = as_columns(lax.rsqrt(squares * (1.0 / d_model) + epsilon))
    which = lax.div(first_token, LANES)
    lane = lax.rem(first_token, LANES)

    def inverse_of(at, size):
        cols = wt[pl.ds(pl.multiple_of(at, 8), size), :]
        picked = cols[:, 0:1]
        for r in range(1, span // LANES):
            picked = jnp.where(which == r, cols[:, r : r + 1], picked)
        return picked

    query = rotated(total * inverse_of(lane, ROWS), q_cos, q_sin) * LANES**-0.5
    qbuf[c, x, z] = query.astype(BF16)

    for k in z_far:
        send(qbuf.at[c, x, z], qbuf.at[c, x, z], BIG, z2r.at[z], z=other_z(k))

    def piece_to_x(t):
        for k in x_far:
            send(qbuf.at[c, x, t], qbuf.at[c, x, t], BIG, x2r.at[x], x=other_x(k))

    piece_to_x(z)

    phase("new_keys")
    gathered = own2[x] + rb2[x].astype(F32)
    receive(xr2.at[pl.ds(0, nx - 1)], w1r)
    for k in range(1, nx):
        gathered = gathered + xr2[other_x(k)].astype(F32)
    for t in range(nz):
        g, quarter = t // quarters, t % quarters
        pair = [
            gathered[quarter * tail : (quarter + 1) * tail, at + g * LANES : at + (g + 1) * LANES]
            for at in (0, kc)
        ]
        zs2[t] = jnp.concatenate(pair, 0).astype(BF16)
    for k in z_far:
        b = other_z(k)
        send(zs2.at[b], zr2.at[z], BIG, v1r, z=b)

    phase("z2_wait")
    for k in z_near:
        b = other_z(k)
        receive(qbuf.at[c, x, b], z2r.at[b])
        piece_to_x(b)

    def block_to_core(b):
        send(qbuf.at[c, b], qbuf.at[c, b], BIG, c2r.at[b], c=sib)

    block_to_core(x)

    phase("new_keys_wait")
    total = zs2[z].astype(F32)
    receive(zr2.at[pl.ds(0, nz - 1)], v1r)
    for k in range(1, nz):
        total = total + zr2[other_z(k)].astype(F32)
    inv_new = inverse_of(lane + my_quarter * tail, tail)
    new_k = (total[0:tail] * inv_new).astype(BF16).astype(F32)
    new_k = rotated(new_k, k_cos, k_sin)
    new_v = total[tail:] * inv_new
    empty = jnp.zeros((LANES - tail, LANES), F32)
    new_k = jnp.concatenate([new_k, empty], 0).astype(BF16)
    new_v = jnp.concatenate([new_v, empty], 0).astype(BF16)
    new_ones = jnp.where(iota((LANES, LANES), 0) < tail, 1.0, 0.0).astype(BF16)
    for g in range(kv):
        ks[g, slots:, :] = new_k
        vs[g, slots:, 0:LANES] = new_v
        vs[g, slots:, LANES:] = new_ones

    def attend(blocks):
        rows = len(blocks) * block
        token = jnp.concatenate(
            [
                other_x(k) * per_x + cc * ROWS + lax.rem(iota((block, LANES), 0), ROWS)
                for cc, k in blocks
            ],
            0,
        )
        lane = iota((rows, LANES), 1)
        seen = jnp.logical_and(lane < tail, k_first + lane <= token)
        for g in range(kv):
            q = [
                qbuf[cc, other_x(k), g * group : (g + 1) * group].reshape(block, LANES) for cc, k in blocks
            ]
            q = jnp.concatenate(q, 0)
            most = jnp.full((rows, LANES), negative, F32)
            for at in range(0, slots, KEYS):
                score = lax.dot_general(
                    q, ks[g, at : at + KEYS, :], (((1,), (1,)), ((), ())), preferred_element_type=F32
                )
                s_ref[g, :, at : at + KEYS] = score
                for lo in range(0, KEYS, LANES):
                    most = jnp.maximum(most, score[:, lo : lo + LANES])
            score = lax.dot_general(
                q, ks[g, slots:, :], (((1,), (1,)), ((), ())), preferred_element_type=F32
            )
            score = jnp.where(jnp.logical_and(seen, my_g == g), score, negative)
            most = jnp.max(jnp.maximum(most, score), axis=1, keepdims=True)
            acc = jnp.dot(
                jnp.exp(score - most).astype(BF16), vs[g, slots:, :], preferred_element_type=F32
            )
            for at in range(0, slots, KEYS):
                prob = jnp.exp(s_ref[g, :, at : at + KEYS] - most).astype(BF16)
                acc = acc + jnp.dot(prob, vs[g, at : at + KEYS, :], preferred_element_type=F32)
            sums = acc[:, LANES:]
            result = acc[:, 0:LANES] / sums
            lse = most + jnp.log(sums)
            for j, (cc, k) in enumerate(blocks):
                b, cut = other_x(k), slice(j * block, (j + 1) * block)
                if cc is sib:
                    obs[b, g * block : (g + 1) * block, :] = result[cut].astype(BF16)
                    lss[b, g : g + 1, :] = lse[cut].T[0:1]
                else:
                    ob[b, g * block : (g + 1) * block, :] = result[cut]
                    lb[b, g : g + 1, :] = lse[cut].T[0:1]
        for cc, k in blocks:
            if cc is sib:
                b = other_x(k)
                send(obs.at[b], obr.at[b], BIG, c3r.at[b], c=sib)
                send(lss.at[b], lsr.at[b], SMALL, c3lr.at[b], c=sib)

    away = sorted(
        ((i, j) for i in range(nx) for j in range(nz)),
        key=lambda k: -min(k[0], nx - k[0]) - min(k[1], nz - k[1]),
    )

    def join(places):
        weights, blocks = [], [other_x(k) for k in places]
        for b in blocks:
            receive(obr.at[b], c3r.at[b])
            receive(lsr.at[b], c3lr.at[b])
            logs = [lb[b], lsr[b]]
            top = jnp.maximum(*logs)
            lse = top + jnp.log(sum(jnp.exp(v - top) for v in logs))
            weights += [jnp.exp(v - lse) for v in logs]
            lxs[b] = lse
        columns = as_columns(jnp.concatenate(weights, 0))
        for i, b in enumerate(blocks):
            for g in range(kv):
                cut = slice(g * block, (g + 1) * block)
                at = 2 * kv * i + g
                out = columns[:, at : at + 1] * ob[b, cut, :]
                out = out + columns[:, at + kv : at + kv + 1] * obr[b, cut, :].astype(F32)
                oxs[b, g * group : (g + 1) * group] = out.astype(BF16).reshape(group, ROWS, LANES)
        for i, j in away:
            if i in places and (i or j):
                b, t = other_x(i), other_z(j)
                send(oxs.at[b, t], oxr.at[x * nz + z], BIG, x3r, x=b, z=t)
                send(lxs.at[b], lxr.at[x * nz + z], SMALL, x3lr, x=b, z=t)

    middle, final_x = list(range(1, nx - 1)), nx - 1
    phase("c2_wait")
    receive(qbuf.at[sib, x], c2r.at[x])
    phase("unit_0")
    attend([(c, 0), (sib, 0)])
    phase("x2_wait")
    for k in x_near:
        b = other_x(k)
        receive(qbuf.at[c, b], x2r.at[b])
        block_to_core(b)
    for k in x_far:
        send(wobuf.at[x, c], wobuf.at[x, c], WEIGHTS, wr, x=other_x(k))
    send(wobuf.at[x, c], wobuf.at[x, c], WEIGHTS, wcr, c=sib)
    if middle:
        phase("unit_1")
        attend([(c, k) for k in middle])
        phase("c2_wait2")
        for k in middle:
            receive(qbuf.at[sib, other_x(k)], c2r.at[other_x(k)])
        phase("unit_2")
        attend([(sib, k) for k in middle])
    phase("join_0")
    join([0])
    if middle:
        phase("join_1")
        join(middle)
    receive(qbuf.at[sib, other_x(final_x)], c2r.at[other_x(final_x)])
    phase("unit_3")
    attend([(sib, final_x), (c, final_x)])
    phase("join_3")
    join([final_x])
    receive(wobuf.at[pl.ds(0, nx - 1), c], wr)
    for k in range(1, nx):
        b = other_x(k)
        send(wobuf.at[b, c], wobuf.at[b, c], WEIGHTS, wcr, c=sib)

    phase("x3_wait")
    outs, logs = [oxs[x, z]], [lxs[x]]
    receive(oxr.at[pl.ds(0, nx * nz - 1)], x3r)
    receive(lxr.at[pl.ds(0, nx * nz - 1)], x3lr)
    for i, j in away:
        if i or j:
            at = other_x(i) * nz + other_z(j)
            outs.append(oxr[at])
            logs.append(lxr[at])
    phase("combine")
    picked = []
    for v in logs:
        row = v[0:1]
        for g in range(1, kv):
            row = jnp.where(my_g == g, v[g : g + 1], row)
        picked.append(row)
    weights = jnp.concatenate(picked, 0)
    weights = jnp.exp(weights - jnp.max(weights, axis=0, keepdims=True))
    wt[...] = as_columns(weights / jnp.sum(weights, axis=0, keepdims=True))
    mine = wt[pl.ds(pl.multiple_of(my_quarter * ROWS, ROWS), ROWS), :]
    attended = sum(mine[:, i : i + 1] * o.astype(F32) for i, o in enumerate(outs))
    att[z] = attended.astype(BF16)

    for k in z_far:
        send(att.at[z], att.at[z], BIG, z4r, z=other_z(k))

    phase("z4_wait")
    receive(wobuf.at[:, sib], wcr)
    receive(att.at[pl.ds(0, nz - 1)], z4r)

    phase("w_out")
    lhs = jnp.concatenate([att[t] for t in range(heads)], 1)
    rhs = wobuf[...].reshape(nx * nc * HALF, heads * LANES)
    got = lax.dot_general(lhs, rhs, (((1,), (1,)), ((), ())), preferred_element_type=F32)
    deep = ROWS // 2
    low = iota((deep, LANES), 1) < HALF
    for b in range(nx):
        both = got[:, b * LANES : (b + 1) * LANES]
        turned = pltpu.roll(both, HALF, 1)
        p5s[b, 0] = jnp.where(low, both[0:deep], turned[deep:]).astype(BF16)
        p5s[b, 1] = jnp.where(low, turned[0:deep], both[deep:]).astype(BF16)

    me = c * ny + y

    def last(b, cc):
        copy(p5s.at[b, cc], p5r.at[me], LAST, y5r, x=b, c=cc, y=x).start()

    for k in x_far:
        for cc in range(nc):
            last(other_x(k), cc)
    last(x, sib)

    @pl.when(x != y)
    def _():
        last(x, c)

    @pl.when(x == y)
    def _():
        p5r[me] = p5s[x, c]

    phase("y5_wait")

    @pl.when(x != y)
    def _():
        receive(p5r, y5r)

    @pl.when(x == y)
    def _():
        receive(p5r.at[pl.ds(0, nc * ny - 1)], y5r)

    for cc in range(nc):
        final = sum(p5r[cc * ny + b].astype(F32) for b in range(ny))
        at = cc * ROWS
        out_ref[at : at + deep, :] = final[:, 0:HALF].astype(BF16)
        out_ref[at + deep : at + ROWS, :] = pltpu.roll(final, HALF, 1)[:, 0:HALF].astype(BF16)

    phase("drain")

    def gone(ref, kind):
        copy(ref, ref, kind, c1r, c=sib).wait_send()

    line = LANES * jnp.dtype(BF16).itemsize
    gone(dummy.at[pl.ds(0, sent[SMALL] // (2 * line))], SMALL)
    gone(kraw.at[pl.ds(0, sent[BIG] // line)], BIG)
    gone(kraw.at[pl.ds(0, sent[WEIGHTS] // line)], WEIGHTS)

    @pl.when(x != y)
    def _():
        gone(p5r, LAST)

    @pl.when(x == y)
    def _():
        gone(p5r.at[pl.ds(0, nc * ny - 1)], LAST)

    phase(None)


def local(
    sizes, hidden_in, norm_gain, w_query, w_key, w_value, w_out, cache_keys, cache_values, lengths, span_start
):
    nx, nz, nc, ny = sizes
    slots, kv, head_dim = cache_keys.shape
    span, depth = hidden_in.shape
    heads = w_query.shape[1] // head_dim
    assert head_dim == LANES and heads == nz and nc == 2 and span == nx * nc * ROWS and nx == ny
    assert w_out.shape[1] == HALF and slots % KEYS == 0 and kv == 2
    cols, cols2 = w_query.shape[1], 2 * w_key.shape[1]
    block = heads * ROWS
    piece = 2 * (ROWS * kv // nz)
    keys = slots + LANES
    rows = 2 * (heads // kv) * ROWS
    lines = span // LANES
    hbm = pl.BlockSpec(memory_space=pltpu.HBM)
    V = pltpu.VMEM
    dma = pltpu.SemaphoreType.DMA
    scratch = [
        pltpu.SMEM(lengths.shape, jnp.int32), pltpu.SMEM(span_start.shape, jnp.int32),
        V((depth, span), BF16), V((1, depth), BF16), V(w_query.shape, BF16), V(w_key.shape, BF16),
        V(w_value.shape, BF16), V((1, LANES), F32),
        V((slots * kv, LANES), BF16), V((slots * kv, LANES), BF16), V((2, CHUNK * kv, LANES), F32),
        V((kv, keys, LANES), BF16), V((kv, keys, 2 * LANES), BF16),
        V((2, slots // CHUNK, LANES), F32), V((2, CHUNK, LANES), F32),
        V((nx, ROWS, cols), BF16), V((nx, ROWS, cols), BF16), V((nx, ROWS, cols), F32),
        V((nx, ROWS, cols), BF16), V((nx, ROWS, cols), BF16),
        V((nz, ROWS, LANES), BF16), V((nz, ROWS, LANES), BF16),
        V((nx, ROWS, cols2), BF16), V((nx, ROWS, cols2), BF16), V((nx, ROWS, cols2), F32),
        V((nx, ROWS, cols2), BF16), V((nx, ROWS, cols2), BF16),
        V((nz, piece, LANES), BF16), V((nz, piece, LANES), BF16),
        V((lines, LANES), F32), V((lines, LANES), F32), V((lines, LANES), F32), V((nx, lines, LANES), F32),
        V((lines, LANES), F32), V((nz, lines, LANES), F32),
        V((nc, nx, heads, ROWS, LANES), BF16), V((kv, rows, slots), F32),
        V((nx, block, LANES), F32), V((nx, kv, LANES), F32),
        V((nx, block, LANES), BF16), V((nx, block, LANES), BF16), V((nx, kv, LANES), F32), V((nx, kv, LANES), F32),
        V((nx, nz, ROWS, LANES), BF16), V((nx * nz, ROWS, LANES), BF16),
        V((nx, kv, LANES), F32), V((nx * nz, kv, LANES), F32),
        V((LANES, LANES), F32),
        V((heads, ROWS, LANES), BF16), V((nx, nc, HALF, w_out.shape[0]), BF16),
        V((nx, nc, ROWS // 2, LANES), BF16), V((nc * ny, ROWS // 2, LANES), BF16),
        V((128, 1, LANES), F32), dma((11,)), dma((4,)),
        dma, dma, dma, dma, dma, dma, dma, dma, dma,
        dma((nz,)), dma((nx,)), dma((nx,)), dma, dma, dma((nx,)), dma((nx,)), dma, dma, dma, dma,
    ]
    return pl.pallas_call(
        functools.partial(kernel, (nx, nz, nc, ny, nx * nz * nc * depth)),
        out_shape=pltpu.VMEM((nc * ROWS, HALF), BF16),
        in_specs=[hbm] * 11,
        out_specs=pl.BlockSpec(memory_space=pltpu.VMEM),
        scratch_shapes=scratch,
        compiler_params=pltpu.CompilerParams(
            collective_id=0, has_side_effects=True, vmem_limit_bytes=60 * 1024 * 1024
        ),
    )(
        lengths, span_start, hidden_in.T, norm_gain, w_query, w_key, w_value, w_out.T, frequencies(),
        cache_keys.reshape(slots * kv, LANES), cache_values.reshape(slots * kv, LANES),
    )


def solution(mesh):
    physical = mesh.devices.shape
    ny = mesh.shape["head"]
    nc, nz = 2, 8
    nx = physical[0] // (nc * nz)
    finer = Mesh(mesh.devices.reshape(nx, nz, nc, ny), ("x", "z", "c", "y"))
    seq = ("x", "z", "c")
    return jax.shard_map(
        functools.partial(local, (nx, nz, nc, ny)),
        mesh=finer,
        in_specs=(
            P(None, seq), P(None, seq), P(seq, "y"), P(seq, "y"), P(seq, "y"), P("y", seq),
            P(seq, "y", None), P(seq, "y", None), P(), P(),
        ),
        out_specs=P("y", seq),
        check_vma=False,
    )
```

```python
import functools
import math

import jax
import jax.numpy as jnp
import numpy as np
from jax import lax
from jax.experimental import pallas as pl
from jax.experimental.pallas import tpu as pltpu
from jax.sharding import Mesh
from jax.sharding import PartitionSpec as P

F32 = jnp.float32
BF16 = jnp.bfloat16
MESH = pl.DeviceIdType.MESH
LANES = 128
HALF = 64
ROWS = 32
CHUNK = 128
KEYS = 512
SMALL, BIG, WEIGHTS, LAST = range(4)

rope_base = 500000.0
stretch = 64.0
initial_context = 8192.0
ramp_low = 1.0
ramp_high = 32.0
epsilon = 1e-05
negative = -1e30
mscale = 0.1 * math.log(stretch) + 1.0


class Phases:
    def __init__(self):
        self.open = None

    def __call__(self, name):
        if self.open is not None:
            self.open.__exit__(None, None, None)
        self.open = None
        if name:
            self.open = jax.named_scope(name)
            self.open.__enter__()


def frequencies():
    base = rope_base ** (-2.0 * np.arange(HALF) / LANES)
    turns = initial_context * base / (2.0 * math.pi)
    share = np.clip((turns - ramp_low) / (ramp_high - ramp_low), 0.0, 1.0)
    freq = (1.0 - share) * base / stretch + share * base
    return np.concatenate([freq, freq])[None, :].astype(np.float32)


def cos_sin(angles):
    turns = jnp.floor(angles * (1.0 / (2.0 * math.pi)) + 0.5)
    first, second = 6.28125, 253.0 / 2.0**17
    third = 2.0 * math.pi - first - second
    rest = angles - turns * first - turns * second - turns * third
    return jnp.cos(rest), jnp.sin(rest)


def iota(shape, dim):
    return lax.broadcasted_iota(jnp.int32, shape, dim)


def signed(sine):
    return jnp.where(iota(sine.shape, 1) < HALF, -sine, sine)


def rotated(vectors, cosine, sine):
    return vectors * cosine + pltpu.roll(vectors, HALF, 1) * sine


def as_columns(rows):
    spare = LANES - rows.shape[0]
    if spare:
        rows = jnp.concatenate([rows, jnp.zeros((spare, LANES), F32)], 0)
    return rows.T


def kernel(
    dims,
    len_hbm, start_hbm, h_hbm, g_hbm, wq_hbm, wk_hbm, wv_hbm, wo_hbm, freq_hbm, k_hbm, v_hbm,
    out_ref,
    len_ref, start_ref,
    h_ref, g_ref, wq_ref, wk_ref, wv_ref, freq_ref, kraw, vraw, tmp, ks, vs, tab_a, tab_b,
    sb, rb, own, xs, xr, zs, zr, sb2, rb2, own2, xs2, xr2, zs2, zr2,
    ssc, sscr, ssx, ssxr, ssz, sszr, qbuf, s_ref,
    ob, lb, obs, obr, lss, lsr, oxs, oxr, lxs, lxr, wt,
    att, wobuf, p5s, p5r,
    dummy, in_sem, sent_sem,
    hear_x, hear_z, hear_y, rel, merged, relr, c1r, x1r, z1r, d1r, w1r, v1r, csr, xsr, zsr,
    z2r, x2r, c2r, wr, wcr, c3r, c3lr, x3r, x3lr, z4r, y5r,
):
    nx, nz, nc, ny, d_model = dims
    x, z, c, y = (lax.axis_index(n) for n in ("x", "z", "c", "y"))
    sib = 1 - c
    slots = kraw.shape[0] // 2
    group = wq_ref.shape[1] // wk_ref.shape[1]
    kv = wk_ref.shape[1] // LANES
    heads = kv * group
    quarters = nz // kv
    tail = ROWS // quarters
    qc = heads * LANES
    kc = kv * LANES
    per_x = nc * ROWS
    block = group * ROWS
    depth, span = h_ref.shape
    cols = own.shape[2]
    phase = Phases()

    sent = [0, 0, 0, 0]

    def copy(src, dst, kind, recv, **to):
        return pltpu.make_async_remote_copy(
            src_ref=src, dst_ref=dst, send_sem=sent_sem.at[kind], recv_sem=recv,
            device_id=to, device_id_type=MESH,
        )

    def send(src, dst, kind, recv, **to):
        copy(src, dst, kind, recv, **to).start()
        sent[kind] += math.prod(src.shape) * jnp.dtype(src.dtype).itemsize

    def receive(dst, recv):
        copy(dst, dst, SMALL, recv, c=sib).wait_recv()

    def other_x(k):
        return lax.rem(x + k, nx)

    def other_z(k):
        return lax.rem(z + k, nz)

    x_far = sorted(range(1, nx), key=lambda k: -min(k, nx - k))
    z_far = sorted(range(1, nz), key=lambda k: -min(k, nz - k))
    z_near = z_far[::-1]
    x_near = x_far[::-1]

    phase("entry")
    barrier = pltpu.get_barrier_semaphore()

    def greet(**to):
        pl.semaphore_signal(barrier, inc=1, device_id=to, device_id_type=MESH)

    beside = {"x": sorted({1, nx - 1}), "z": sorted({1, nz - 1}), "y": sorted({1, ny - 1})}
    places = {"x": (x, nx), "z": (z, nz), "y": (y, ny)}

    def neighbours(axis):
        at, size = places[axis]
        return [{axis: lax.rem(at + k, size)} for k in beside[axis]]

    for axis in ("z", "x", "y"):
        for to in neighbours(axis):
            greet(**to)
    greet(c=sib)

    def tell(sem, axis):
        for to in neighbours(axis):
            pl.semaphore_signal(sem, inc=1, device_id=to, device_id_type=MESH)

    def hear(sem, axis):
        pl.semaphore_wait(sem, len(beside[axis]))

    fetches = []
    for i, (src, dst) in enumerate(
        (
            (h_hbm, h_ref), (g_hbm, g_ref), (wq_hbm, wq_ref), (wk_hbm, wk_ref), (wv_hbm, wv_ref),
            (freq_hbm, freq_ref), (len_hbm, len_ref), (start_hbm, start_ref),
            (k_hbm, kraw), (v_hbm, vraw), (wo_hbm, wobuf.at[x, c]),
        )
    ):
        fetches.append(pltpu.make_async_copy(src, dst, in_sem.at[i]))
        fetches[-1].start()
    get_h, get_g, get_wq, get_wk, get_wv, get_freq, get_len, get_start, get_k, get_v, get_wo = fetches

    get_h.wait()
    get_g.wait()
    hidden = h_ref[...].astype(F32)
    squares = jnp.sum(hidden * hidden, axis=0, keepdims=True)
    for r in range(span // LANES):
        ssc[r : r + 1, :] = squares[:, r * LANES : (r + 1) * LANES]
    gain = jnp.concatenate([g_ref[...].astype(F32), jnp.zeros((1, LANES - depth), F32)], 1)
    gain = jnp.broadcast_to(gain, (LANES, LANES)).T[0:depth, 0:1]
    scaled = jnp.concatenate([hidden * gain, jnp.zeros((LANES - depth, span), F32)], 0).T
    get_wq.wait()
    get_wk.wait()
    get_wv.wait()

    def rows_of(cc):
        blocks = [
            jnp.where(cc == 0, scaled[b * per_x : b * per_x + ROWS], scaled[b * per_x + ROWS : (b + 1) * per_x])
            for b in range(nx)
        ]
        return jnp.concatenate(blocks, 0)[:, 0:depth].astype(BF16)

    def project(rows, weights, to):
        at = 0
        for w in weights:
            got = jnp.dot(rows, w[...], preferred_element_type=F32)
            for b in range(nx):
                to[b, :, at : at + got.shape[1]] = got[b * ROWS : (b + 1) * ROWS].astype(to.dtype)
            at += got.shape[1]

    project(rows_of(sib), (wq_ref,), sb)
    project(rows_of(sib), (wk_ref, wv_ref), sb2)

    phase("barrier")
    pl.semaphore_wait(barrier, 1 + sum(len(beside[axis]) for axis in beside))
    tell(hear_x, "x")
    tell(hear_z.at[0], "z")

    phase("core1_project")
    for b in range(nx):
        send(sb.at[b], rb.at[b], BIG, c1r, c=sib)
    send(ssc, sscr, SMALL, csr, c=sib)
    for b in range(nx):
        send(sb2.at[b], rb2.at[b], BIG, d1r, c=sib)

    project(rows_of(c), (wq_ref,), own)
    project(rows_of(c), (wk_ref, wv_ref), own2)
    get_freq.wait()
    freq = freq_ref[...]

    phase("core1_wait")
    receive(rb, c1r)
    hear(hear_x, "x")
    hear(hear_z.at[0], "z")
    tell(hear_z.at[1], "z")
    relayed = nx == 4
    deep = ROWS // 2
    for k in x_far:
        b = other_x(k)
        sums = (own[b] + rb[b].astype(F32)).astype(BF16)
        xs[2 * b] = sums[0:deep]
        xs[2 * b + 1] = sums[deep:]
        send(xs.at[2 * b], xr.at[2 * x], BIG, x1r, x=b)
        if relayed and k > 1:
            def direct():
                copy(xs.at[2 * b + 1], xr.at[2 * x + 1], BIG, x1r, x=b).start()

            pl.when(c == 0)(direct)
            if k == 2:

                @pl.when(c == 1)
                def _():
                    copy(xs.at[2 * b + 1], rel, BIG, relr, x=other_x(3)).start()

            sent[BIG] += deep * cols * 2
        else:
            send(xs.at[2 * b + 1], xr.at[2 * x + 1], BIG, x1r, x=b)
    receive(sscr, csr)
    ssx[...] = ssc[...] + sscr[...]
    for k in x_far:
        send(ssx, ssxr.at[x], SMALL, xsr, x=other_x(k))

    phase("keys")
    get_len.wait()
    get_start.wait()
    my = (x * nz + z) * nc + c
    count = nx * nz * nc

    def add_lengths(r, carry):
        before, total = carry
        return before + jnp.where(r < my, len_ref[r], 0), total + len_ref[r]

    offset, first_pos = lax.fori_loop(0, count, add_lengths, (jnp.int32(0), jnp.int32(0)))
    first_pos = first_pos + start_ref[0]
    live = len_ref[my]

    a_count = slots // CHUNK
    a_pos = (offset + CHUNK * iota((a_count, LANES), 0)).astype(F32)
    a_cos, a_sin = cos_sin(a_pos * freq)
    tab_a[0] = a_cos * mscale
    tab_a[1] = a_sin * mscale
    b_cos, b_sin = cos_sin(iota((CHUNK, LANES), 0).astype(F32) * freq)
    tab_b[0] = b_cos
    tab_b[1] = b_sin
    first_token = x * per_x + c * ROWS
    my_g, my_quarter = lax.div(z, quarters), lax.rem(z, quarters)
    k_first = first_token + my_quarter * tail
    q_pos = (first_pos + first_token + iota((ROWS, LANES), 0)).astype(F32)
    q_cos, q_sin = cos_sin(q_pos * freq)
    k_pos = (first_pos + k_first + iota((tail, LANES), 0)).astype(F32)
    k_cos, k_sin = cos_sin(k_pos * freq)
    q_cos, q_sin = q_cos * mscale, signed(q_sin * mscale)
    k_cos, k_sin = k_cos * mscale, signed(k_sin * mscale)

    get_k.wait()

    def slot_angles(a, size):
        cos_a = tab_a[0, pl.ds(a, 1), :]
        sin_a = tab_a[1, pl.ds(a, 1), :]
        cos_b, sin_b = tab_b[0, 0:size, :], tab_b[1, 0:size, :]
        return cos_a * cos_b - sin_a * sin_b, signed(sin_a * cos_b + cos_a * sin_b)

    tmp[0, 0 : 8 * kv, :] = kraw[0 : 8 * kv, :].astype(F32)
    slot_cos, slot_sin = slot_angles(0, 8)
    head_keys = [
        rotated(tmp[0, pl.ds(g, 8, stride=kv), :], slot_cos, slot_sin)[0:1] for g in range(kv)
    ]

    def rotate_chunks(j, _):
        for u in range(2):
            a = 2 * j + u
            at = pl.multiple_of(a * CHUNK, CHUNK)
            tmp[u] = kraw[pl.ds(pl.multiple_of(2 * at, 2 * CHUNK), 2 * CHUNK), :].astype(F32)
            cosine, sine = slot_angles(a, CHUNK)
            alive = at + iota((CHUNK, LANES), 0) < live
            for g in range(kv):
                keys = rotated(tmp[u, pl.ds(g, CHUNK, stride=kv), :], cosine, sine)
                ks[g, pl.ds(at, CHUNK), :] = jnp.where(alive, keys, head_keys[g]).astype(BF16)
        return 0

    steps = a_count // 2
    early = steps * 3 // 4
    lax.fori_loop(0, early, rotate_chunks, 0)

    phase("x1_wait")
    hear(hear_z.at[1], "z")
    tell(hear_z.at[2], "z")
    gathered = own[x] + rb[x].astype(F32)
    if relayed:

        @pl.when(c == 1)
        def _():
            b = other_x(3)
            receive(rel, relr)
            merged[...] = (own[b, deep:] + rb[b, deep:].astype(F32) + rel[...].astype(F32)).astype(BF16)
            copy(merged, xr.at[2 * x + 1], BIG, x1r, x=b).start()
            receive(xr.at[pl.ds(0, 2 * nx - 3)], x1r)

        @pl.when(c == 0)
        def _():
            receive(xr.at[pl.ds(0, 2 * nx - 2)], x1r)

    else:
        receive(xr.at[pl.ds(0, 2 * nx - 2)], x1r)
    for k in range(1, nx):
        b = other_x(k)
        second = xr[2 * b + 1].astype(F32)
        if relayed and k == 2:
            second = jnp.where(c == 0, second, 0.0)
        gathered = gathered + jnp.concatenate([xr[2 * b].astype(F32), second], 0)
    tell(hear_y.at[0], "y")
    hear(hear_z.at[2], "z")
    for t in range(nz):
        zs[t] = gathered[:, t * LANES : (t + 1) * LANES].astype(BF16)
    for k in z_far:
        b = other_z(k)
        send(zs.at[b], zr.at[z], BIG, z1r, z=b)
    squares = ssx[...]
    receive(ssxr.at[pl.ds(0, nx - 1)], xsr)
    for k in range(1, nx):
        squares = squares + ssxr[other_x(k)]
    ssz[...] = squares
    for k in z_far:
        send(ssz, sszr.at[z], SMALL, zsr, z=other_z(k))

    receive(rb2, d1r)
    for k in x_far:
        b = other_x(k)
        xs2[b] = (own2[b] + rb2[b].astype(F32)).astype(BF16)
        send(xs2.at[b], xr2.at[x], BIG, w1r, x=b)

    phase("values")
    lax.fori_loop(early, steps, rotate_chunks, 0)
    get_v.wait()

    def value_chunks(j, _):
        for u in range(2):
            at = pl.multiple_of((2 * j + u) * CHUNK, CHUNK)
            tmp[u] = vraw[pl.ds(pl.multiple_of(2 * at, 2 * CHUNK), 2 * CHUNK), :].astype(F32)
            alive = at + iota((CHUNK, LANES), 0) < live
            ones = jnp.where(alive, 1.0, 0.0).astype(BF16)
            for g in range(kv):
                values = jnp.where(alive, tmp[u, pl.ds(g, CHUNK, stride=kv), :], 0.0)
                vs[g, pl.ds(at, CHUNK), 0:LANES] = values.astype(BF16)
                vs[g, pl.ds(at, CHUNK), LANES:] = ones
        return 0

    lax.fori_loop(0, steps, value_chunks, 0)
    get_wo.wait()

    phase("kv_pieces")
    gathered = own2[x] + rb2[x].astype(F32)
    receive(xr2.at[pl.ds(0, nx - 1)], w1r)
    for k in range(1, nx):
        gathered = gathered + xr2[other_x(k)].astype(F32)
    for t in range(nz):
        g, quarter = t // quarters, t % quarters
        pair = [
            gathered[quarter * tail : (quarter + 1) * tail, at + g * LANES : at + (g + 1) * LANES]
            for at in (0, kc)
        ]
        zs2[t] = jnp.concatenate(pair, 0).astype(BF16)
    for k in z_far:
        b = other_z(k)
        send(zs2.at[b], zr2.at[z], BIG, v1r, z=b)

    phase("z1_wait")
    hear(hear_y.at[0], "y")
    tell(hear_y.at[1], "y")
    total = zs[z].astype(F32)
    receive(zr.at[pl.ds(0, nz - 1)], z1r)
    for k in range(1, nz):
        total = total + zr[other_z(k)].astype(F32)
    receive(sszr.at[pl.ds(0, nz - 1)], zsr)
    for k in range(1, nz):
        squares = squares + sszr[other_z(k)]
    wt[...] = as_columns(lax.rsqrt(squares * (1.0 / d_model) + epsilon))
    which = lax.div(first_token, LANES)
    lane = lax.rem(first_token, LANES)

    def inverse_of(at, size):
        cols = wt[pl.ds(pl.multiple_of(at, 8), size), :]
        picked = cols[:, 0:1]
        for r in range(1, span // LANES):
            picked = jnp.where(which == r, cols[:, r : r + 1], picked)
        return picked

    query = rotated(total * inverse_of(lane, ROWS), q_cos, q_sin) * LANES**-0.5
    qbuf[c, x, z] = query.astype(BF16)

    for k in z_far:
        send(qbuf.at[c, x, z], qbuf.at[c, x, z], BIG, z2r.at[z], z=other_z(k))

    @pl.when(c == 0)
    def _():
        mine = qbuf.at[c, x, z]
        for k in z_far:
            copy(mine, mine, BIG, c2r.at[x], z=other_z(k), c=1).start()
        copy(mine, mine, BIG, c2r.at[x], c=1).start()

    def piece_to_x(t):
        for k in x_far:
            send(qbuf.at[c, x, t], qbuf.at[c, x, t], BIG, x2r.at[x], x=other_x(k))

    piece_to_x(z)

    phase("z2_wait")
    for k in z_near:
        b = other_z(k)
        receive(qbuf.at[c, x, b], z2r.at[b])
        piece_to_x(b)

    def block_to_core(b):
        send(qbuf.at[c, b], qbuf.at[c, b], BIG, c2r.at[b], c=sib)

    @pl.when(c == 1)
    def _():
        copy(qbuf.at[c, x], qbuf.at[c, x], BIG, c2r.at[x], c=sib).start()

    sent[BIG] += heads * ROWS * LANES * 2

    phase("new_keys_wait")
    total = zs2[z].astype(F32)
    receive(zr2.at[pl.ds(0, nz - 1)], v1r)
    for k in range(1, nz):
        total = total + zr2[other_z(k)].astype(F32)
    inv_new = inverse_of(lane + my_quarter * tail, tail)
    new_k = (total[0:tail] * inv_new).astype(BF16).astype(F32)
    new_k = rotated(new_k, k_cos, k_sin)
    new_v = total[tail:] * inv_new
    empty = jnp.zeros((LANES - tail, LANES), F32)
    new_k = jnp.concatenate([new_k, empty], 0).astype(BF16)
    new_v = jnp.concatenate([new_v, empty], 0).astype(BF16)
    new_ones = jnp.where(iota((LANES, LANES), 0) < tail, 1.0, 0.0).astype(BF16)
    for g in range(kv):
        ks[g, slots:, :] = new_k
        vs[g, slots:, 0:LANES] = new_v
        vs[g, slots:, LANES:] = new_ones

    def attend(blocks):
        rows = len(blocks) * block
        token = jnp.concatenate(
            [
                other_x(k) * per_x + cc * ROWS + lax.rem(iota((block, LANES), 0), ROWS)
                for cc, k in blocks
            ],
            0,
        )
        lane = iota((rows, LANES), 1)
        seen = jnp.logical_and(lane < tail, k_first + lane <= token)
        for g in range(kv):
            q = [
                qbuf[cc, other_x(k), g * group : (g + 1) * group].reshape(block, LANES) for cc, k in blocks
            ]
            q = jnp.concatenate(q, 0)
            most = jnp.full((rows, LANES), negative, F32)
            for at in range(0, slots, KEYS):
                score = lax.dot_general(
                    q, ks[g, at : at + KEYS, :], (((1,), (1,)), ((), ())), preferred_element_type=F32
                )
                s_ref[g, :, at : at + KEYS] = score
                for lo in range(0, KEYS, LANES):
                    most = jnp.maximum(most, score[:, lo : lo + LANES])
            score = lax.dot_general(
                q, ks[g, slots:, :], (((1,), (1,)), ((), ())), preferred_element_type=F32
            )
            score = jnp.where(jnp.logical_and(seen, my_g == g), score, negative)
            most = jnp.max(jnp.maximum(most, score), axis=1, keepdims=True)
            acc = jnp.dot(
                jnp.exp(score - most).astype(BF16), vs[g, slots:, :], preferred_element_type=F32
            )
            for at in range(0, slots, KEYS):
                prob = jnp.exp(s_ref[g, :, at : at + KEYS] - most).astype(BF16)
                acc = acc + jnp.dot(prob, vs[g, at : at + KEYS, :], preferred_element_type=F32)
            sums = acc[:, LANES:]
            result = acc[:, 0:LANES] / sums
            lse = most + jnp.log(sums)
            for j, (cc, k) in enumerate(blocks):
                b, cut = other_x(k), slice(j * block, (j + 1) * block)
                if cc is sib:
                    obs[b, g * block : (g + 1) * block, :] = result[cut].astype(BF16)
                    lss[b, g : g + 1, :] = lse[cut].T[0:1]
                else:
                    ob[b, g * block : (g + 1) * block, :] = result[cut]
                    lb[b, g : g + 1, :] = lse[cut].T[0:1]
        for cc, k in blocks:
            if cc is sib:
                b = other_x(k)
                send(obs.at[b], obr.at[b], BIG, c3r.at[b], c=sib)
                send(lss.at[b], lsr.at[b], SMALL, c3lr.at[b], c=sib)

    away = sorted(
        ((i, j) for i in range(nx) for j in range(nz)),
        key=lambda k: -min(k[0], nx - k[0]) - min(k[1], nz - k[1]),
    )

    def join(places):
        weights, blocks = [], [other_x(k) for k in places]
        for b in blocks:
            receive(obr.at[b], c3r.at[b])
            receive(lsr.at[b], c3lr.at[b])
            logs = [lb[b], lsr[b]]
            top = jnp.maximum(*logs)
            lse = top + jnp.log(sum(jnp.exp(v - top) for v in logs))
            weights += [jnp.exp(v - lse) for v in logs]
            lxs[b] = lse
        columns = as_columns(jnp.concatenate(weights, 0))
        for i, b in enumerate(blocks):
            for g in range(kv):
                cut = slice(g * block, (g + 1) * block)
                at = 2 * kv * i + g
                out = columns[:, at : at + 1] * ob[b, cut, :]
                out = out + columns[:, at + kv : at + kv + 1] * obr[b, cut, :].astype(F32)
                oxs[b, g * group : (g + 1) * group] = out.astype(BF16).reshape(group, ROWS, LANES)
        for i, j in away:
            if i in places and (i or j):
                b, t = other_x(i), other_z(j)
                send(oxs.at[b, t], oxr.at[x * nz + z], BIG, x3r, x=b, z=t)
                send(lxs.at[b], lxr.at[x * nz + z], SMALL, x3lr, x=b, z=t)

    middle, final_x = list(range(1, nx - 1)), nx - 1
    phase("c2_wait")
    receive(qbuf.at[sib, x], c2r.at[x])
    phase("unit_0")
    attend([(c, 0), (sib, 0)])
    phase("x2_wait")
    for k in x_near:
        b = other_x(k)
        receive(qbuf.at[c, b], x2r.at[b])
        block_to_core(b)
    for k in x_far:
        send(wobuf.at[x, c], wobuf.at[x, c], WEIGHTS, wr, x=other_x(k))
    send(wobuf.at[x, c], wobuf.at[x, c], WEIGHTS, wcr, c=sib)
    if middle:
        phase("unit_1")
        attend([(c, k) for k in middle])
        phase("c2_wait2")
        for k in middle:
            receive(qbuf.at[sib, other_x(k)], c2r.at[other_x(k)])
        phase("unit_2")
        attend([(sib, k) for k in middle])
    phase("join_0")
    join([0])
    if middle:
        phase("join_1")
        join(middle)
    receive(qbuf.at[sib, other_x(final_x)], c2r.at[other_x(final_x)])
    phase("unit_3")
    attend([(sib, final_x), (c, final_x)])
    phase("join_3")
    join([final_x])
    receive(wobuf.at[pl.ds(0, nx - 1), c], wr)
    for k in range(1, nx):
        b = other_x(k)
        send(wobuf.at[b, c], wobuf.at[b, c], WEIGHTS, wcr, c=sib)

    phase("x3_wait")
    outs, logs = [oxs[x, z]], [lxs[x]]
    receive(oxr.at[pl.ds(0, nx * nz - 1)], x3r)
    receive(lxr.at[pl.ds(0, nx * nz - 1)], x3lr)
    for i, j in away:
        if i or j:
            at = other_x(i) * nz + other_z(j)
            outs.append(oxr[at])
            logs.append(lxr[at])
    phase("combine")
    picked = []
    for v in logs:
        row = v[0:1]
        for g in range(1, kv):
            row = jnp.where(my_g == g, v[g : g + 1], row)
        picked.append(row)
    weights = jnp.concatenate(picked, 0)
    weights = jnp.exp(weights - jnp.max(weights, axis=0, keepdims=True))
    wt[...] = as_columns(weights / jnp.sum(weights, axis=0, keepdims=True))
    mine = wt[pl.ds(pl.multiple_of(my_quarter * ROWS, ROWS), ROWS), :]
    attended = sum(mine[:, i : i + 1] * o.astype(F32) for i, o in enumerate(outs))
    att[z] = attended.astype(BF16)

    for k in z_far:
        send(att.at[z], att.at[z], BIG, z4r, z=other_z(k))

    phase("z4_wait")
    receive(wobuf.at[:, sib], wcr)
    receive(att.at[pl.ds(0, nz - 1)], z4r)

    phase("w_out")
    lhs = jnp.concatenate([att[t] for t in range(heads)], 1)
    rhs = wobuf[...].reshape(nx * nc * HALF, heads * LANES)
    got = lax.dot_general(lhs, rhs, (((1,), (1,)), ((), ())), preferred_element_type=F32)
    low = iota((deep, LANES), 1) < HALF
    for b in range(nx):
        both = got[:, b * LANES : (b + 1) * LANES]
        turned = pltpu.roll(both, HALF, 1)
        p5s[b, 0] = jnp.where(low, both[0:deep], turned[deep:]).astype(BF16)
        p5s[b, 1] = jnp.where(low, turned[0:deep], both[deep:]).astype(BF16)

    me = c * ny + y
    hear(hear_y.at[1], "y")

    def last(b, cc):
        copy(p5s.at[b, cc], p5r.at[me], LAST, y5r, x=b, c=cc, y=x).start()

    for k in x_far:
        for cc in range(nc):
            last(other_x(k), cc)
    last(x, sib)

    @pl.when(x != y)
    def _():
        last(x, c)

    @pl.when(x == y)
    def _():
        p5r[me] = p5s[x, c]

    phase("y5_wait")

    @pl.when(x != y)
    def _():
        receive(p5r, y5r)

    @pl.when(x == y)
    def _():
        receive(p5r.at[pl.ds(0, nc * ny - 1)], y5r)

    for cc in range(nc):
        final = sum(p5r[cc * ny + b].astype(F32) for b in range(ny))
        at = cc * ROWS
        out_ref[at : at + deep, :] = final[:, 0:HALF].astype(BF16)
        out_ref[at + deep : at + ROWS, :] = pltpu.roll(final, HALF, 1)[:, 0:HALF].astype(BF16)

    phase("drain")

    def gone(ref, kind):
        copy(ref, ref, kind, c1r, c=sib).wait_send()

    line = LANES * jnp.dtype(BF16).itemsize
    gone(dummy.at[pl.ds(0, sent[SMALL] // (2 * line))], SMALL)
    gone(kraw.at[pl.ds(0, sent[BIG] // line)], BIG)
    gone(kraw.at[pl.ds(0, sent[WEIGHTS] // line)], WEIGHTS)

    @pl.when(x != y)
    def _():
        gone(p5r, LAST)

    @pl.when(x == y)
    def _():
        gone(p5r.at[pl.ds(0, nc * ny - 1)], LAST)

    phase(None)


def local(
    sizes, hidden_in, norm_gain, w_query, w_key, w_value, w_out, cache_keys, cache_values, lengths, span_start
):
    nx, nz, nc, ny = sizes
    slots, kv, head_dim = cache_keys.shape
    span, depth = hidden_in.shape
    heads = w_query.shape[1] // head_dim
    assert head_dim == LANES and heads == nz and nc == 2 and span == nx * nc * ROWS and nx == ny
    assert w_out.shape[1] == HALF and slots % KEYS == 0 and kv == 2
    cols, cols2 = w_query.shape[1], 2 * w_key.shape[1]
    block = heads * ROWS
    piece = 2 * (ROWS * kv // nz)
    keys = slots + LANES
    rows = 2 * (heads // kv) * ROWS
    lines = span // LANES
    hbm = pl.BlockSpec(memory_space=pltpu.HBM)
    V = pltpu.VMEM
    dma = pltpu.SemaphoreType.DMA
    scratch = [
        pltpu.SMEM(lengths.shape, jnp.int32), pltpu.SMEM(span_start.shape, jnp.int32),
        V((depth, span), BF16), V((1, depth), BF16), V(w_query.shape, BF16), V(w_key.shape, BF16),
        V(w_value.shape, BF16), V((1, LANES), F32),
        V((slots * kv, LANES), BF16), V((slots * kv, LANES), BF16), V((2, CHUNK * kv, LANES), F32),
        V((kv, keys, LANES), BF16), V((kv, keys, 2 * LANES), BF16),
        V((2, slots // CHUNK, LANES), F32), V((2, CHUNK, LANES), F32),
        V((nx, ROWS, cols), BF16), V((nx, ROWS, cols), BF16), V((nx, ROWS, cols), F32),
        V((2 * nx, ROWS // 2, cols), BF16), V((2 * nx, ROWS // 2, cols), BF16),
        V((nz, ROWS, LANES), BF16), V((nz, ROWS, LANES), BF16),
        V((nx, ROWS, cols2), BF16), V((nx, ROWS, cols2), BF16), V((nx, ROWS, cols2), F32),
        V((nx, ROWS, cols2), BF16), V((nx, ROWS, cols2), BF16),
        V((nz, piece, LANES), BF16), V((nz, piece, LANES), BF16),
        V((lines, LANES), F32), V((lines, LANES), F32), V((lines, LANES), F32), V((nx, lines, LANES), F32),
        V((lines, LANES), F32), V((nz, lines, LANES), F32),
        V((nc, nx, heads, ROWS, LANES), BF16), V((kv, rows, slots), F32),
        V((nx, block, LANES), F32), V((nx, kv, LANES), F32),
        V((nx, block, LANES), BF16), V((nx, block, LANES), BF16), V((nx, kv, LANES), F32), V((nx, kv, LANES), F32),
        V((nx, nz, ROWS, LANES), BF16), V((nx * nz, ROWS, LANES), BF16),
        V((nx, kv, LANES), F32), V((nx * nz, kv, LANES), F32),
        V((LANES, LANES), F32),
        V((heads, ROWS, LANES), BF16), V((nx, nc, HALF, w_out.shape[0]), BF16),
        V((nx, nc, ROWS // 2, LANES), BF16), V((nc * ny, ROWS // 2, LANES), BF16),
        V((128, 1, LANES), F32), dma((11,)), dma((4,)),
        pltpu.SemaphoreType.REGULAR, pltpu.SemaphoreType.REGULAR((3,)), pltpu.SemaphoreType.REGULAR((2,)),
        V((ROWS // 2, cols), BF16), V((ROWS // 2, cols), BF16),
        dma, dma, dma, dma, dma, dma, dma, dma, dma, dma,
        dma((nz,)), dma((nx,)), dma((nx,)), dma, dma, dma((nx,)), dma((nx,)), dma, dma, dma, dma,
    ]
    return pl.pallas_call(
        functools.partial(kernel, (nx, nz, nc, ny, nx * nz * nc * depth)),
        out_shape=pltpu.VMEM((nc * ROWS, HALF), BF16),
        in_specs=[hbm] * 11,
        out_specs=pl.BlockSpec(memory_space=pltpu.VMEM),
        scratch_shapes=scratch,
        compiler_params=pltpu.CompilerParams(
            collective_id=0, has_side_effects=True, vmem_limit_bytes=60 * 1024 * 1024
        ),
    )(
        lengths, span_start, hidden_in.T, norm_gain, w_query, w_key, w_value, w_out.T, frequencies(),
        cache_keys.reshape(slots * kv, LANES), cache_values.reshape(slots * kv, LANES),
    )


def solution(mesh):
    physical = mesh.devices.shape
    ny = mesh.shape["head"]
    nc, nz = 2, 8
    nx = physical[0] // (nc * nz)
    finer = Mesh(mesh.devices.reshape(nx, nz, nc, ny), ("x", "z", "c", "y"))
    seq = ("x", "z", "c")
    return jax.shard_map(
        functools.partial(local, (nx, nz, nc, ny)),
        mesh=finer,
        in_specs=(
            P(None, seq), P(None, seq), P(seq, "y"), P(seq, "y"), P(seq, "y"), P("y", seq),
            P(seq, "y", None), P(seq, "y", None), P(), P(),
        ),
        out_specs=P("y", seq),
        check_vma=False,
    )
```

```python
import functools
import math

import jax
import jax.numpy as jnp
import numpy as np
from jax import lax
from jax.experimental import pallas as pl
from jax.experimental.pallas import tpu as pltpu
from jax.sharding import Mesh
from jax.sharding import PartitionSpec as P

F32 = jnp.float32
BF16 = jnp.bfloat16
MESH = pl.DeviceIdType.MESH
LANES = 128
HALF = 64
ROWS = 32
CHUNK = 128
KEYS = 512
SMALL, BIG, WEIGHTS, LAST = range(4)

rope_base = 500000.0
stretch = 64.0
initial_context = 8192.0
ramp_low = 1.0
ramp_high = 32.0
epsilon = 1e-05
negative = -1e30
mscale = 0.1 * math.log(stretch) + 1.0


class Phases:
    def __init__(self):
        self.open = None

    def __call__(self, name):
        if self.open is not None:
            self.open.__exit__(None, None, None)
        self.open = None
        if name:
            self.open = jax.named_scope(name)
            self.open.__enter__()


def frequencies():
    base = rope_base ** (-2.0 * np.arange(HALF) / LANES)
    turns = initial_context * base / (2.0 * math.pi)
    share = np.clip((turns - ramp_low) / (ramp_high - ramp_low), 0.0, 1.0)
    freq = (1.0 - share) * base / stretch + share * base
    return np.concatenate([freq, freq])[None, :].astype(np.float32)


def cos_sin(angles):
    turns = jnp.floor(angles * (1.0 / (2.0 * math.pi)) + 0.5)
    first, second = 6.28125, 253.0 / 2.0**17
    third = 2.0 * math.pi - first - second
    rest = angles - turns * first - turns * second - turns * third
    return jnp.cos(rest), jnp.sin(rest)


def iota(shape, dim):
    return lax.broadcasted_iota(jnp.int32, shape, dim)


def signed(sine):
    return jnp.where(iota(sine.shape, 1) < HALF, -sine, sine)


def rotated(vectors, cosine, sine):
    return vectors * cosine + pltpu.roll(vectors, HALF, 1) * sine


def as_columns(rows):
    spare = LANES - rows.shape[0]
    if spare:
        rows = jnp.concatenate([rows, jnp.zeros((spare, LANES), F32)], 0)
    return rows.T


def kernel(
    dims,
    len_hbm, start_hbm, h_hbm, g_hbm, wq_hbm, wk_hbm, wv_hbm, wo_hbm, freq_hbm, k_hbm, v_hbm,
    out_ref,
    len_ref, start_ref,
    h_ref, g_ref, wq_ref, wk_ref, wv_ref, freq_ref, kraw, vraw, tmp, ks, vs, tab_a, tab_b,
    sb, rb, own, xs, xr, zs, zr, sb2, rb2, own2, xs2, xr2, zs2, zr2,
    ssc, sscr, ssx, ssxr, ssz, sszr, qbuf, s_ref,
    ob, lb, obs, obr, lss, lsr, oxs, oxr, lxs, lxr, wt,
    att, wobuf, p5s, p5r,
    dummy, in_sem, sent_sem,
    hear_x, hear_z, hear_y, rel, merged, relr, c1r, x1r, z1r, d1r, w1r, v1r, csr, xsr, zsr,
    z2r, x2r, c2r, wr, wcr, c3r, c3lr, x3r, x3lr, z4r, y5r,
):
    nx, nz, nc, ny, d_model = dims
    x, z, c, y = (lax.axis_index(n) for n in ("x", "z", "c", "y"))
    sib = 1 - c
    slots = kraw.shape[0] // 2
    group = wq_ref.shape[1] // wk_ref.shape[1]
    kv = wk_ref.shape[1] // LANES
    heads = kv * group
    quarters = nz // kv
    tail = ROWS // quarters
    qc = heads * LANES
    kc = kv * LANES
    per_x = nc * ROWS
    block = group * ROWS
    depth, span = h_ref.shape
    cols = own.shape[2]
    phase = Phases()

    sent = [0, 0, 0, 0]

    def copy(src, dst, kind, recv, **to):
        return pltpu.make_async_remote_copy(
            src_ref=src, dst_ref=dst, send_sem=sent_sem.at[kind], recv_sem=recv,
            device_id=to, device_id_type=MESH,
        )

    def send(src, dst, kind, recv, **to):
        copy(src, dst, kind, recv, **to).start()
        sent[kind] += math.prod(src.shape) * jnp.dtype(src.dtype).itemsize

    def receive(dst, recv):
        copy(dst, dst, SMALL, recv, c=sib).wait_recv()

    def other_x(k):
        return lax.rem(x + k, nx)

    def other_z(k):
        return lax.rem(z + k, nz)

    x_far = sorted(range(1, nx), key=lambda k: -min(k, nx - k))
    z_far = sorted(range(1, nz), key=lambda k: -min(k, nz - k))
    z_near = z_far[::-1]
    x_near = x_far[::-1]

    phase("entry")
    barrier = pltpu.get_barrier_semaphore()

    def greet(**to):
        pl.semaphore_signal(barrier, inc=1, device_id=to, device_id_type=MESH)

    beside = {"x": sorted({1, nx - 1}), "z": sorted({1, nz - 1}), "y": sorted({1, ny - 1})}
    places = {"x": (x, nx), "z": (z, nz), "y": (y, ny)}

    def neighbours(axis):
        at, size = places[axis]
        return [{axis: lax.rem(at + k, size)} for k in beside[axis]]

    for axis in ("z", "x", "y"):
        for to in neighbours(axis):
            greet(**to)
    greet(c=sib)

    def tell(sem, axis):
        for to in neighbours(axis):
            pl.semaphore_signal(sem, inc=1, device_id=to, device_id_type=MESH)

    def hear(sem, axis):
        pl.semaphore_wait(sem, len(beside[axis]))

    fetches = []
    for i, (src, dst) in enumerate(
        (
            (h_hbm, h_ref), (g_hbm, g_ref), (wq_hbm, wq_ref), (wk_hbm, wk_ref), (wv_hbm, wv_ref),
            (freq_hbm, freq_ref), (len_hbm, len_ref), (start_hbm, start_ref),
            (k_hbm, kraw), (v_hbm, vraw), (wo_hbm, wobuf.at[x, c]),
        )
    ):
        fetches.append(pltpu.make_async_copy(src, dst, in_sem.at[i]))
        fetches[-1].start()
    get_h, get_g, get_wq, get_wk, get_wv, get_freq, get_len, get_start, get_k, get_v, get_wo = fetches

    get_h.wait()
    get_g.wait()
    hidden = h_ref[...].astype(F32)
    squares = jnp.sum(hidden * hidden, axis=0, keepdims=True)
    for r in range(span // LANES):
        ssc[r : r + 1, :] = squares[:, r * LANES : (r + 1) * LANES]
    gain = jnp.concatenate([g_ref[...].astype(F32), jnp.zeros((1, LANES - depth), F32)], 1)
    gain = jnp.broadcast_to(gain, (LANES, LANES)).T[0:depth, 0:1]
    scaled = jnp.concatenate([hidden * gain, jnp.zeros((LANES - depth, span), F32)], 0).T
    get_wq.wait()
    get_wk.wait()
    get_wv.wait()

    def rows_of(cc):
        blocks = [
            jnp.where(cc == 0, scaled[b * per_x : b * per_x + ROWS], scaled[b * per_x + ROWS : (b + 1) * per_x])
            for b in range(nx)
        ]
        return jnp.concatenate(blocks, 0)[:, 0:depth].astype(BF16)

    def project(rows, weights, to):
        at = 0
        for w in weights:
            got = jnp.dot(rows, w[...], preferred_element_type=F32)
            for b in range(nx):
                to[b, :, at : at + got.shape[1]] = got[b * ROWS : (b + 1) * ROWS].astype(to.dtype)
            at += got.shape[1]

    project(rows_of(sib), (wq_ref,), sb)
    project(rows_of(sib), (wk_ref, wv_ref), sb2)

    phase("barrier")
    pl.semaphore_wait(barrier, 1 + sum(len(beside[axis]) for axis in beside))
    tell(hear_x, "x")
    tell(hear_z.at[0], "z")

    phase("core1_project")
    for b in range(nx):
        send(sb.at[b], rb.at[b], BIG, c1r, c=sib)
    send(ssc, sscr, SMALL, csr, c=sib)
    for b in range(nx):
        send(sb2.at[b], rb2.at[b], BIG, d1r, c=sib)

    project(rows_of(c), (wq_ref,), own)
    project(rows_of(c), (wk_ref, wv_ref), own2)
    get_freq.wait()
    freq = freq_ref[...]

    phase("core1_wait")
    receive(rb, c1r)
    hear(hear_x, "x")
    hear(hear_z.at[0], "z")
    tell(hear_z.at[1], "z")
    relayed = nx == 4
    deep = ROWS // 2
    for k in x_far:
        b = other_x(k)
        sums = (own[b] + rb[b].astype(F32)).astype(BF16)
        xs[2 * b] = sums[0:deep]
        xs[2 * b + 1] = sums[deep:]
        send(xs.at[2 * b], xr.at[2 * x], BIG, x1r, x=b)
        if relayed and k > 1:
            def direct():
                copy(xs.at[2 * b + 1], xr.at[2 * x + 1], BIG, x1r, x=b).start()

            pl.when(c == 0)(direct)
            if k == 2:

                @pl.when(c == 1)
                def _():
                    copy(xs.at[2 * b + 1], rel, BIG, relr, x=other_x(3)).start()

            sent[BIG] += deep * cols * 2
        else:
            send(xs.at[2 * b + 1], xr.at[2 * x + 1], BIG, x1r, x=b)
    receive(sscr, csr)
    ssx[...] = ssc[...] + sscr[...]
    for k in x_far:
        send(ssx, ssxr.at[x], SMALL, xsr, x=other_x(k))

    phase("keys")
    get_len.wait()
    get_start.wait()
    my = (x * nz + z) * nc + c
    count = nx * nz * nc

    def add_lengths(r, carry):
        before, total = carry
        return before + jnp.where(r < my, len_ref[r], 0), total + len_ref[r]

    offset, first_pos = lax.fori_loop(0, count, add_lengths, (jnp.int32(0), jnp.int32(0)))
    first_pos = first_pos + start_ref[0]
    live = len_ref[my]

    a_count = slots // CHUNK
    a_pos = (offset + CHUNK * iota((a_count, LANES), 0)).astype(F32)
    a_cos, a_sin = cos_sin(a_pos * freq)
    tab_a[0] = a_cos * mscale
    tab_a[1] = a_sin * mscale
    b_cos, b_sin = cos_sin(iota((CHUNK, LANES), 0).astype(F32) * freq)
    tab_b[0] = b_cos
    tab_b[1] = b_sin
    first_token = x * per_x + c * ROWS
    my_g, my_quarter = lax.div(z, quarters), lax.rem(z, quarters)
    k_first = first_token + my_quarter * tail
    q_pos = (first_pos + first_token + iota((ROWS, LANES), 0)).astype(F32)
    q_cos, q_sin = cos_sin(q_pos * freq)
    k_pos = (first_pos + k_first + iota((tail, LANES), 0)).astype(F32)
    k_cos, k_sin = cos_sin(k_pos * freq)
    q_cos, q_sin = q_cos * mscale, signed(q_sin * mscale)
    k_cos, k_sin = k_cos * mscale, signed(k_sin * mscale)

    get_k.wait()

    def slot_angles(a, size):
        cos_a = tab_a[0, pl.ds(a, 1), :]
        sin_a = tab_a[1, pl.ds(a, 1), :]
        cos_b, sin_b = tab_b[0, 0:size, :], tab_b[1, 0:size, :]
        return cos_a * cos_b - sin_a * sin_b, signed(sin_a * cos_b + cos_a * sin_b)

    tmp[0, 0 : 8 * kv, :] = kraw[0 : 8 * kv, :].astype(F32)
    slot_cos, slot_sin = slot_angles(0, 8)
    head_keys = [
        rotated(tmp[0, pl.ds(g, 8, stride=kv), :], slot_cos, slot_sin)[0:1] for g in range(kv)
    ]

    def rotate_chunks(j, _):
        for u in range(2):
            a = 2 * j + u
            at = pl.multiple_of(a * CHUNK, CHUNK)
            tmp[u] = kraw[pl.ds(pl.multiple_of(2 * at, 2 * CHUNK), 2 * CHUNK), :].astype(F32)
            cosine, sine = slot_angles(a, CHUNK)
            alive = at + iota((CHUNK, LANES), 0) < live
            for g in range(kv):
                keys = rotated(tmp[u, pl.ds(g, CHUNK, stride=kv), :], cosine, sine)
                ks[g, pl.ds(at, CHUNK), :] = jnp.where(alive, keys, head_keys[g]).astype(BF16)
        return 0

    steps = a_count // 2
    early = steps * 3 // 4
    lax.fori_loop(0, early, rotate_chunks, 0)

    phase("x1_wait")
    hear(hear_z.at[1], "z")
    tell(hear_z.at[2], "z")
    gathered = own[x] + rb[x].astype(F32)
    if relayed:

        @pl.when(c == 1)
        def _():
            b = other_x(3)
            receive(rel, relr)
            merged[...] = (own[b, deep:] + rb[b, deep:].astype(F32) + rel[...].astype(F32)).astype(BF16)
            copy(merged, xr.at[2 * x + 1], BIG, x1r, x=b).start()
            receive(xr.at[pl.ds(0, 2 * nx - 3)], x1r)

        @pl.when(c == 0)
        def _():
            receive(xr.at[pl.ds(0, 2 * nx - 2)], x1r)

    else:
        receive(xr.at[pl.ds(0, 2 * nx - 2)], x1r)
    for k in range(1, nx):
        b = other_x(k)
        second = xr[2 * b + 1].astype(F32)
        if relayed and k == 2:
            second = jnp.where(c == 0, second, 0.0)
        gathered = gathered + jnp.concatenate([xr[2 * b].astype(F32), second], 0)
    tell(hear_y.at[0], "y")
    hear(hear_z.at[2], "z")
    for t in range(nz):
        zs[t] = gathered[:, t * LANES : (t + 1) * LANES].astype(BF16)
    for k in z_far:
        b = other_z(k)
        send(zs.at[b], zr.at[z], BIG, z1r, z=b)
    squares = ssx[...]
    receive(ssxr.at[pl.ds(0, nx - 1)], xsr)
    for k in range(1, nx):
        squares = squares + ssxr[other_x(k)]
    ssz[...] = squares
    for k in z_far:
        send(ssz, sszr.at[z], SMALL, zsr, z=other_z(k))

    receive(rb2, d1r)
    for k in x_far:
        b = other_x(k)
        xs2[b] = (own2[b] + rb2[b].astype(F32)).astype(BF16)
        send(xs2.at[b], xr2.at[x], BIG, w1r, x=b)

    phase("values")
    lax.fori_loop(early, steps, rotate_chunks, 0)
    get_v.wait()

    def value_chunks(j, _):
        for u in range(2):
            at = pl.multiple_of((2 * j + u) * CHUNK, CHUNK)
            tmp[u] = vraw[pl.ds(pl.multiple_of(2 * at, 2 * CHUNK), 2 * CHUNK), :].astype(F32)
            alive = at + iota((CHUNK, LANES), 0) < live
            ones = jnp.where(alive, 1.0, 0.0).astype(BF16)
            for g in range(kv):
                values = jnp.where(alive, tmp[u, pl.ds(g, CHUNK, stride=kv), :], 0.0)
                vs[g, pl.ds(at, CHUNK), 0:LANES] = values.astype(BF16)
                vs[g, pl.ds(at, CHUNK), LANES:] = ones
        return 0

    lax.fori_loop(0, steps, value_chunks, 0)
    get_wo.wait()

    phase("kv_pieces")
    gathered = own2[x] + rb2[x].astype(F32)
    receive(xr2.at[pl.ds(0, nx - 1)], w1r)
    for k in range(1, nx):
        gathered = gathered + xr2[other_x(k)].astype(F32)
    for t in range(nz):
        g, quarter = t // quarters, t % quarters
        pair = [
            gathered[quarter * tail : (quarter + 1) * tail, at + g * LANES : at + (g + 1) * LANES]
            for at in (0, kc)
        ]
        zs2[t] = jnp.concatenate(pair, 0).astype(BF16)
    for k in z_far:
        b = other_z(k)
        send(zs2.at[b], zr2.at[z], BIG, v1r, z=b)

    phase("z1_wait")
    hear(hear_y.at[0], "y")
    tell(hear_y.at[1], "y")
    total = zs[z].astype(F32)
    receive(zr.at[pl.ds(0, nz - 1)], z1r)
    for k in range(1, nz):
        total = total + zr[other_z(k)].astype(F32)
    receive(sszr.at[pl.ds(0, nz - 1)], zsr)
    for k in range(1, nz):
        squares = squares + sszr[other_z(k)]
    wt[...] = as_columns(lax.rsqrt(squares * (1.0 / d_model) + epsilon))
    which = lax.div(first_token, LANES)
    lane = lax.rem(first_token, LANES)

    def inverse_of(at, size):
        cols = wt[pl.ds(pl.multiple_of(at, 8), size), :]
        picked = cols[:, 0:1]
        for r in range(1, span // LANES):
            picked = jnp.where(which == r, cols[:, r : r + 1], picked)
        return picked

    query = rotated(total * inverse_of(lane, ROWS), q_cos, q_sin) * LANES**-0.5
    qbuf[c, x, z] = query.astype(BF16)

    for k in z_far:
        send(qbuf.at[c, x, z], qbuf.at[c, x, z], BIG, z2r.at[z], z=other_z(k))

    @pl.when(c == 0)
    def _():
        mine = qbuf.at[c, x, z]
        for k in z_far:
            copy(mine, mine, BIG, c2r.at[x], z=other_z(k), c=1).start()
        copy(mine, mine, BIG, c2r.at[x], c=1).start()

    def piece_to_x(t):
        for k in x_far:
            send(qbuf.at[c, x, t], qbuf.at[c, x, t], BIG, x2r.at[x], x=other_x(k))

    piece_to_x(z)

    phase("z2_wait")
    for k in z_near:
        b = other_z(k)
        receive(qbuf.at[c, x, b], z2r.at[b])
        piece_to_x(b)

    def block_to_core(b):
        send(qbuf.at[c, b], qbuf.at[c, b], BIG, c2r.at[b], c=sib)

    @pl.when(c == 1)
    def _():
        copy(qbuf.at[c, x], qbuf.at[c, x], BIG, c2r.at[x], c=sib).start()

    sent[BIG] += heads * ROWS * LANES * 2

    phase("new_keys_wait")
    total = zs2[z].astype(F32)
    receive(zr2.at[pl.ds(0, nz - 1)], v1r)
    for k in range(1, nz):
        total = total + zr2[other_z(k)].astype(F32)
    inv_new = inverse_of(lane + my_quarter * tail, tail)
    new_k = (total[0:tail] * inv_new).astype(BF16).astype(F32)
    new_k = rotated(new_k, k_cos, k_sin)
    new_v = total[tail:] * inv_new
    empty = jnp.zeros((LANES - tail, LANES), F32)
    new_k = jnp.concatenate([new_k, empty], 0).astype(BF16)
    new_v = jnp.concatenate([new_v, empty], 0).astype(BF16)
    new_ones = jnp.where(iota((LANES, LANES), 0) < tail, 1.0, 0.0).astype(BF16)
    for g in range(kv):
        ks[g, slots:, :] = new_k
        vs[g, slots:, 0:LANES] = new_v
        vs[g, slots:, LANES:] = new_ones

    def attend(blocks):
        rows = len(blocks) * block
        token = jnp.concatenate(
            [
                other_x(k) * per_x + cc * ROWS + lax.rem(iota((block, LANES), 0), ROWS)
                for cc, k in blocks
            ],
            0,
        )
        lane = iota((rows, LANES), 1)
        seen = jnp.logical_and(lane < tail, k_first + lane <= token)
        for g in range(kv):
            q = [
                qbuf[cc, other_x(k), g * group : (g + 1) * group].reshape(block, LANES) for cc, k in blocks
            ]
            q = jnp.concatenate(q, 0)
            most = jnp.full((rows, LANES), negative, F32)
            for at in range(0, slots, KEYS):
                score = lax.dot_general(
                    q, ks[g, at : at + KEYS, :], (((1,), (1,)), ((), ())), preferred_element_type=F32
                )
                s_ref[g, :, at : at + KEYS] = score
                for lo in range(0, KEYS, LANES):
                    most = jnp.maximum(most, score[:, lo : lo + LANES])
            score = lax.dot_general(
                q, ks[g, slots:, :], (((1,), (1,)), ((), ())), preferred_element_type=F32
            )
            score = jnp.where(jnp.logical_and(seen, my_g == g), score, negative)
            most = jnp.max(jnp.maximum(most, score), axis=1, keepdims=True)
            acc = jnp.dot(
                jnp.exp(score - most).astype(BF16), vs[g, slots:, :], preferred_element_type=F32
            )
            for at in range(0, slots, KEYS):
                prob = jnp.exp(s_ref[g, :, at : at + KEYS] - most).astype(BF16)
                acc = acc + jnp.dot(prob, vs[g, at : at + KEYS, :], preferred_element_type=F32)
            sums = acc[:, LANES:]
            result = acc[:, 0:LANES] / sums
            lse = most + jnp.log(sums)
            for j, (cc, k) in enumerate(blocks):
                b, cut = other_x(k), slice(j * block, (j + 1) * block)
                if cc is sib:
                    obs[b, g * block : (g + 1) * block, :] = result[cut].astype(BF16)
                    lss[b, g : g + 1, :] = lse[cut].T[0:1]
                else:
                    ob[b, g * block : (g + 1) * block, :] = result[cut]
                    lb[b, g : g + 1, :] = lse[cut].T[0:1]
        for cc, k in blocks:
            if cc is sib:
                b = other_x(k)
                send(obs.at[b], obr.at[b], BIG, c3r.at[b], c=sib)
                send(lss.at[b], lsr.at[b], SMALL, c3lr.at[b], c=sib)

    away = sorted(
        ((i, j) for i in range(nx) for j in range(nz)),
        key=lambda k: -min(k[0], nx - k[0]) - min(k[1], nz - k[1]),
    )

    def join(places):
        weights, blocks = [], [other_x(k) for k in places]
        for b in blocks:
            receive(obr.at[b], c3r.at[b])
            receive(lsr.at[b], c3lr.at[b])
            logs = [lb[b], lsr[b]]
            top = jnp.maximum(*logs)
            lse = top + jnp.log(sum(jnp.exp(v - top) for v in logs))
            weights += [jnp.exp(v - lse) for v in logs]
            lxs[b] = lse
        columns = as_columns(jnp.concatenate(weights, 0))
        for i, b in enumerate(blocks):
            for g in range(kv):
                cut = slice(g * block, (g + 1) * block)
                at = 2 * kv * i + g
                out = columns[:, at : at + 1] * ob[b, cut, :]
                out = out + columns[:, at + kv : at + kv + 1] * obr[b, cut, :].astype(F32)
                oxs[b, g * group : (g + 1) * group] = out.astype(BF16).reshape(group, ROWS, LANES)
        slot = c * nx * nz + x * nz + z
        for i, j in away:
            if i in places and (i or j):
                b, t = other_x(i), other_z(j)
                send(oxs.at[b, t], oxr.at[slot], BIG, x3r, x=b, z=t, c=1)
                send(lxs.at[b], lxr.at[slot], SMALL, x3lr, x=b, z=t, c=1)
        if 0 in places:

            @pl.when(c == 0)
            def _():
                copy(oxs.at[x, z], oxr.at[slot], BIG, x3r, c=1).start()
                copy(lxs.at[x], lxr.at[slot], SMALL, x3lr, c=1).start()

            @pl.when(c == 1)
            def _():
                oxr[slot] = oxs[x, z]
                lxr[slot] = lxs[x]

    middle, final_x = list(range(1, nx - 1)), nx - 1
    phase("c2_wait")
    receive(qbuf.at[sib, x], c2r.at[x])
    phase("unit_0")
    attend([(c, 0), (sib, 0)])
    phase("x2_wait")
    for k in x_near:
        b = other_x(k)
        receive(qbuf.at[c, b], x2r.at[b])
        block_to_core(b)
    for k in x_far:
        send(wobuf.at[x, c], wobuf.at[x, c], WEIGHTS, wr, x=other_x(k))
    send(wobuf.at[x, c], wobuf.at[x, c], WEIGHTS, wcr, c=sib)
    if middle:
        phase("unit_1")
        attend([(c, k) for k in middle])
        phase("c2_wait2")
        for k in middle:
            receive(qbuf.at[sib, other_x(k)], c2r.at[other_x(k)])
        phase("unit_2")
        attend([(sib, k) for k in middle])
    phase("join_0")
    join([0])
    if middle:
        phase("join_1")
        join(middle)
    receive(qbuf.at[sib, other_x(final_x)], c2r.at[other_x(final_x)])
    phase("unit_3")
    attend([(sib, final_x), (c, final_x)])
    phase("join_3")
    join([final_x])
    receive(wobuf.at[pl.ds(0, nx - 1), c], wr)
    for k in range(1, nx):
        b = other_x(k)
        send(wobuf.at[b, c], wobuf.at[b, c], WEIGHTS, wcr, c=sib)

    phase("tail")
    hear(hear_y.at[1], "y")
    receive(wobuf.at[:, sib], wcr)

    def last(b, cc):
        copy(p5s.at[b, cc], p5r.at[y], LAST, y5r, x=b, c=cc, y=x).start()

    def finish():
        sources = nx * nz
        receive(oxr.at[pl.ds(0, 2 * sources - 1)], x3r)
        receive(lxr.at[pl.ds(0, 2 * sources - 1)], x3lr)
        shares = []
        for cc in range(nc):
            picked = []
            for i in range(sources):
                v = lxr[cc * sources + i]
                row = v[0:1]
                for g in range(1, kv):
                    row = jnp.where(my_g == g, v[g : g + 1], row)
                picked.append(row)
            logs = jnp.concatenate(picked, 0)
            logs = jnp.exp(logs - jnp.max(logs, axis=0, keepdims=True))
            shares.append(logs / jnp.sum(logs, axis=0, keepdims=True))
        wt[...] = as_columns(jnp.concatenate(shares, 0))
        mine = wt[pl.ds(pl.multiple_of(my_quarter * ROWS, ROWS), ROWS), :]
        for cc in range(nc):
            span_of = range(cc * sources, (cc + 1) * sources)
            attended = sum(mine[:, i : i + 1] * oxr[i].astype(F32) for i in span_of)
            att[z, cc * ROWS : (cc + 1) * ROWS, :] = attended.astype(BF16)
        for k in z_far:
            copy(att.at[z], att.at[z], BIG, z4r, z=other_z(k)).start()
        receive(att.at[pl.ds(0, nz - 1)], z4r)

        lhs = jnp.concatenate([att[t] for t in range(heads)], 1)
        rhs = wobuf[...].reshape(nx * nc * HALF, heads * LANES)
        got = lax.dot_general(lhs, rhs, (((1,), (1,)), ((), ())), preferred_element_type=F32)
        low = iota((ROWS, LANES), 1) < HALF
        for b in range(nx):
            both = got[:, b * LANES : (b + 1) * LANES]
            turned = pltpu.roll(both, HALF, 1)
            p5s[b, 0] = jnp.where(low, both[0:ROWS], turned[ROWS:]).astype(BF16)
            p5s[b, 1] = jnp.where(low, turned[0:ROWS], both[ROWS:]).astype(BF16)
        for k in x_far:
            for cc in range(nc):
                last(other_x(k), cc)
        last(x, 0)

        @pl.when(x != y)
        def _():
            last(x, 1)

        @pl.when(x == y)
        def _():
            p5r[y] = p5s[x, 1]

    pl.when(c == 1)(finish)

    phase("y5_wait")
    own_piece = jnp.logical_and(x == y, c == 1)

    @pl.when(jnp.logical_not(own_piece))
    def _():
        receive(p5r, y5r)

    @pl.when(own_piece)
    def _():
        receive(p5r.at[pl.ds(0, ny - 1)], y5r)

    final = sum(p5r[b].astype(F32) for b in range(ny))
    out_ref[0:ROWS, :] = final[:, 0:HALF].astype(BF16)
    out_ref[ROWS:, :] = pltpu.roll(final, HALF, 1)[:, 0:HALF].astype(BF16)

    phase("drain")

    def gone(ref, kind):
        copy(ref, ref, kind, c1r, c=sib).wait_send()

    line = LANES * jnp.dtype(BF16).itemsize
    piece = ROWS * LANES * 2

    @pl.when(c == 0)
    def _():
        gone(dummy.at[pl.ds(0, (sent[SMALL] + kv * LANES * 4) // (2 * line))], SMALL)
        gone(kraw.at[pl.ds(0, (sent[BIG] + piece) // line)], BIG)

    @pl.when(c == 1)
    def _():
        gone(dummy.at[pl.ds(0, sent[SMALL] // (2 * line))], SMALL)
        gone(kraw.at[pl.ds(0, (sent[BIG] + (nz - 1) * nc * piece) // line)], BIG)

    gone(kraw.at[pl.ds(0, sent[WEIGHTS] // line)], WEIGHTS)

    @pl.when(jnp.logical_and(c == 1, x != y))
    def _():
        gone(kraw.at[pl.ds(0, nx * nc * piece // line)], LAST)

    @pl.when(own_piece)
    def _():
        gone(kraw.at[pl.ds(0, (nx * nc - 1) * piece // line)], LAST)

    phase(None)


def local(
    sizes, hidden_in, norm_gain, w_query, w_key, w_value, w_out, cache_keys, cache_values, lengths, span_start
):
    nx, nz, nc, ny = sizes
    slots, kv, head_dim = cache_keys.shape
    span, depth = hidden_in.shape
    heads = w_query.shape[1] // head_dim
    assert head_dim == LANES and heads == nz and nc == 2 and span == nx * nc * ROWS and nx == ny
    assert w_out.shape[1] == HALF and slots % KEYS == 0 and kv == 2
    cols, cols2 = w_query.shape[1], 2 * w_key.shape[1]
    block = heads * ROWS
    piece = 2 * (ROWS * kv // nz)
    keys = slots + LANES
    rows = 2 * (heads // kv) * ROWS
    lines = span // LANES
    hbm = pl.BlockSpec(memory_space=pltpu.HBM)
    V = pltpu.VMEM
    dma = pltpu.SemaphoreType.DMA
    scratch = [
        pltpu.SMEM(lengths.shape, jnp.int32), pltpu.SMEM(span_start.shape, jnp.int32),
        V((depth, span), BF16), V((1, depth), BF16), V(w_query.shape, BF16), V(w_key.shape, BF16),
        V(w_value.shape, BF16), V((1, LANES), F32),
        V((slots * kv, LANES), BF16), V((slots * kv, LANES), BF16), V((2, CHUNK * kv, LANES), F32),
        V((kv, keys, LANES), BF16), V((kv, keys, 2 * LANES), BF16),
        V((2, slots // CHUNK, LANES), F32), V((2, CHUNK, LANES), F32),
        V((nx, ROWS, cols), BF16), V((nx, ROWS, cols), BF16), V((nx, ROWS, cols), F32),
        V((2 * nx, ROWS // 2, cols), BF16), V((2 * nx, ROWS // 2, cols), BF16),
        V((nz, ROWS, LANES), BF16), V((nz, ROWS, LANES), BF16),
        V((nx, ROWS, cols2), BF16), V((nx, ROWS, cols2), BF16), V((nx, ROWS, cols2), F32),
        V((nx, ROWS, cols2), BF16), V((nx, ROWS, cols2), BF16),
        V((nz, piece, LANES), BF16), V((nz, piece, LANES), BF16),
        V((lines, LANES), F32), V((lines, LANES), F32), V((lines, LANES), F32), V((nx, lines, LANES), F32),
        V((lines, LANES), F32), V((nz, lines, LANES), F32),
        V((nc, nx, heads, ROWS, LANES), BF16), V((kv, rows, slots), F32),
        V((nx, block, LANES), F32), V((nx, kv, LANES), F32),
        V((nx, block, LANES), BF16), V((nx, block, LANES), BF16), V((nx, kv, LANES), F32), V((nx, kv, LANES), F32),
        V((nx, nz, ROWS, LANES), BF16), V((nc * nx * nz, ROWS, LANES), BF16),
        V((nx, kv, LANES), F32), V((nc * nx * nz, kv, LANES), F32),
        V((LANES, LANES), F32),
        V((heads, nc * ROWS, LANES), BF16), V((nx, nc, HALF, w_out.shape[0]), BF16),
        V((nx, nc, ROWS, LANES), BF16), V((ny, ROWS, LANES), BF16),
        V((128, 1, LANES), F32), dma((11,)), dma((4,)),
        pltpu.SemaphoreType.REGULAR, pltpu.SemaphoreType.REGULAR((3,)), pltpu.SemaphoreType.REGULAR((2,)),
        V((ROWS // 2, cols), BF16), V((ROWS // 2, cols), BF16),
        dma, dma, dma, dma, dma, dma, dma, dma, dma, dma,
        dma((nz,)), dma((nx,)), dma((nx,)), dma, dma, dma((nx,)), dma((nx,)), dma, dma, dma, dma,
    ]
    return pl.pallas_call(
        functools.partial(kernel, (nx, nz, nc, ny, nx * nz * nc * depth)),
        out_shape=pltpu.VMEM((nc * ROWS, HALF), BF16),
        in_specs=[hbm] * 11,
        out_specs=pl.BlockSpec(memory_space=pltpu.VMEM),
        scratch_shapes=scratch,
        compiler_params=pltpu.CompilerParams(
            collective_id=0, has_side_effects=True, vmem_limit_bytes=60 * 1024 * 1024
        ),
    )(
        lengths, span_start, hidden_in.T, norm_gain, w_query, w_key, w_value, w_out.T, frequencies(),
        cache_keys.reshape(slots * kv, LANES), cache_values.reshape(slots * kv, LANES),
    )


def solution(mesh):
    physical = mesh.devices.shape
    ny = mesh.shape["head"]
    nc, nz = 2, 8
    nx = physical[0] // (nc * nz)
    finer = Mesh(mesh.devices.reshape(nx, nz, nc, ny), ("x", "z", "c", "y"))
    seq = ("x", "z", "c")
    return jax.shard_map(
        functools.partial(local, (nx, nz, nc, ny)),
        mesh=finer,
        in_specs=(
            P(None, seq), P(None, seq), P(seq, "y"), P(seq, "y"), P(seq, "y"), P("y", seq),
            P(seq, "y", None), P(seq, "y", None), P(), P(),
        ),
        out_specs=P("y", seq),
        check_vma=False,
    )
```

```python
import functools
import math

import jax
import jax.numpy as jnp
import numpy as np
from jax import lax
from jax.experimental import pallas as pl
from jax.experimental.pallas import tpu as pltpu
from jax.sharding import Mesh
from jax.sharding import PartitionSpec as P

F32 = jnp.float32
BF16 = jnp.bfloat16
MESH = pl.DeviceIdType.MESH
LANES = 128
HALF = 64
ROWS = 32
CHUNK = 128
KEYS = 1024
SMALL, BIG, WEIGHTS, LAST = range(4)

rope_base = 500000.0
stretch = 64.0
initial_context = 8192.0
ramp_low = 1.0
ramp_high = 32.0
epsilon = 1e-05
negative = -1e30
mscale = 0.1 * math.log(stretch) + 1.0


class Phases:
    def __init__(self):
        self.open = None

    def __call__(self, name):
        if self.open is not None:
            self.open.__exit__(None, None, None)
        self.open = None
        if name:
            self.open = jax.named_scope(name)
            self.open.__enter__()


def frequencies():
    base = rope_base ** (-2.0 * np.arange(HALF) / LANES)
    turns = initial_context * base / (2.0 * math.pi)
    share = np.clip((turns - ramp_low) / (ramp_high - ramp_low), 0.0, 1.0)
    freq = (1.0 - share) * base / stretch + share * base
    return np.concatenate([freq, freq])[None, :].astype(np.float32)


def cos_sin(angles):
    turns = jnp.floor(angles * (1.0 / (2.0 * math.pi)) + 0.5)
    first, second = 6.28125, 253.0 / 2.0**17
    third = 2.0 * math.pi - first - second
    rest = angles - turns * first - turns * second - turns * third
    return jnp.cos(rest), jnp.sin(rest)


def iota(shape, dim):
    return lax.broadcasted_iota(jnp.int32, shape, dim)


def signed(sine):
    return jnp.where(iota(sine.shape, 1) < HALF, -sine, sine)


def rotated(vectors, cosine, sine):
    return vectors * cosine + pltpu.roll(vectors, HALF, 1) * sine


def as_columns(rows):
    spare = LANES - rows.shape[0]
    if spare:
        rows = jnp.concatenate([rows, jnp.zeros((spare, LANES), F32)], 0)
    return rows.T


def kernel(
    dims,
    len_hbm, start_hbm, h_hbm, g_hbm, wq_hbm, wk_hbm, wv_hbm, wo_hbm, freq_hbm, k_hbm, v_hbm,
    out_ref,
    len_ref, start_ref,
    h_ref, g_ref, wq_ref, wk_ref, wv_ref, freq_ref, kraw, vraw, tmp, ks, vs, tab_a, tab_b,
    sb, rb, own, xs, xr, zs, zr, sb2, rb2, own2, xs2, xr2, zs2, zr2,
    ssc, sscr, ssx, ssxr, ssz, sszr, qbuf, s_ref,
    ob, lb, obs, obr, lss, lsr, oxs, oxr, lxs, lxr, wt,
    att, wobuf, p5s, p5r,
    dummy, in_sem, sent_sem,
    hear_x, hear_z, hear_y, rel, merged, relr, c1r, x1r, z1r, d1r, w1r, v1r, csr, xsr, zsr,
    z2r, x2r, c2r, wr, wcr, c3r, c3lr, x3r, x3lr, z4r, y5r,
):
    nx, nz, nc, ny, d_model = dims
    x, z, c, y = (lax.axis_index(n) for n in ("x", "z", "c", "y"))
    sib = 1 - c
    slots = kraw.shape[0] // 2
    group = wq_ref.shape[1] // wk_ref.shape[1]
    kv = wk_ref.shape[1] // LANES
    heads = kv * group
    quarters = nz // kv
    tail = ROWS // quarters
    qc = heads * LANES
    kc = kv * LANES
    per_x = nc * ROWS
    block = group * ROWS
    depth, span = h_ref.shape
    cols = own.shape[2]
    phase = Phases()

    sent = [0, 0, 0, 0]

    def copy(src, dst, kind, recv, **to):
        return pltpu.make_async_remote_copy(
            src_ref=src, dst_ref=dst, send_sem=sent_sem.at[kind], recv_sem=recv,
            device_id=to, device_id_type=MESH,
        )

    def send(src, dst, kind, recv, **to):
        copy(src, dst, kind, recv, **to).start()
        sent[kind] += math.prod(src.shape) * jnp.dtype(src.dtype).itemsize

    def receive(dst, recv):
        copy(dst, dst, SMALL, recv, c=sib).wait_recv()

    def other_x(k):
        return lax.rem(x + k, nx)

    def other_z(k):
        return lax.rem(z + k, nz)

    x_far = sorted(range(1, nx), key=lambda k: -min(k, nx - k))
    z_far = sorted(range(1, nz), key=lambda k: -min(k, nz - k))
    z_near = z_far[::-1]
    x_near = x_far[::-1]

    phase("entry")
    barrier = pltpu.get_barrier_semaphore()

    def greet(**to):
        pl.semaphore_signal(barrier, inc=1, device_id=to, device_id_type=MESH)

    beside = {"x": sorted({1, nx - 1}), "z": sorted({1, nz - 1}), "y": sorted({1, ny - 1})}
    places = {"x": (x, nx), "z": (z, nz), "y": (y, ny)}

    def neighbours(axis):
        at, size = places[axis]
        return [{axis: lax.rem(at + k, size)} for k in beside[axis]]

    for axis in ("z", "x", "y"):
        for to in neighbours(axis):
            greet(**to)
    greet(c=sib)

    def tell(sem, axis):
        for to in neighbours(axis):
            pl.semaphore_signal(sem, inc=1, device_id=to, device_id_type=MESH)

    def hear(sem, axis):
        pl.semaphore_wait(sem, len(beside[axis]))

    fetches = []
    for i, (src, dst) in enumerate(
        (
            (h_hbm, h_ref), (g_hbm, g_ref), (wq_hbm, wq_ref), (wk_hbm, wk_ref), (wv_hbm, wv_ref),
            (freq_hbm, freq_ref), (len_hbm, len_ref), (start_hbm, start_ref),
            (k_hbm, kraw), (v_hbm, vraw), (wo_hbm, wobuf.at[x, c]),
        )
    ):
        fetches.append(pltpu.make_async_copy(src, dst, in_sem.at[i]))
        fetches[-1].start()
    get_h, get_g, get_wq, get_wk, get_wv, get_freq, get_len, get_start, get_k, get_v, get_wo = fetches

    get_h.wait()
    get_g.wait()
    hidden = h_ref[...].astype(F32)
    squares = jnp.sum(hidden * hidden, axis=0, keepdims=True)
    for r in range(span // LANES):
        ssc[r : r + 1, :] = squares[:, r * LANES : (r + 1) * LANES]
    gain = jnp.concatenate([g_ref[...].astype(F32), jnp.zeros((1, LANES - depth), F32)], 1)
    gain = jnp.broadcast_to(gain, (LANES, LANES)).T[0:depth, 0:1]
    scaled = jnp.concatenate([hidden * gain, jnp.zeros((LANES - depth, span), F32)], 0).T
    get_wq.wait()
    get_wk.wait()
    get_wv.wait()

    def rows_of(cc):
        blocks = [
            jnp.where(cc == 0, scaled[b * per_x : b * per_x + ROWS], scaled[b * per_x + ROWS : (b + 1) * per_x])
            for b in range(nx)
        ]
        return jnp.concatenate(blocks, 0)[:, 0:depth].astype(BF16)

    def project(rows, weights, to):
        at = 0
        for w in weights:
            got = jnp.dot(rows, w[...], preferred_element_type=F32)
            for b in range(nx):
                to[b, :, at : at + got.shape[1]] = got[b * ROWS : (b + 1) * ROWS].astype(to.dtype)
            at += got.shape[1]

    project(rows_of(sib), (wq_ref,), sb)
    project(rows_of(sib), (wk_ref, wv_ref), sb2)

    phase("barrier")
    pl.semaphore_wait(barrier, 1 + sum(len(beside[axis]) for axis in beside))
    tell(hear_x, "x")
    tell(hear_z.at[0], "z")

    phase("core1_project")
    for b in range(nx):
        send(sb.at[b], rb.at[b], BIG, c1r, c=sib)
    send(ssc, sscr, SMALL, csr, c=sib)
    for b in range(nx):
        send(sb2.at[b], rb2.at[b], BIG, d1r, c=sib)

    project(rows_of(c), (wq_ref,), own)
    project(rows_of(c), (wk_ref, wv_ref), own2)
    get_freq.wait()
    freq = freq_ref[...]

    phase("core1_wait")
    receive(rb, c1r)
    hear(hear_x, "x")
    hear(hear_z.at[0], "z")
    tell(hear_z.at[1], "z")
    relayed = nx == 4
    deep = ROWS // 2
    for k in x_far:
        b = other_x(k)
        sums = (own[b] + rb[b].astype(F32)).astype(BF16)
        xs[2 * b] = sums[0:deep]
        xs[2 * b + 1] = sums[deep:]
        send(xs.at[2 * b], xr.at[2 * x], BIG, x1r, x=b)
        if relayed and k > 1:
            def direct():
                copy(xs.at[2 * b + 1], xr.at[2 * x + 1], BIG, x1r, x=b).start()

            pl.when(c == 0)(direct)
            if k == 2:

                @pl.when(c == 1)
                def _():
                    copy(xs.at[2 * b + 1], rel, BIG, relr, x=other_x(3)).start()

            sent[BIG] += deep * cols * 2
        else:
            send(xs.at[2 * b + 1], xr.at[2 * x + 1], BIG, x1r, x=b)
    receive(sscr, csr)
    ssx[...] = ssc[...] + sscr[...]
    for k in x_far:
        send(ssx, ssxr.at[x], SMALL, xsr, x=other_x(k))

    phase("keys")
    get_len.wait()
    get_start.wait()
    my = (x * nz + z) * nc + c
    count = nx * nz * nc

    def add_lengths(r, carry):
        before, total = carry
        return before + jnp.where(r < my, len_ref[r], 0), total + len_ref[r]

    offset, first_pos = lax.fori_loop(0, count, add_lengths, (jnp.int32(0), jnp.int32(0)))
    first_pos = first_pos + start_ref[0]
    live = len_ref[my]

    a_count = slots // CHUNK
    a_pos = (offset + CHUNK * iota((a_count, LANES), 0)).astype(F32)
    a_cos, a_sin = cos_sin(a_pos * freq)
    tab_a[0] = a_cos * mscale
    tab_a[1] = a_sin * mscale
    b_cos, b_sin = cos_sin(iota((CHUNK, LANES), 0).astype(F32) * freq)
    tab_b[0] = b_cos
    tab_b[1] = b_sin
    first_token = x * per_x + c * ROWS
    my_g, my_quarter = lax.div(z, quarters), lax.rem(z, quarters)
    k_first = first_token + my_quarter * tail
    q_pos = (first_pos + first_token + iota((ROWS, LANES), 0)).astype(F32)
    q_cos, q_sin = cos_sin(q_pos * freq)
    k_pos = (first_pos + k_first + iota((tail, LANES), 0)).astype(F32)
    k_cos, k_sin = cos_sin(k_pos * freq)
    q_cos, q_sin = q_cos * mscale, signed(q_sin * mscale)
    k_cos, k_sin = k_cos * mscale, signed(k_sin * mscale)

    get_k.wait()

    def slot_angles(a, size):
        cos_a = tab_a[0, pl.ds(a, 1), :]
        sin_a = tab_a[1, pl.ds(a, 1), :]
        cos_b, sin_b = tab_b[0, 0:size, :], tab_b[1, 0:size, :]
        return cos_a * cos_b - sin_a * sin_b, signed(sin_a * cos_b + cos_a * sin_b)

    tmp[0, 0 : 8 * kv, :] = kraw[0 : 8 * kv, :].astype(F32)
    slot_cos, slot_sin = slot_angles(0, 8)
    head_keys = [
        rotated(tmp[0, pl.ds(g, 8, stride=kv), :], slot_cos, slot_sin)[0:1] for g in range(kv)
    ]

    def rotate_chunks(j, _):
        for u in range(2):
            a = 2 * j + u
            at = pl.multiple_of(a * CHUNK, CHUNK)
            tmp[u] = kraw[pl.ds(pl.multiple_of(2 * at, 2 * CHUNK), 2 * CHUNK), :].astype(F32)
            cosine, sine = slot_angles(a, CHUNK)
            alive = at + iota((CHUNK, LANES), 0) < live
            for g in range(kv):
                keys = rotated(tmp[u, pl.ds(g, CHUNK, stride=kv), :], cosine, sine)
                ks[g, pl.ds(at, CHUNK), :] = jnp.where(alive, keys, head_keys[g]).astype(BF16)
        return 0

    steps = a_count // 2
    early = steps * 3 // 4
    lax.fori_loop(0, early, rotate_chunks, 0)

    phase("x1_wait")
    hear(hear_z.at[1], "z")
    tell(hear_z.at[2], "z")
    gathered = own[x] + rb[x].astype(F32)
    if relayed:

        @pl.when(c == 1)
        def _():
            b = other_x(3)
            receive(rel, relr)
            merged[...] = (own[b, deep:] + rb[b, deep:].astype(F32) + rel[...].astype(F32)).astype(BF16)
            copy(merged, xr.at[2 * x + 1], BIG, x1r, x=b).start()
            receive(xr.at[pl.ds(0, 2 * nx - 3)], x1r)

        @pl.when(c == 0)
        def _():
            receive(xr.at[pl.ds(0, 2 * nx - 2)], x1r)

    else:
        receive(xr.at[pl.ds(0, 2 * nx - 2)], x1r)
    for k in range(1, nx):
        b = other_x(k)
        second = xr[2 * b + 1].astype(F32)
        if relayed and k == 2:
            second = jnp.where(c == 0, second, 0.0)
        gathered = gathered + jnp.concatenate([xr[2 * b].astype(F32), second], 0)
    tell(hear_y.at[0], "y")
    hear(hear_z.at[2], "z")
    for t in range(nz):
        zs[t] = gathered[:, t * LANES : (t + 1) * LANES].astype(BF16)
    for k in z_far:
        b = other_z(k)
        send(zs.at[b], zr.at[z], BIG, z1r, z=b)
    squares = ssx[...]
    receive(ssxr.at[pl.ds(0, nx - 1)], xsr)
    for k in range(1, nx):
        squares = squares + ssxr[other_x(k)]
    ssz[...] = squares
    for k in z_far:
        send(ssz, sszr.at[z], SMALL, zsr, z=other_z(k))

    receive(rb2, d1r)
    for k in x_far:
        b = other_x(k)
        xs2[b] = (own2[b] + rb2[b].astype(F32)).astype(BF16)
        send(xs2.at[b], xr2.at[x], BIG, w1r, x=b)

    phase("values")
    lax.fori_loop(early, steps, rotate_chunks, 0)
    get_v.wait()

    def value_chunks(j, _):
        for u in range(2):
            at = pl.multiple_of((2 * j + u) * CHUNK, CHUNK)
            tmp[u] = vraw[pl.ds(pl.multiple_of(2 * at, 2 * CHUNK), 2 * CHUNK), :].astype(F32)
            alive = at + iota((CHUNK, LANES), 0) < live
            ones = jnp.where(alive, 1.0, 0.0).astype(BF16)
            for g in range(kv):
                values = jnp.where(alive, tmp[u, pl.ds(g, CHUNK, stride=kv), :], 0.0)
                vs[g, pl.ds(at, CHUNK), 0:LANES] = values.astype(BF16)
                vs[g, pl.ds(at, CHUNK), LANES:] = ones
        return 0

    lax.fori_loop(0, steps, value_chunks, 0)
    get_wo.wait()

    phase("kv_pieces")
    gathered = own2[x] + rb2[x].astype(F32)
    receive(xr2.at[pl.ds(0, nx - 1)], w1r)
    for k in range(1, nx):
        gathered = gathered + xr2[other_x(k)].astype(F32)
    for t in range(nz):
        g, quarter = t // quarters, t % quarters
        pair = [
            gathered[quarter * tail : (quarter + 1) * tail, at + g * LANES : at + (g + 1) * LANES]
            for at in (0, kc)
        ]
        zs2[t] = jnp.concatenate(pair, 0).astype(BF16)
    for k in z_far:
        b = other_z(k)
        send(zs2.at[b], zr2.at[z], BIG, v1r, z=b)

    phase("z1_wait")
    hear(hear_y.at[0], "y")
    tell(hear_y.at[1], "y")
    total = zs[z].astype(F32)
    receive(zr.at[pl.ds(0, nz - 1)], z1r)
    for k in range(1, nz):
        total = total + zr[other_z(k)].astype(F32)
    receive(sszr.at[pl.ds(0, nz - 1)], zsr)
    for k in range(1, nz):
        squares = squares + sszr[other_z(k)]
    wt[...] = as_columns(lax.rsqrt(squares * (1.0 / d_model) + epsilon))
    which = lax.div(first_token, LANES)
    lane = lax.rem(first_token, LANES)

    def inverse_of(at, size):
        cols = wt[pl.ds(pl.multiple_of(at, 8), size), :]
        picked = cols[:, 0:1]
        for r in range(1, span // LANES):
            picked = jnp.where(which == r, cols[:, r : r + 1], picked)
        return picked

    query = rotated(total * inverse_of(lane, ROWS), q_cos, q_sin) * LANES**-0.5
    qbuf[c, x, z] = query.astype(BF16)

    for k in z_far:
        send(qbuf.at[c, x, z], qbuf.at[c, x, z], BIG, z2r.at[z], z=other_z(k))

    @pl.when(c == 0)
    def _():
        mine = qbuf.at[c, x, z]
        for k in z_far:
            copy(mine, mine, BIG, c2r.at[x], z=other_z(k), c=1).start()
        copy(mine, mine, BIG, c2r.at[x], c=1).start()

    def piece_to_x(t):
        for k in x_far:
            send(qbuf.at[c, x, t], qbuf.at[c, x, t], BIG, x2r.at[x], x=other_x(k))

    piece_to_x(z)

    phase("z2_wait")
    for k in z_near:
        b = other_z(k)
        receive(qbuf.at[c, x, b], z2r.at[b])
        piece_to_x(b)

    def block_to_core(b):
        send(qbuf.at[c, b], qbuf.at[c, b], BIG, c2r.at[b], c=sib)

    @pl.when(c == 1)
    def _():
        copy(qbuf.at[c, x], qbuf.at[c, x], BIG, c2r.at[x], c=sib).start()

    sent[BIG] += heads * ROWS * LANES * 2

    phase("new_keys_wait")
    total = zs2[z].astype(F32)
    receive(zr2.at[pl.ds(0, nz - 1)], v1r)
    for k in range(1, nz):
        total = total + zr2[other_z(k)].astype(F32)
    inv_new = inverse_of(lane + my_quarter * tail, tail)
    new_k = (total[0:tail] * inv_new).astype(BF16).astype(F32)
    new_k = rotated(new_k, k_cos, k_sin)
    new_v = total[tail:] * inv_new
    empty = jnp.zeros((LANES - tail, LANES), F32)
    new_k = jnp.concatenate([new_k, empty], 0).astype(BF16)
    new_v = jnp.concatenate([new_v, empty], 0).astype(BF16)
    new_ones = jnp.where(iota((LANES, LANES), 0) < tail, 1.0, 0.0).astype(BF16)
    for g in range(kv):
        ks[g, slots:, :] = new_k
        vs[g, slots:, 0:LANES] = new_v
        vs[g, slots:, LANES:] = new_ones

    def attend(blocks):
        rows = len(blocks) * block
        token = jnp.concatenate(
            [
                other_x(k) * per_x + cc * ROWS + lax.rem(iota((block, LANES), 0), ROWS)
                for cc, k in blocks
            ],
            0,
        )
        lane = iota((rows, LANES), 1)
        seen = jnp.logical_and(lane < tail, k_first + lane <= token)
        for g in range(kv):
            q = [
                qbuf[cc, other_x(k), g * group : (g + 1) * group].reshape(block, LANES) for cc, k in blocks
            ]
            q = jnp.concatenate(q, 0)
            most = jnp.full((rows, LANES), negative, F32)
            for at in range(0, slots, KEYS):
                score = lax.dot_general(
                    q, ks[g, at : at + KEYS, :], (((1,), (1,)), ((), ())), preferred_element_type=F32
                )
                s_ref[g, :, at : at + KEYS] = score
                for lo in range(0, KEYS, LANES):
                    most = jnp.maximum(most, score[:, lo : lo + LANES])
            score = lax.dot_general(
                q, ks[g, slots:, :], (((1,), (1,)), ((), ())), preferred_element_type=F32
            )
            score = jnp.where(jnp.logical_and(seen, my_g == g), score, negative)
            most = jnp.max(jnp.maximum(most, score), axis=1, keepdims=True)
            acc = jnp.dot(
                jnp.exp(score - most).astype(BF16), vs[g, slots:, :], preferred_element_type=F32
            )
            for at in range(0, slots, KEYS):
                prob = jnp.exp(s_ref[g, :, at : at + KEYS] - most).astype(BF16)
                acc = acc + jnp.dot(prob, vs[g, at : at + KEYS, :], preferred_element_type=F32)
            sums = acc[:, LANES:]
            result = acc[:, 0:LANES] / sums
            lse = most + jnp.log(sums)
            for j, (cc, k) in enumerate(blocks):
                b, cut = other_x(k), slice(j * block, (j + 1) * block)
                if cc is sib:
                    obs[b, g * block : (g + 1) * block, :] = result[cut].astype(BF16)
                    lss[b, g : g + 1, :] = lse[cut].T[0:1]
                else:
                    ob[b, g * block : (g + 1) * block, :] = result[cut]
                    lb[b, g : g + 1, :] = lse[cut].T[0:1]
        for cc, k in blocks:
            if cc is sib:
                b = other_x(k)
                send(obs.at[b], obr.at[b], BIG, c3r.at[b], c=sib)
                send(lss.at[b], lsr.at[b], SMALL, c3lr.at[b], c=sib)

    away = sorted(
        ((i, j) for i in range(nx) for j in range(nz)),
        key=lambda k: -min(k[0], nx - k[0]) - min(k[1], nz - k[1]),
    )

    def join(places):
        weights, blocks = [], [other_x(k) for k in places]
        for b in blocks:
            receive(obr.at[b], c3r.at[b])
            receive(lsr.at[b], c3lr.at[b])
            logs = [lb[b], lsr[b]]
            top = jnp.maximum(*logs)
            lse = top + jnp.log(sum(jnp.exp(v - top) for v in logs))
            weights += [jnp.exp(v - lse) for v in logs]
            lxs[b] = lse
        columns = as_columns(jnp.concatenate(weights, 0))
        for i, b in enumerate(blocks):
            for g in range(kv):
                cut = slice(g * block, (g + 1) * block)
                at = 2 * kv * i + g
                out = columns[:, at : at + 1] * ob[b, cut, :]
                out = out + columns[:, at + kv : at + kv + 1] * obr[b, cut, :].astype(F32)
                oxs[b, g * group : (g + 1) * group] = out.astype(BF16).reshape(group, ROWS, LANES)
        slot = c * nx * nz + x * nz + z
        for i, j in away:
            if i in places and (i or j):
                b, t = other_x(i), other_z(j)
                send(oxs.at[b, t], oxr.at[slot], BIG, x3r, x=b, z=t, c=1)
                send(lxs.at[b], lxr.at[slot], SMALL, x3lr, x=b, z=t, c=1)
        if 0 in places:

            @pl.when(c == 0)
            def _():
                copy(oxs.at[x, z], oxr.at[slot], BIG, x3r, c=1).start()
                copy(lxs.at[x], lxr.at[slot], SMALL, x3lr, c=1).start()

            @pl.when(c == 1)
            def _():
                oxr[slot] = oxs[x, z]
                lxr[slot] = lxs[x]

    middle, final_x = list(range(1, nx - 1)), nx - 1
    phase("c2_wait")
    receive(qbuf.at[sib, x], c2r.at[x])
    phase("unit_0")
    attend([(c, 0), (sib, 0)])
    phase("x2_wait")
    for k in x_near:
        b = other_x(k)
        receive(qbuf.at[c, b], x2r.at[b])
        block_to_core(b)
    for k in x_far:
        send(wobuf.at[x, c], wobuf.at[x, c], WEIGHTS, wr, x=other_x(k))
    send(wobuf.at[x, c], wobuf.at[x, c], WEIGHTS, wcr, c=sib)
    if middle:
        phase("unit_1")
        attend([(c, k) for k in middle])
        phase("c2_wait2")
        for k in middle:
            receive(qbuf.at[sib, other_x(k)], c2r.at[other_x(k)])
        phase("unit_2")
        attend([(sib, k) for k in middle])
    phase("join_0")
    join([0])
    if middle:
        phase("join_1")
        join(middle)
    receive(qbuf.at[sib, other_x(final_x)], c2r.at[other_x(final_x)])
    phase("unit_3")
    attend([(sib, final_x), (c, final_x)])
    phase("join_3")
    join([final_x])
    receive(wobuf.at[pl.ds(0, nx - 1), c], wr)
    for k in range(1, nx):
        b = other_x(k)
        send(wobuf.at[b, c], wobuf.at[b, c], WEIGHTS, wcr, c=sib)

    phase("tail")
    hear(hear_y.at[1], "y")
    receive(wobuf.at[:, sib], wcr)

    def last(b, cc):
        copy(p5s.at[b, cc], p5r.at[y], LAST, y5r, x=b, c=cc, y=x).start()

    def finish():
        sources = nx * nz
        receive(oxr.at[pl.ds(0, 2 * sources - 1)], x3r)
        receive(lxr.at[pl.ds(0, 2 * sources - 1)], x3lr)
        shares = []
        for cc in range(nc):
            picked = []
            for i in range(sources):
                v = lxr[cc * sources + i]
                row = v[0:1]
                for g in range(1, kv):
                    row = jnp.where(my_g == g, v[g : g + 1], row)
                picked.append(row)
            logs = jnp.concatenate(picked, 0)
            logs = jnp.exp(logs - jnp.max(logs, axis=0, keepdims=True))
            shares.append(logs / jnp.sum(logs, axis=0, keepdims=True))
        wt[...] = as_columns(jnp.concatenate(shares, 0))
        mine = wt[pl.ds(pl.multiple_of(my_quarter * ROWS, ROWS), ROWS), :]
        for cc in range(nc):
            span_of = range(cc * sources, (cc + 1) * sources)
            attended = sum(mine[:, i : i + 1] * oxr[i].astype(F32) for i in span_of)
            att[z, cc * ROWS : (cc + 1) * ROWS, :] = attended.astype(BF16)
        for k in z_far:
            copy(att.at[z], att.at[z], BIG, z4r, z=other_z(k)).start()
        receive(att.at[pl.ds(0, nz - 1)], z4r)

        lhs = jnp.concatenate([att[t] for t in range(heads)], 1)
        rhs = wobuf[...].reshape(nx * nc * HALF, heads * LANES)
        got = lax.dot_general(lhs, rhs, (((1,), (1,)), ((), ())), preferred_element_type=F32)
        low = iota((ROWS, LANES), 1) < HALF
        for b in range(nx):
            both = got[:, b * LANES : (b + 1) * LANES]
            turned = pltpu.roll(both, HALF, 1)
            p5s[b, 0] = jnp.where(low, both[0:ROWS], turned[ROWS:]).astype(BF16)
            p5s[b, 1] = jnp.where(low, turned[0:ROWS], both[ROWS:]).astype(BF16)
        for k in x_far:
            for cc in range(nc):
                last(other_x(k), cc)
        last(x, 0)

        @pl.when(x != y)
        def _():
            last(x, 1)

        @pl.when(x == y)
        def _():
            p5r[y] = p5s[x, 1]

    pl.when(c == 1)(finish)

    phase("y5_wait")
    own_piece = jnp.logical_and(x == y, c == 1)

    @pl.when(jnp.logical_not(own_piece))
    def _():
        receive(p5r, y5r)

    @pl.when(own_piece)
    def _():
        receive(p5r.at[pl.ds(0, ny - 1)], y5r)

    final = sum(p5r[b].astype(F32) for b in range(ny))
    out_ref[0:ROWS, :] = final[:, 0:HALF].astype(BF16)
    out_ref[ROWS:, :] = pltpu.roll(final, HALF, 1)[:, 0:HALF].astype(BF16)

    phase("drain")

    def gone(ref, kind):
        copy(ref, ref, kind, c1r, c=sib).wait_send()

    line = LANES * jnp.dtype(BF16).itemsize
    piece = ROWS * LANES * 2

    @pl.when(c == 0)
    def _():
        gone(dummy.at[pl.ds(0, (sent[SMALL] + kv * LANES * 4) // (2 * line))], SMALL)
        gone(kraw.at[pl.ds(0, (sent[BIG] + piece) // line)], BIG)

    @pl.when(c == 1)
    def _():
        gone(dummy.at[pl.ds(0, sent[SMALL] // (2 * line))], SMALL)
        gone(kraw.at[pl.ds(0, (sent[BIG] + (nz - 1) * nc * piece) // line)], BIG)

    gone(kraw.at[pl.ds(0, sent[WEIGHTS] // line)], WEIGHTS)

    @pl.when(jnp.logical_and(c == 1, x != y))
    def _():
        gone(kraw.at[pl.ds(0, nx * nc * piece // line)], LAST)

    @pl.when(own_piece)
    def _():
        gone(kraw.at[pl.ds(0, (nx * nc - 1) * piece // line)], LAST)

    phase(None)


def local(
    sizes, hidden_in, norm_gain, w_query, w_key, w_value, w_out, cache_keys, cache_values, lengths, span_start
):
    nx, nz, nc, ny = sizes
    slots, kv, head_dim = cache_keys.shape
    span, depth = hidden_in.shape
    heads = w_query.shape[1] // head_dim
    assert head_dim == LANES and heads == nz and nc == 2 and span == nx * nc * ROWS and nx == ny
    assert w_out.shape[1] == HALF and slots % KEYS == 0 and kv == 2
    cols, cols2 = w_query.shape[1], 2 * w_key.shape[1]
    block = heads * ROWS
    piece = 2 * (ROWS * kv // nz)
    keys = slots + LANES
    rows = 2 * (heads // kv) * ROWS
    lines = span // LANES
    hbm = pl.BlockSpec(memory_space=pltpu.HBM)
    V = pltpu.VMEM
    dma = pltpu.SemaphoreType.DMA
    scratch = [
        pltpu.SMEM(lengths.shape, jnp.int32), pltpu.SMEM(span_start.shape, jnp.int32),
        V((depth, span), BF16), V((1, depth), BF16), V(w_query.shape, BF16), V(w_key.shape, BF16),
        V(w_value.shape, BF16), V((1, LANES), F32),
        V((slots * kv, LANES), BF16), V((slots * kv, LANES), BF16), V((2, CHUNK * kv, LANES), F32),
        V((kv, keys, LANES), BF16), V((kv, keys, 2 * LANES), BF16),
        V((2, slots // CHUNK, LANES), F32), V((2, CHUNK, LANES), F32),
        V((nx, ROWS, cols), BF16), V((nx, ROWS, cols), BF16), V((nx, ROWS, cols), F32),
        V((2 * nx, ROWS // 2, cols), BF16), V((2 * nx, ROWS // 2, cols), BF16),
        V((nz, ROWS, LANES), BF16), V((nz, ROWS, LANES), BF16),
        V((nx, ROWS, cols2), BF16), V((nx, ROWS, cols2), BF16), V((nx, ROWS, cols2), F32),
        V((nx, ROWS, cols2), BF16), V((nx, ROWS, cols2), BF16),
        V((nz, piece, LANES), BF16), V((nz, piece, LANES), BF16),
        V((lines, LANES), F32), V((lines, LANES), F32), V((lines, LANES), F32), V((nx, lines, LANES), F32),
        V((lines, LANES), F32), V((nz, lines, LANES), F32),
        V((nc, nx, heads, ROWS, LANES), BF16), V((kv, rows, slots), F32),
        V((nx, block, LANES), F32), V((nx, kv, LANES), F32),
        V((nx, block, LANES), BF16), V((nx, block, LANES), BF16), V((nx, kv, LANES), F32), V((nx, kv, LANES), F32),
        V((nx, nz, ROWS, LANES), BF16), V((nc * nx * nz, ROWS, LANES), BF16),
        V((nx, kv, LANES), F32), V((nc * nx * nz, kv, LANES), F32),
        V((LANES, LANES), F32),
        V((heads, nc * ROWS, LANES), BF16), V((nx, nc, HALF, w_out.shape[0]), BF16),
        V((nx, nc, ROWS, LANES), BF16), V((ny, ROWS, LANES), BF16),
        V((128, 1, LANES), F32), dma((11,)), dma((4,)),
        pltpu.SemaphoreType.REGULAR, pltpu.SemaphoreType.REGULAR((3,)), pltpu.SemaphoreType.REGULAR((2,)),
        V((ROWS // 2, cols), BF16), V((ROWS // 2, cols), BF16),
        dma, dma, dma, dma, dma, dma, dma, dma, dma, dma,
        dma((nz,)), dma((nx,)), dma((nx,)), dma, dma, dma((nx,)), dma((nx,)), dma, dma, dma, dma,
    ]
    return pl.pallas_call(
        functools.partial(kernel, (nx, nz, nc, ny, nx * nz * nc * depth)),
        out_shape=pltpu.VMEM((nc * ROWS, HALF), BF16),
        in_specs=[hbm] * 11,
        out_specs=pl.BlockSpec(memory_space=pltpu.VMEM),
        scratch_shapes=scratch,
        compiler_params=pltpu.CompilerParams(
            collective_id=0, has_side_effects=True, vmem_limit_bytes=60 * 1024 * 1024
        ),
    )(
        lengths, span_start, hidden_in.T, norm_gain, w_query, w_key, w_value, w_out.T, frequencies(),
        cache_keys.reshape(slots * kv, LANES), cache_values.reshape(slots * kv, LANES),
    )


def solution(mesh):
    physical = mesh.devices.shape
    ny = mesh.shape["head"]
    nc, nz = 2, 8
    nx = physical[0] // (nc * nz)
    finer = Mesh(mesh.devices.reshape(nx, nz, nc, ny), ("x", "z", "c", "y"))
    seq = ("x", "z", "c")
    return jax.shard_map(
        functools.partial(local, (nx, nz, nc, ny)),
        mesh=finer,
        in_specs=(
            P(None, seq), P(None, seq), P(seq, "y"), P(seq, "y"), P(seq, "y"), P("y", seq),
            P(seq, "y", None), P(seq, "y", None), P(), P(),
        ),
        out_specs=P("y", seq),
        check_vma=False,
    )
```
